32 devices in a mesh: gx: 8 (over y, x, core), gy: 4 (over z).
Axes of the slice: x: 2, y: 2, z: 4, core: 2. Of those that a mesh axis runs over, the one named last changes fastest.
Arguments:
- terminal: float32 [128, 2048], P('gx', 'gy'), may hold values from -15 to 15
- initial_density: float32 [128, 2048], P('gx', 'gy'), may hold values from 0.1 to 1
- density_guess: float32 [2, 128, 2048], P(None, 'gx', 'gy'), may hold values from 0.1 to 1
- diagonal: float32 [128, 2048], P('gx', 'gy'), may hold values from 0.1 to 2
Outputs:
- value_field: float32 [128, 2048], P('gx', 'gy')
- density_field: float32 [128, 2048], P('gx', 'gy')
The draws below stay inside these ranges and needn't reach their ends.
All inputs are finite; a program needn't handle non-finite values.
Results may differ from the reference program's by a relative error of at most 0.00011.
Values sent between devices are 32-bit elements; how exact they have to be, the bound alone decides.
A program may use at most 64 MiB of HBM per device.

```python
import math
import jax
import jax.numpy as jnp

LEVELS = 2
STEPS = 3
NX = 128
NY = 2048


def draw_terminal(key, part):
    rows = jnp.arange(NX, dtype=jnp.float32)[:, None]
    scale = jnp.exp(jnp.log(3.0) * rows / max(NX - 1, 1))
    noise = jnp.clip(jax.random.normal(key, (NX, NY), jnp.float32), -5.0, 5.0)
    return scale * noise


def block_levels(rng, dims, pieces, low, largest):
    def one(position, shards_of):
        heights = jax.random.uniform(jax.random.fold_in(jax.random.fold_in(rng, 6), position), (shards_of,), jnp.float32, low / len(pieces), largest / len(pieces))
        return jnp.repeat(jnp.exp(heights), dims[position] // shards_of).reshape((-1,) + (1,) * (len(dims) - position - 1))

    gain = one(*pieces[0])
    for cut in pieces[1:]:
        gain = gain * one(*cut)
    return gain


def setup_inputs(seed: int = 0) -> dict:
    splits = jax.random.split(jax.random.key(seed), 5)
    terminal = draw_terminal(jax.random.fold_in(splits[4], 71), 0)
    initial_density = jnp.clip(jnp.exp(math.log(1.0) - 2.3025851 * jax.random.uniform(splits[1], (NX, NY), jnp.float32) ** block_levels(splits[1], (NX, NY), ((0, 8), (1, 4)), -0.2, 0.2)), 0.1, 1.0)
    density_guess = jnp.clip(jnp.exp(math.log(1.0) - 2.3025851 * jax.random.uniform(splits[2], (LEVELS, NX, NY), jnp.float32) ** block_levels(splits[2], (LEVELS, NX, NY), ((1, 8), (2, 4)), -0.2, 0.2)), 0.1, 1.0)
    diagonal = jnp.clip(jnp.exp(math.log(2.0) - 2.9957323 * jax.random.uniform(splits[3], (NX, NY), jnp.float32) ** block_levels(splits[3], (NX, NY), ((0, 8), (1, 4)), -0.2, 0.2)), 0.1, 2.0)
    return {"terminal": terminal, "initial_density": initial_density, "density_guess": density_guess, "diagonal": diagonal}


inv_step = 0.5
coupling = 0.5


def apply_padded(padded, center, diagonal):
    beside = padded[2:, 1:-1] + padded[:-2, 1:-1] + padded[1:-1, 2:] + padded[1:-1, :-2]
    return (inv_step + diagonal) * center + (4.0 * center - beside)


def hamiltonian(padded):
    center = padded[1:-1, 1:-1]
    back_x = center - padded[:-2, 1:-1]
    ahead_x = padded[2:, 1:-1] - center
    back_y = center - padded[1:-1, :-2]
    ahead_y = padded[1:-1, 2:] - center
    return 0.5 * (jnp.maximum(back_x, 0.0) ** 2 + jnp.minimum(ahead_x, 0.0) ** 2
                  + jnp.maximum(back_y, 0.0) ** 2 + jnp.minimum(ahead_y, 0.0) ** 2)


def divergence(pad_m, pad_u):
    m_mid = pad_m[1:-1, 1:-1]
    u_mid = pad_u[1:-1, 1:-1]
    speed_ahead = -(pad_u[2:, 1:-1] - u_mid)
    speed_back = -(u_mid - pad_u[:-2, 1:-1])
    flux_ahead = jnp.maximum(speed_ahead, 0.0) * m_mid + jnp.minimum(speed_ahead, 0.0) * pad_m[2:, 1:-1]
    flux_back = jnp.maximum(speed_back, 0.0) * pad_m[:-2, 1:-1] + jnp.minimum(speed_back, 0.0) * m_mid
    total = flux_ahead - flux_back
    speed_ahead = -(pad_u[1:-1, 2:] - u_mid)
    speed_back = -(u_mid - pad_u[1:-1, :-2])
    flux_ahead = jnp.maximum(speed_ahead, 0.0) * m_mid + jnp.minimum(speed_ahead, 0.0) * pad_m[1:-1, 2:]
    flux_back = jnp.maximum(speed_back, 0.0) * pad_m[1:-1, :-2] + jnp.minimum(speed_back, 0.0) * m_mid
    return total + flux_ahead - flux_back


def solve(rhs, diagonal):
    answer = jnp.zeros_like(rhs)
    resid = rhs
    direction = rhs
    norm_now = jnp.sum(resid * resid)
    for step in range(STEPS):
        image = apply_padded(jnp.pad(direction, 1), direction, diagonal)
        alpha = norm_now / jnp.sum(direction * image)
        answer = answer + alpha * direction
        resid = resid - alpha * image
        norm_next = jnp.sum(resid * resid)
        direction = resid + (norm_next / norm_now) * direction
        norm_now = norm_next
    return answer


def reference(terminal, initial_density, density_guess, diagonal):
    levels = [None] * LEVELS
    later = terminal
    for level in reversed(range(LEVELS)):
        rhs = inv_step * later - hamiltonian(jnp.pad(later, 1)) + coupling * density_guess[level]
        later = solve(rhs, diagonal)
        levels[level] = later
    density = initial_density
    for level in range(LEVELS):
        rhs = inv_step * density - divergence(jnp.pad(density, 1), jnp.pad(levels[level], 1))
        density = solve(rhs, diagonal)
    return levels[0], density
```

```python
import functools

import jax
import jax.numpy as jnp
from jax import lax
from jax.experimental import pallas as pl
from jax.experimental.pallas import tpu as pltpu
from jax.sharding import PartitionSpec as P

MESH = pl.DeviceIdType.MESH

LEVELS = 2
MARGIN = 16
LANES = 128

inv_step = 0.5
coupling = 0.5

SCALE = 0.25
SHIFT = 5.5

DIRECTIONS = [(r, c) for r in (-1, 0, 1) for c in (-1, 0, 1) if (r, c) != (0, 0)]
TINY = 2e-7


def solve_small(nu):
    g00 = nu[1] / SCALE + SHIFT * nu[0]
    g01 = nu[2] / SCALE + SHIFT * nu[1]
    g02 = nu[3] / SCALE + SHIFT * nu[2]
    g12 = nu[4] / SCALE + SHIFT * nu[3]
    g22 = nu[5] / SCALE + SHIFT * nu[4]
    g11 = g02
    inv0 = 1.0 / g00
    l10 = g01 * inv0
    l20 = g02 * inv0
    d1 = g11 - l10 * g01
    ok1 = d1 > TINY * g11
    inv1 = jnp.where(ok1, 1.0 / jnp.where(ok1, d1, 1.0), 0.0)
    t = g12 - l20 * g01
    l21 = t * inv1
    d2 = g22 - l20 * g02 - l21 * t
    ok2 = ok1 & (d2 > TINY * g22)
    inv2 = jnp.where(ok2, 1.0 / jnp.where(ok2, d2, 1.0), 0.0)
    y1 = nu[1] - l10 * nu[0]
    y2 = nu[2] - l20 * nu[0] - l21 * y1
    c2 = y2 * inv2
    c1 = y1 * inv1 - l21 * c2
    c0 = nu[0] * inv0 - l10 * c1 - l20 * c2
    return c0, c1, c2


def kernel(nx, ny, term_ref, dens_ref, guess_ref, diag_ref, both_ref,
           main, left, right, sent, slots, halo_send, halo_recv, own_sem, sum_send, sum_recv,
           ready, scaled_tall, scaled_mid, scaled_small):
    rows, cols = term_ref.shape
    gx = lax.axis_index("gx")
    gy = lax.axis_index("gy")
    count = nx * ny
    me = gx * ny + gy

    def inside(dr, dc):
        ok = None
        for here_at, step, size in ((gx, dr, nx), (gy, dc, ny)):
            if step == 1:
                test = here_at < size - 1
            elif step == -1:
                test = here_at > 0
            else:
                continue
            ok = test if ok is None else ok & test
        return ok

    def across(k):
        return (lax.rem(gx + k, nx), gy)

    def along(k):
        return (gx, lax.rem(gy + k, ny))

    barrier = pltpu.get_barrier_semaphore()
    greeted = nx + ny - 2
    for k in range(1, nx):
        pl.semaphore_signal(barrier, inc=1, device_id=across(k), device_id_type=MESH)
    for k in range(1, ny):
        pl.semaphore_signal(barrier, inc=1, device_id=along(k), device_id_type=MESH)
    for dr, dc in DIRECTIONS:
        if dr != 0 and dc != 0:
            there = inside(dr, dc)
            greeted = greeted + jnp.where(there, 1, 0)

            @pl.when(there)
            def _():
                pl.semaphore_signal(
                    barrier, inc=1, device_id=(gx + dr, gy + dc), device_id_type=MESH)

    here = pl.ds(MARGIN, rows)
    own = [
        pltpu.make_async_copy(source, main.at[at, here], own_sem.at[at])
        for at, source in enumerate(
            (term_ref, diag_ref, guess_ref.at[1], guess_ref.at[0], dens_ref))
    ]
    for copy in own:
        copy.start()
    wide = cols + LANES
    half = LANES // 2
    tall = rows + 2 * MARGIN
    low_mid, high_mid = MARGIN - 8, MARGIN + rows + 8

    def mask_of(size, cyclic, margin):
        row = lax.broadcasted_iota(jnp.int32, (size, wide), 0)
        col = lax.broadcasted_iota(jnp.int32, (size, wide), 1)
        col_low = jnp.where(gy < ny - 1, cols + half, cols)
        col_high = jnp.where(gy > 0, cols + half, wide)
        ok = (col < col_low) | (col >= col_high)
        if cyclic:
            row_low = jnp.where(gx < nx - 1, rows + 4, rows)
            row_high = jnp.where(gx > 0, rows + 4, size)
            return ok & ((row < row_low) | (row >= row_high))
        row_low = jnp.where(gx > 0, 0, margin)
        row_high = jnp.where(gx < nx - 1, size, margin + rows)
        return ok & (row >= row_low) & (row < row_high)

    scaled = {"tall": scaled_tall, "mid": scaled_mid, "small": scaled_small}
    scaled_tall[...] = jnp.where(mask_of(tall, False, MARGIN), SCALE, 0.0)
    scaled_mid[...] = jnp.where(mask_of(rows + 16, False, 8), SCALE, 0.0)
    scaled_small[...] = jnp.where(mask_of(rows + 8, True, 4), SCALE, 0.0)

    for copy in own:
        copy.wait()
    pl.semaphore_wait(barrier, greeted)

    def pieces(dr):
        if dr == 0:
            return [(0, 3, 0, rows), (3, 2, 0, rows)]
        return [(0, 3, 0, 8), (0, 4, 8, 8), (3, 2, 0, 8)]

    def halo(d, piece):
        dr, dc = DIRECTIONS[d]
        first, many, out, size = pieces(dr)[piece]
        if dr == 0:
            src_rows, dst_rows = here, here
        elif dr == 1:
            src_rows = pl.ds(MARGIN + rows - out - size, size)
            dst_rows = pl.ds(MARGIN - out - size, size)
        else:
            src_rows = pl.ds(MARGIN + out, size)
            dst_rows = pl.ds(MARGIN + rows + out, size)
        if dc == 0:
            src_cols, buf = pl.ds(0, cols), main
        elif dc == 1:
            src_cols, buf = pl.ds(cols - LANES, LANES), left
        else:
            src_cols, buf = pl.ds(0, LANES), right
        return pltpu.make_async_remote_copy(
            src_ref=main.at[pl.ds(first, many), src_rows, src_cols],
            dst_ref=buf.at[pl.ds(first, many), dst_rows, :],
            send_sem=halo_send.at[d, piece], recv_sem=halo_recv.at[d, piece],
            device_id=(gx + dr, gy + dc), device_id_type=MESH)

    def each_halo(near, act, back=False):
        for d, (dr, dc) in enumerate(DIRECTIONS):
            @pl.when(inside(-dr, -dc) if back else inside(dr, dc))
            def _():
                for piece in [0] if near else range(1, len(pieces(dr))):
                    act(halo(d, piece))

    each_halo(True, lambda copy: copy.start())
    for k in range(1, nx):
        pl.semaphore_signal(ready, inc=1, device_id=across(k), device_id_type=MESH)
    each_halo(False, lambda copy: copy.start())

    def shrink(x, start):
        sub = lax.broadcasted_iota(jnp.int32, (8, x.shape[1]), 0)
        ends = jnp.where(sub < 4, x[start + rows:start + rows + 8], x[start - 8:start])
        return jnp.concatenate([x[start:start + rows], ends], axis=0)

    def strip(a, begin, end):
        lane = lax.broadcasted_iota(jnp.int32, (end - begin, LANES), 1)
        edge = jnp.where(lane < half, right[a, begin:end], left[a, begin:end])
        return jnp.concatenate([main[a, begin:end], edge], axis=1)

    def field(a, window):
        if window == "tall":
            return strip(a, 0, tall)
        x = strip(a, low_mid, high_mid)
        return x if window == "mid" else shrink(x, 8)

    def up(x):
        return pltpu.roll(x, 1, 0)

    def down(x):
        return pltpu.roll(x, x.shape[0] - 1, 0)

    def before(x):
        return pltpu.roll(x, 1, 1)

    def after(x):
        return pltpu.roll(x, x.shape[1] - 1, 1)

    def masked(x, window):
        return jnp.where(scaled[window][...] > 0.0, x, 0.0)

    def core_of(window):
        return masked(SCALE * (field(1, window) + (inv_step + 4.0 - SHIFT)), window)

    def apply_b(v, core, window):
        beside = (up(v) + down(v)) + (before(v) + after(v))
        return core * v - scaled[window][...] * beside

    def apply_half(v, core):
        return (0.5 * core) * v - SCALE * (down(v) + after(v))

    def hamiltonian(u):
        dx = u - up(u)
        dy = u - before(u)
        px, qx = jnp.maximum(dx, 0.0), jnp.minimum(dx, 0.0)
        py, qy = jnp.maximum(dy, 0.0), jnp.minimum(dy, 0.0)
        return (px * px + down(qx * qx)) + (py * py + after(qy * qy))

    def faces(u):
        sx = u - down(u)
        sy = u - after(u)
        return jnp.maximum(sx, 0.0), jnp.minimum(sx, 0.0), jnp.maximum(sy, 0.0), jnp.minimum(sy, 0.0)

    def advance(m, face, window):
        px, qx, py, qy = face
        fx = px * m + qx * down(m)
        fy = py * m + qy * after(m)
        net = (fx - up(fx)) + (fy - before(fy))
        return scaled[window][...] * ((inv_step / SCALE) * m - (1.0 / SCALE) * net)

    def value_rhs(later, level, window):
        guess = masked(coupling * field(2 if level == 1 else 3, window), window)
        own_part = (inv_step / SCALE) * later - (0.5 / SCALE) * hamiltonian(later)
        return scaled[window][...] * own_part + guess

    def fold(p):
        parts = [p[i:i + 8, j:j + LANES] for i in range(0, rows, 8) for j in range(0, cols, LANES)]
        while len(parts) > 1:
            odd = parts[len(parts) // 2 * 2:]
            parts = [parts[i] + parts[i + 1] for i in range(0, len(parts) - 1, 2)] + odd
        return parts[0]

    def dot(x, y):
        return fold(x * y)

    sub8 = lax.broadcasted_iota(jnp.int32, (8, LANES), 0)
    lane8 = lax.broadcasted_iota(jnp.int32, (8, LANES), 1)

    def pack(tiles):
        spread = None
        for first in range(0, len(tiles), 8):
            group = tiles[first:first + 8]
            group = group + [jnp.zeros((8, LANES), jnp.float32)] * (8 - len(group))
            for step in (4, 2, 1):
                keep = lax.rem(sub8, 2 * step) < step
                group = [
                    jnp.where(keep, a + pltpu.roll(a, 8 - step, 0), b + pltpu.roll(b, step, 0))
                    for a, b in zip(group[:step], group[step:])
                ]
            sums = jnp.sum(group[0], axis=1, keepdims=True)
            part = jnp.where(lane8 == sub8 + first, sums, 0.0)
            spread = part if spread is None else spread + part
        return jnp.sum(spread, axis=0, keepdims=True)

    def send_sums(which, values):
        packed = pack(values)
        sent[which] = packed
        slots[which, me] = packed

        def send(px, py):
            pltpu.make_async_remote_copy(
                src_ref=sent.at[which], dst_ref=slots.at[which, me],
                send_sem=sum_send.at[which], recv_sem=sum_recv.at[which],
                device_id=(px, py), device_id_type=MESH).start()

        columns = [lax.rem(gy + k, ny) for k in range(ny)]

        def line(k, carry):
            px = lax.rem(gx + k, nx)
            for py in columns:
                send(px, py)
            return carry

        lax.fori_loop(1, nx, line, 0)
        for py in columns[1:]:
            send(gx, py)

    def take_sums(which, many):
        others = slots.at[which, pl.ds(0, count - 1)]
        pltpu.make_async_copy(others, others, sum_recv.at[which]).wait()
        total = jnp.sum(slots[which], axis=0)
        return [total[:, k:k + 1] for k in range(many)]

    def basis(b, core, window, last=True):
        v1 = apply_b(b, core, window)
        v2 = apply_b(v1, core, window)
        return (b, v1, v2, apply_half(v2, core)) if last else (b, v1, v2)

    def mix(c, v):
        return c[0] * v[0] + c[1] * v[1] + c[2] * v[2]

    def pairs(x, y):
        return [dot(x[0], y[0]), dot(x[0], y[1]), dot(x[1], y[1]),
                dot(x[1], y[2]), dot(x[2], y[2]),
                2.0 * dot(x[2], x[3]) if x is y
                else fold(x[2] * y[3] + y[2] * x[3])]

    def own_small(v):
        return [x[:rows, :cols] for x in v]

    each_halo(True, lambda copy: copy.wait_recv(), back=True)
    small_core = core_of("small")
    later = masked(field(0, "small"), "small")
    w = own_small(basis(value_rhs(later, 1, "small"), small_core, "small"))
    moments = pairs(w, w)
    pl.semaphore_wait(ready, nx - 1)
    send_sums(0, moments)
    each_halo(False, lambda copy: copy.wait_recv(), back=True)
    core = core_of("tall")
    later = masked(field(0, "tall"), "tall")
    v = basis(value_rhs(later, 1, "tall"), core, "tall", last=False)
    vs = [shrink(x, MARGIN) for x in v]
    c = solve_small(take_sums(0, 6))

    first_small = mix(c, vs)
    w = own_small(basis(value_rhs(first_small, 0, "small"), small_core, "small"))
    send_sums(1, pairs(w, w))
    first = mix(c, v)
    v = basis(value_rhs(first, 0, "tall"), core, "tall", last=False)
    v = [x[low_mid:high_mid] for x in v]
    face = faces(first_small)
    density = masked(field(4, "mid"), "mid")
    mid_core = core_of("mid")
    c = solve_small(take_sums(1, 6))
    second = mix(c, v)

    a = basis(advance(density, faces(second), "mid"), mid_core, "mid", last=False)
    a = [shrink(x, 8) for x in a]
    last = apply_half(a[2], small_core)
    inner = own_small(a + [last])
    families = [
        own_small(basis(advance(a[i], face, "small"), small_core, "small")) for i in range(3)]
    moments = pairs(inner, inner)
    for i in range(3):
        for j in range(i, 3):
            moments += pairs(families[i], families[j])
    send_sums(2, moments)
    both_ref[0] = second[8:8 + rows, :cols]
    each_halo(True, lambda copy: copy.wait_send())
    each_halo(False, lambda copy: copy.wait_send())
    for which in range(3):
        others = slots.at[which, pl.ds(0, count - 1)]
        pltpu.make_async_copy(others, others, sum_send.at[which]).wait()
    total = take_sums(2, len(moments))
    c = solve_small(total[:6])
    nu = [0.0] * 6
    at = 6
    for i in range(3):
        for j in range(i, 3):
            weight = c[i] * c[j] * (1.0 if i == j else 2.0)
            for k in range(6):
                nu[k] = nu[k] + weight * total[at + k]
            at += 6
    e = solve_small(nu)
    result = None
    for i in range(3):
        for k in range(3):
            part = (c[i] * e[k]) * families[i][k]
            result = part if result is None else result + part
    both_ref[1] = result


def solution(mesh):
    nx, ny = mesh.shape["gx"], mesh.shape["gy"]

    def shards(terminal, initial_density, density_guess, diagonal):
        rows, cols = terminal.shape
        tall = rows + 2 * MARGIN
        hbm = pl.BlockSpec(memory_space=pl.ANY)
        vmem = pl.BlockSpec(memory_space=pltpu.VMEM)
        shape = jax.ShapeDtypeStruct((rows, cols), jnp.float32)
        both = pl.pallas_call(
            functools.partial(kernel, nx, ny),
            out_shape=jax.ShapeDtypeStruct((2, rows, cols), jnp.float32),
            in_specs=[hbm] * 4,
            out_specs=vmem,
            scratch_shapes=[
                pltpu.VMEM((5, tall, cols), jnp.float32),
                pltpu.VMEM((5, tall, LANES), jnp.float32),
                pltpu.VMEM((5, tall, LANES), jnp.float32),
                pltpu.VMEM((3, 1, LANES), jnp.float32),
                pltpu.VMEM((3, nx * ny, 1, LANES), jnp.float32),
                pltpu.SemaphoreType.DMA((8, 3)),
                pltpu.SemaphoreType.DMA((8, 3)),
                pltpu.SemaphoreType.DMA((5,)),
                pltpu.SemaphoreType.DMA((3,)),
                pltpu.SemaphoreType.DMA((3,)),
                pltpu.SemaphoreType.REGULAR,
                pltpu.VMEM((tall, cols + LANES), jnp.float32),
                pltpu.VMEM((rows + 16, cols + LANES), jnp.float32),
                pltpu.VMEM((rows + 8, cols + LANES), jnp.float32),
            ],
            compiler_params=pltpu.CompilerParams(collective_id=0, has_side_effects=True, vmem_limit_bytes=4 * 1024 * 1024),
        )(*[pltpu.with_memory_space_constraint(x, pltpu.HBM) for x in (terminal, initial_density, density_guess, diagonal)])
        return both[0], both[1]

    placed = (P("gx", "gy"), P("gx", "gy"), P(None, "gx", "gy"), P("gx", "gy"))
    return jax.shard_map(
        shards,
        mesh=mesh,
        in_specs=placed,
        out_specs=(P("gx", "gy"), P("gx", "gy")),
        check_vma=False,
    )
```

```python
import functools

import jax
import jax.numpy as jnp
from jax import lax
from jax.experimental import pallas as pl
from jax.experimental.pallas import tpu as pltpu
from jax.sharding import PartitionSpec as P

MESH = pl.DeviceIdType.MESH

LEVELS = 2
MARGIN = 16
LANES = 128

inv_step = 0.5
coupling = 0.5

SCALE = 0.25
SHIFT = 5.5

DIRECTIONS = [(r, c) for r in (-1, 0, 1) for c in (-1, 0, 1) if (r, c) != (0, 0)]
TINY = 2e-7


def solve_small(nu):
    g00 = nu[1] / SCALE + SHIFT * nu[0]
    g01 = nu[2] / SCALE + SHIFT * nu[1]
    g02 = nu[3] / SCALE + SHIFT * nu[2]
    g12 = nu[4] / SCALE + SHIFT * nu[3]
    g22 = nu[5] / SCALE + SHIFT * nu[4]
    g11 = g02
    inv0 = 1.0 / g00
    l10 = g01 * inv0
    l20 = g02 * inv0
    d1 = g11 - l10 * g01
    ok1 = d1 > TINY * g11
    inv1 = jnp.where(ok1, 1.0 / jnp.where(ok1, d1, 1.0), 0.0)
    t = g12 - l20 * g01
    l21 = t * inv1
    d2 = g22 - l20 * g02 - l21 * t
    ok2 = ok1 & (d2 > TINY * g22)
    inv2 = jnp.where(ok2, 1.0 / jnp.where(ok2, d2, 1.0), 0.0)
    y1 = nu[1] - l10 * nu[0]
    y2 = nu[2] - l20 * nu[0] - l21 * y1
    c2 = y2 * inv2
    c1 = y1 * inv1 - l21 * c2
    c0 = nu[0] * inv0 - l10 * c1 - l20 * c2
    return c0, c1, c2


def kernel(nx, ny, term_ref, dens_ref, guess_ref, diag_ref, both_ref,
           main, left, right, sent, slots, halo_send, halo_recv, own_sem, sum_send, sum_recv,
           ready, scaled_tall, scaled_mid, scaled_small):
    rows, cols = term_ref.shape
    gx = lax.axis_index("gx")
    gy = lax.axis_index("gy")
    count = nx * ny
    me = gx * ny + gy

    def inside(dr, dc):
        ok = None
        for here_at, step, size in ((gx, dr, nx), (gy, dc, ny)):
            if step == 1:
                test = here_at < size - 1
            elif step == -1:
                test = here_at > 0
            else:
                continue
            ok = test if ok is None else ok & test
        return ok

    def across(k):
        return (lax.rem(gx + k, nx), gy)

    def along(k):
        return (gx, lax.rem(gy + k, ny))

    barrier = pltpu.get_barrier_semaphore()
    greeted = nx + ny - 2
    for k in range(1, nx):
        pl.semaphore_signal(barrier, inc=1, device_id=across(k), device_id_type=MESH)
    for k in range(1, ny):
        pl.semaphore_signal(barrier, inc=1, device_id=along(k), device_id_type=MESH)
    for dr, dc in DIRECTIONS:
        if dr != 0 and dc != 0:
            there = inside(dr, dc)
            greeted = greeted + jnp.where(there, 1, 0)

            @pl.when(there)
            def _():
                pl.semaphore_signal(
                    barrier, inc=1, device_id=(gx + dr, gy + dc), device_id_type=MESH)

    here = pl.ds(MARGIN, rows)
    own = [
        pltpu.make_async_copy(source, main.at[at, here], own_sem.at[at])
        for at, source in enumerate(
            (term_ref, diag_ref, guess_ref.at[1], guess_ref.at[0], dens_ref))
    ]
    for copy in own:
        copy.start()
    wide = cols + LANES
    half = LANES // 2
    tall = rows + 2 * MARGIN
    low_mid, high_mid = MARGIN - 8, MARGIN + rows + 8

    def mask_of(size, cyclic, margin):
        row = lax.broadcasted_iota(jnp.int32, (size, wide), 0)
        col = lax.broadcasted_iota(jnp.int32, (size, wide), 1)
        col_low = jnp.where(gy < ny - 1, cols + half, cols)
        col_high = jnp.where(gy > 0, cols + half, wide)
        ok = (col < col_low) | (col >= col_high)
        if cyclic:
            row_low = jnp.where(gx < nx - 1, rows + 4, rows)
            row_high = jnp.where(gx > 0, rows + 4, size)
            return ok & ((row < row_low) | (row >= row_high))
        row_low = jnp.where(gx > 0, 0, margin)
        row_high = jnp.where(gx < nx - 1, size, margin + rows)
        return ok & (row >= row_low) & (row < row_high)

    scaled = {"tall": scaled_tall, "mid": scaled_mid, "small": scaled_small}
    scaled_tall[...] = jnp.where(mask_of(tall, False, MARGIN), SCALE, 0.0)
    scaled_mid[...] = jnp.where(mask_of(rows + 16, False, 8), SCALE, 0.0)
    scaled_small[...] = jnp.where(mask_of(rows + 8, True, 4), SCALE, 0.0)

    for copy in own:
        copy.wait()
    pl.semaphore_wait(barrier, greeted)

    def pieces(dr):
        if dr == 0:
            return [(0, 3, 0, rows), (3, 2, 0, rows)]
        return [(0, 3, 0, 8), (0, 4, 8, 8), (3, 2, 0, 8)]

    def halo(d, piece):
        dr, dc = DIRECTIONS[d]
        first, many, out, size = pieces(dr)[piece]
        if dr == 0:
            src_rows, dst_rows = here, here
        elif dr == 1:
            src_rows = pl.ds(MARGIN + rows - out - size, size)
            dst_rows = pl.ds(MARGIN - out - size, size)
        else:
            src_rows = pl.ds(MARGIN + out, size)
            dst_rows = pl.ds(MARGIN + rows + out, size)
        if dc == 0:
            src_cols, buf = pl.ds(0, cols), main
        elif dc == 1:
            src_cols, buf = pl.ds(cols - LANES, LANES), left
        else:
            src_cols, buf = pl.ds(0, LANES), right
        return pltpu.make_async_remote_copy(
            src_ref=main.at[pl.ds(first, many), src_rows, src_cols],
            dst_ref=buf.at[pl.ds(first, many), dst_rows, :],
            send_sem=halo_send.at[d, piece], recv_sem=halo_recv.at[d, piece],
            device_id=(gx + dr, gy + dc), device_id_type=MESH)

    def each_halo(near, act, back=False):
        for d, (dr, dc) in enumerate(DIRECTIONS):
            @pl.when(inside(-dr, -dc) if back else inside(dr, dc))
            def _():
                for piece in [0] if near else range(1, len(pieces(dr))):
                    act(halo(d, piece))

    each_halo(True, lambda copy: copy.start())
    for k in range(1, nx):
        pl.semaphore_signal(ready, inc=1, device_id=across(k), device_id_type=MESH)
    each_halo(False, lambda copy: copy.start())

    def shrink(x, start):
        sub = lax.broadcasted_iota(jnp.int32, (8, x.shape[1]), 0)
        ends = jnp.where(sub < 4, x[start + rows:start + rows + 8], x[start - 8:start])
        return jnp.concatenate([x[start:start + rows], ends], axis=0)

    def strip(a, begin, end):
        lane = lax.broadcasted_iota(jnp.int32, (end - begin, LANES), 1)
        edge = jnp.where(lane < half, right[a, begin:end], left[a, begin:end])
        return jnp.concatenate([main[a, begin:end], edge], axis=1)

    def field(a, window):
        if window == "tall":
            return strip(a, 0, tall)
        x = strip(a, low_mid, high_mid)
        return x if window == "mid" else shrink(x, 8)

    def up(x):
        return pltpu.roll(x, 1, 0)

    def down(x):
        return pltpu.roll(x, x.shape[0] - 1, 0)

    def before(x):
        return pltpu.roll(x, 1, 1)

    def after(x):
        return pltpu.roll(x, x.shape[1] - 1, 1)

    def masked(x, window):
        return jnp.where(scaled[window][...] > 0.0, x, 0.0)

    def core_of(window):
        return masked(SCALE * (field(1, window) + (inv_step + 4.0 - SHIFT)), window)

    def apply_b(v, core, window):
        beside = (up(v) + down(v)) + (before(v) + after(v))
        return core * v - scaled[window][...] * beside

    def apply_half(v, core):
        return (0.5 * core) * v - SCALE * (down(v) + after(v))

    def hamiltonian(u):
        dx = u - up(u)
        dy = u - before(u)
        px, qx = jnp.maximum(dx, 0.0), jnp.minimum(dx, 0.0)
        py, qy = jnp.maximum(dy, 0.0), jnp.minimum(dy, 0.0)
        return (px * px + down(qx * qx)) + (py * py + after(qy * qy))

    def faces(u):
        sx = u - down(u)
        sy = u - after(u)
        return jnp.maximum(sx, 0.0), jnp.minimum(sx, 0.0), jnp.maximum(sy, 0.0), jnp.minimum(sy, 0.0)

    def advance(m, face, window):
        px, qx, py, qy = face
        fx = px * m + qx * down(m)
        fy = py * m + qy * after(m)
        net = (fx - up(fx)) + (fy - before(fy))
        return scaled[window][...] * ((inv_step / SCALE) * m - (1.0 / SCALE) * net)

    def value_rhs(later, level, window):
        guess = masked(coupling * field(2 if level == 1 else 3, window), window)
        own_part = (inv_step / SCALE) * later - (0.5 / SCALE) * hamiltonian(later)
        return scaled[window][...] * own_part + guess

    def tree(parts):
        while len(parts) > 1:
            odd = parts[len(parts) // 2 * 2:]
            parts = [parts[i] + parts[i + 1] for i in range(0, len(parts) - 1, 2)] + odd
        return parts[0]

    def fold(p):
        return tree([p[i:i + 8, j:j + LANES] for i in range(0, rows, 8) for j in range(0, cols, LANES)])

    def dot(x, y):
        return fold(x * y)

    sub8 = lax.broadcasted_iota(jnp.int32, (8, LANES), 0)
    lane8 = lax.broadcasted_iota(jnp.int32, (8, LANES), 1)

    def pack(tiles):
        spread = None
        for first in range(0, len(tiles), 8):
            group = tiles[first:first + 8]
            group = group + [jnp.zeros((8, LANES), jnp.float32)] * (8 - len(group))
            for step in (4, 2, 1):
                keep = lax.rem(sub8, 2 * step) < step
                group = [
                    jnp.where(keep, a + pltpu.roll(a, 8 - step, 0), b + pltpu.roll(b, step, 0))
                    for a, b in zip(group[:step], group[step:])
                ]
            sums = jnp.sum(group[0], axis=1, keepdims=True)
            part = jnp.where(lane8 == sub8 + first, sums, 0.0)
            spread = part if spread is None else spread + part
        return jnp.sum(spread, axis=0, keepdims=True)

    def send_sums(which, values):
        packed = pack(values)
        sent[which] = packed
        slots[which, me] = packed

        def send(px, py):
            pltpu.make_async_remote_copy(
                src_ref=sent.at[which], dst_ref=slots.at[which, me],
                send_sem=sum_send.at[which], recv_sem=sum_recv.at[which],
                device_id=(px, py), device_id_type=MESH).start()

        def line(k, carry):
            px = lax.rem(gx + k, nx)
            for j in range(ny):
                send(px, jnp.where(2 * gy < ny, ny - 1 - j, j))
            return carry

        lax.fori_loop(1, nx, line, 0)
        for k in range(1, ny):
            send(gx, lax.rem(gy + k, ny))

    def take_sums(which, many):
        others = slots.at[which, pl.ds(0, count - 1)]
        pltpu.make_async_copy(others, others, sum_recv.at[which]).wait()
        total = jnp.broadcast_to(tree([slots[which, k] for k in range(count)]), (8, LANES))
        return [jnp.broadcast_to(total[:, k:k + 1], (8, LANES)) for k in range(many)]

    def basis(b, core, window, last=True):
        v1 = apply_b(b, core, window)
        v2 = apply_b(v1, core, window)
        return (b, v1, v2, apply_half(v2, core)) if last else (b, v1, v2)

    def spread(tile, like):
        wide_tile = jnp.concatenate([tile] * (like.shape[1] // LANES), axis=1)
        return jnp.concatenate([wide_tile] * (like.shape[0] // 8), axis=0)

    def mix(c, v):
        parts = [spread(a, x) * x for a, x in zip(c, v)]
        return (parts[0] + parts[1]) + parts[2]

    def pairs(x, y):
        return [dot(x[0], y[0]), dot(x[0], y[1]), dot(x[1], y[1]),
                dot(x[1], y[2]), dot(x[2], y[2]),
                2.0 * dot(x[2], x[3]) if x is y
                else fold(x[2] * y[3] + y[2] * x[3])]

    def own_small(v):
        return [x[:rows, :cols] for x in v]

    each_halo(True, lambda copy: copy.wait_recv(), back=True)
    small_core = core_of("small")
    later = masked(field(0, "small"), "small")
    w = own_small(basis(value_rhs(later, 1, "small"), small_core, "small"))
    moments = pairs(w, w)
    pl.semaphore_wait(ready, nx - 1)
    send_sums(0, moments)
    each_halo(False, lambda copy: copy.wait_recv(), back=True)
    core = core_of("tall")
    later = masked(field(0, "tall"), "tall")
    v = basis(value_rhs(later, 1, "tall"), core, "tall", last=False)
    vs = [shrink(x, MARGIN) for x in v]
    c = solve_small(take_sums(0, 6))

    first_small = mix(c, vs)
    w = own_small(basis(value_rhs(first_small, 0, "small"), small_core, "small"))
    send_sums(1, pairs(w, w))
    first = mix(c, v)
    v = basis(value_rhs(first, 0, "tall"), core, "tall", last=False)
    v = [x[low_mid:high_mid] for x in v]
    face = faces(first_small)
    density = masked(field(4, "mid"), "mid")
    mid_core = core_of("mid")
    c = solve_small(take_sums(1, 6))
    second = mix(c, v)

    a = basis(advance(density, faces(second), "mid"), mid_core, "mid", last=False)
    a = [shrink(x, 8) for x in a]
    last = apply_half(a[2], small_core)
    inner = own_small(a + [last])
    families = [
        own_small(basis(advance(a[i], face, "small"), small_core, "small")) for i in range(3)]
    moments = pairs(inner, inner)
    for i in range(3):
        for j in range(i, 3):
            moments += pairs(families[i], families[j])
    send_sums(2, moments)
    both_ref[0] = second[8:8 + rows, :cols]
    each_halo(True, lambda copy: copy.wait_send())
    each_halo(False, lambda copy: copy.wait_send())
    for which in range(3):
        others = slots.at[which, pl.ds(0, count - 1)]
        pltpu.make_async_copy(others, others, sum_send.at[which]).wait()
    total = take_sums(2, len(moments))
    c = solve_small(total[:6])
    picks = [(i, j) for i in range(3) for j in range(i, 3)]
    weights = [c[i] * c[j] * (1.0 if i == j else 2.0) for i, j in picks]
    nu = [
        tree([weight * total[6 + 6 * at + k] for at, weight in enumerate(weights)])
        for k in range(6)
    ]
    e = solve_small(nu)
    result = mix(e, [mix(c, [families[i][k] for i in range(3)]) for k in range(3)])
    both_ref[1] = result


def solution(mesh):
    nx, ny = mesh.shape["gx"], mesh.shape["gy"]

    def shards(terminal, initial_density, density_guess, diagonal):
        rows, cols = terminal.shape
        tall = rows + 2 * MARGIN
        hbm = pl.BlockSpec(memory_space=pl.ANY)
        vmem = pl.BlockSpec(memory_space=pltpu.VMEM)
        shape = jax.ShapeDtypeStruct((rows, cols), jnp.float32)
        both = pl.pallas_call(
            functools.partial(kernel, nx, ny),
            out_shape=jax.ShapeDtypeStruct((2, rows, cols), jnp.float32),
            in_specs=[hbm] * 4,
            out_specs=vmem,
            scratch_shapes=[
                pltpu.VMEM((5, tall, cols), jnp.float32),
                pltpu.VMEM((5, tall, LANES), jnp.float32),
                pltpu.VMEM((5, tall, LANES), jnp.float32),
                pltpu.VMEM((3, 1, LANES), jnp.float32),
                pltpu.VMEM((3, nx * ny, 1, LANES), jnp.float32),
                pltpu.SemaphoreType.DMA((8, 3)),
                pltpu.SemaphoreType.DMA((8, 3)),
                pltpu.SemaphoreType.DMA((5,)),
                pltpu.SemaphoreType.DMA((3,)),
                pltpu.SemaphoreType.DMA((3,)),
                pltpu.SemaphoreType.REGULAR,
                pltpu.VMEM((tall, cols + LANES), jnp.float32),
                pltpu.VMEM((rows + 16, cols + LANES), jnp.float32),
                pltpu.VMEM((rows + 8, cols + LANES), jnp.float32),
            ],
            compiler_params=pltpu.CompilerParams(collective_id=0, has_side_effects=True, vmem_limit_bytes=4 * 1024 * 1024),
        )(*[pltpu.with_memory_space_constraint(x, pltpu.HBM) for x in (terminal, initial_density, density_guess, diagonal)])
        return both[0], both[1]

    placed = (P("gx", "gy"), P("gx", "gy"), P(None, "gx", "gy"), P("gx", "gy"))
    return jax.shard_map(
        shards,
        mesh=mesh,
        in_specs=placed,
        out_specs=(P("gx", "gy"), P("gx", "gy")),
        check_vma=False,
    )
```

```python
import functools

import jax
import jax.numpy as jnp
from jax import lax
from jax.experimental import pallas as pl
from jax.experimental.pallas import tpu as pltpu
from jax.sharding import PartitionSpec as P

MESH = pl.DeviceIdType.MESH

LEVELS = 2
MARGIN = 16
LANES = 128

inv_step = 0.5
coupling = 0.5

SCALE = 0.25
SHIFT = 5.5

DIRECTIONS = [(r, c) for r in (-1, 0, 1) for c in (-1, 0, 1) if (r, c) != (0, 0)]
TINY = 2e-7


def solve_small(nu):
    g00 = nu[1] / SCALE + SHIFT * nu[0]
    g01 = nu[2] / SCALE + SHIFT * nu[1]
    g02 = nu[3] / SCALE + SHIFT * nu[2]
    g12 = nu[4] / SCALE + SHIFT * nu[3]
    g22 = nu[5] / SCALE + SHIFT * nu[4]
    g11 = g02
    inv0 = 1.0 / g00
    l10 = g01 * inv0
    l20 = g02 * inv0
    d1 = g11 - l10 * g01
    ok1 = d1 > TINY * g11
    inv1 = jnp.where(ok1, 1.0 / jnp.where(ok1, d1, 1.0), 0.0)
    t = g12 - l20 * g01
    l21 = t * inv1
    d2 = g22 - l20 * g02 - l21 * t
    ok2 = ok1 & (d2 > TINY * g22)
    inv2 = jnp.where(ok2, 1.0 / jnp.where(ok2, d2, 1.0), 0.0)
    y1 = nu[1] - l10 * nu[0]
    y2 = nu[2] - l20 * nu[0] - l21 * y1
    c2 = y2 * inv2
    c1 = y1 * inv1 - l21 * c2
    c0 = nu[0] * inv0 - l10 * c1 - l20 * c2
    return c0, c1, c2


def kernel(nx, ny, term_ref, dens_ref, guess_ref, diag_ref, both_ref,
           main, left, right, sent, slots, sizes, halo_send, halo_recv, own_sem, sum_send, sum_recv,
           ready, scaled_tall, scaled_mid, scaled_small):
    rows, cols = term_ref.shape
    gx = lax.axis_index("gx")
    gy = lax.axis_index("gy")
    count = nx * ny
    me = gx * ny + gy

    def inside(dr, dc):
        ok = None
        for here_at, step, size in ((gx, dr, nx), (gy, dc, ny)):
            if step == 1:
                test = here_at < size - 1
            elif step == -1:
                test = here_at > 0
            else:
                continue
            ok = test if ok is None else ok & test
        return ok

    def across(k):
        return (lax.rem(gx + k, nx), gy)

    def along(k):
        return (gx, lax.rem(gy + k, ny))

    barrier = pltpu.get_barrier_semaphore()
    greeted = nx + ny - 2
    for k in range(1, nx):
        pl.semaphore_signal(barrier, inc=1, device_id=across(k), device_id_type=MESH)
    for k in range(1, ny):
        pl.semaphore_signal(barrier, inc=1, device_id=along(k), device_id_type=MESH)
    for dr, dc in DIRECTIONS:
        if dr != 0 and dc != 0:
            there = inside(dr, dc)
            greeted = greeted + jnp.where(there, 1, 0)

            @pl.when(there)
            def _():
                pl.semaphore_signal(
                    barrier, inc=1, device_id=(gx + dr, gy + dc), device_id_type=MESH)

    here = pl.ds(MARGIN, rows)
    own = [
        pltpu.make_async_copy(source, main.at[at, here], own_sem)
        for at, source in enumerate(
            (term_ref, diag_ref, guess_ref.at[1], guess_ref.at[0], dens_ref))
    ]
    for copy in own:
        copy.start()
    wide = cols + LANES
    half = LANES // 2
    tall = rows + 2 * MARGIN
    low_mid, high_mid = MARGIN - 8, MARGIN + rows + 8

    def mask_of(size, cyclic, margin):
        row = lax.broadcasted_iota(jnp.int32, (size, wide), 0)
        col = lax.broadcasted_iota(jnp.int32, (size, wide), 1)
        col_low = jnp.where(gy < ny - 1, cols + half, cols)
        col_high = jnp.where(gy > 0, cols + half, wide)
        ok = (col < col_low) | (col >= col_high)
        if cyclic:
            row_low = jnp.where(gx < nx - 1, rows + 4, rows)
            row_high = jnp.where(gx > 0, rows + 4, size)
            return ok & ((row < row_low) | (row >= row_high))
        row_low = jnp.where(gx > 0, 0, margin)
        row_high = jnp.where(gx < nx - 1, size, margin + rows)
        return ok & (row >= row_low) & (row < row_high)

    scaled = {"tall": scaled_tall, "mid": scaled_mid, "small": scaled_small}
    scaled_tall[...] = jnp.where(mask_of(tall, False, MARGIN), SCALE, 0.0)
    scaled_mid[...] = jnp.where(mask_of(rows + 16, False, 8), SCALE, 0.0)
    scaled_small[...] = jnp.where(mask_of(rows + 8, True, 4), SCALE, 0.0)

    pltpu.make_async_copy(main.at[:, here], main.at[:, here], own_sem).wait()
    pl.semaphore_wait(barrier, greeted)

    def pieces(dr):
        if dr == 0:
            return [(0, 3, 0, rows), (3, 2, 0, rows)]
        return [(0, 3, 0, 8), (0, 4, 8, 8), (3, 2, 0, 8)]

    def halo(d, piece):
        dr, dc = DIRECTIONS[d]
        first, many, out, size = pieces(dr)[piece]
        if dr == 0:
            src_rows, dst_rows = here, here
        elif dr == 1:
            src_rows = pl.ds(MARGIN + rows - out - size, size)
            dst_rows = pl.ds(MARGIN - out - size, size)
        else:
            src_rows = pl.ds(MARGIN + out, size)
            dst_rows = pl.ds(MARGIN + rows + out, size)
        if dc == 0:
            src_cols, buf = pl.ds(0, cols), main
        elif dc == 1:
            src_cols, buf = pl.ds(cols - LANES, LANES), left
        else:
            src_cols, buf = pl.ds(0, LANES), right
        return pltpu.make_async_remote_copy(
            src_ref=main.at[pl.ds(first, many), src_rows, src_cols],
            dst_ref=buf.at[pl.ds(first, many), dst_rows, :],
            send_sem=halo_send, recv_sem=halo_recv.at[0 if piece == 0 else 1],
            device_id=(gx + dr, gy + dc), device_id_type=MESH)

    def start_halo(near):
        for d, (dr, dc) in enumerate(DIRECTIONS):
            @pl.when(inside(dr, dc))
            def _():
                for piece in [0] if near else range(1, len(pieces(dr))):
                    halo(d, piece).start()

    def tiles(ends, sides, near):
        total = 0
        for dr, dc in ((1, 0), (0, 1), (1, 1)):
            times = (ends if dr else 1) * (sides if dc else 1)
            for at, (_, many, _, size) in enumerate(pieces(dr)):
                if near is None or (at == 0) == near:
                    total += times * many * (size // 8) * (1 if dc else cols // LANES)
        return total

    def beside_count(here_at, size):
        return jnp.where(here_at > 0, 1, 0) + jnp.where(here_at < size - 1, 1, 0)

    def wait_halo(sem, near):
        for ends in range(min(1, nx - 1), min(2, nx - 1) + 1):
            for sides in range(min(1, ny - 1), min(2, ny - 1) + 1):
                many = tiles(ends, sides, near)
                if many == 0:
                    continue

                @pl.when((beside_count(gx, nx) == ends) & (beside_count(gy, ny) == sides))
                def _():
                    span = sizes.at[pl.ds(0, many)]
                    pltpu.make_async_copy(span, span, sem).wait()

    start_halo(True)
    for k in range(1, nx):
        pl.semaphore_signal(ready, inc=1, device_id=across(k), device_id_type=MESH)
    start_halo(False)

    def shrink(x, start):
        sub = lax.broadcasted_iota(jnp.int32, (8, x.shape[1]), 0)
        ends = jnp.where(sub < 4, x[start + rows:start + rows + 8], x[start - 8:start])
        return jnp.concatenate([x[start:start + rows], ends], axis=0)

    def strip(a, begin, end):
        lane = lax.broadcasted_iota(jnp.int32, (end - begin, LANES), 1)
        edge = jnp.where(lane < half, right[a, begin:end], left[a, begin:end])
        return jnp.concatenate([main[a, begin:end], edge], axis=1)

    def field(a, window):
        if window == "tall":
            return strip(a, 0, tall)
        x = strip(a, low_mid, high_mid)
        return x if window == "mid" else shrink(x, 8)

    def up(x):
        return pltpu.roll(x, 1, 0)

    def down(x):
        return pltpu.roll(x, x.shape[0] - 1, 0)

    def before(x):
        return pltpu.roll(x, 1, 1)

    def after(x):
        return pltpu.roll(x, x.shape[1] - 1, 1)

    def masked(x, window):
        return jnp.where(scaled[window][...] > 0.0, x, 0.0)

    def core_of(window):
        return masked(SCALE * (field(1, window) + (inv_step + 4.0 - SHIFT)), window)

    def apply_b(v, core, window):
        beside = (up(v) + down(v)) + (before(v) + after(v))
        return core * v - scaled[window][...] * beside

    def apply_half(v, core):
        return (0.5 * core) * v - SCALE * (down(v) + after(v))

    def hamiltonian(u):
        dx = u - up(u)
        dy = u - before(u)
        px, qx = jnp.maximum(dx, 0.0), jnp.minimum(dx, 0.0)
        py, qy = jnp.maximum(dy, 0.0), jnp.minimum(dy, 0.0)
        return (px * px + down(qx * qx)) + (py * py + after(qy * qy))

    def faces(u):
        sx = u - down(u)
        sy = u - after(u)
        return jnp.maximum(sx, 0.0), jnp.minimum(sx, 0.0), jnp.maximum(sy, 0.0), jnp.minimum(sy, 0.0)

    def advance(m, face, window):
        px, qx, py, qy = face
        fx = px * m + qx * down(m)
        fy = py * m + qy * after(m)
        net = (fx - up(fx)) + (fy - before(fy))
        return scaled[window][...] * ((inv_step / SCALE) * m - (1.0 / SCALE) * net)

    def value_rhs(later, level, window):
        guess = masked(coupling * field(2 if level == 1 else 3, window), window)
        own_part = (inv_step / SCALE) * later - (0.5 / SCALE) * hamiltonian(later)
        return scaled[window][...] * own_part + guess

    def tree(parts):
        while len(parts) > 1:
            odd = parts[len(parts) // 2 * 2:]
            parts = [parts[i] + parts[i + 1] for i in range(0, len(parts) - 1, 2)] + odd
        return parts[0]

    def fold(p):
        return tree([p[i:i + 8, j:j + LANES] for i in range(0, rows, 8) for j in range(0, cols, LANES)])

    def dot(x, y):
        return fold(x * y)

    sub8 = lax.broadcasted_iota(jnp.int32, (8, LANES), 0)
    lane8 = lax.broadcasted_iota(jnp.int32, (8, LANES), 1)

    def pack(tiles):
        spread = None
        for first in range(0, len(tiles), 8):
            group = tiles[first:first + 8]
            group = group + [jnp.zeros((8, LANES), jnp.float32)] * (8 - len(group))
            for step in (4, 2, 1):
                keep = lax.rem(sub8, 2 * step) < step
                group = [
                    jnp.where(keep, a + pltpu.roll(a, 8 - step, 0), b + pltpu.roll(b, step, 0))
                    for a, b in zip(group[:step], group[step:])
                ]
            sums = jnp.sum(group[0], axis=1, keepdims=True)
            part = jnp.where(lane8 == sub8 + first, sums, 0.0)
            spread = part if spread is None else spread + part
        return jnp.sum(spread, axis=0, keepdims=True)

    def send_sums(which, values):
        packed = pack(values)
        sent[which] = packed
        slots[which, me] = packed

        def send(px, py):
            pltpu.make_async_remote_copy(
                src_ref=sent.at[which], dst_ref=slots.at[which, me],
                send_sem=sum_send, recv_sem=sum_recv.at[which % 2],
                device_id=(px, py), device_id_type=MESH).start()

        def line(k, carry):
            px = lax.rem(gx + k, nx)
            for j in range(ny):
                send(px, jnp.where(2 * gy < ny, ny - 1 - j, j))
            return carry

        lax.fori_loop(1, nx, line, 0)
        for k in range(1, ny):
            send(gx, lax.rem(gy + k, ny))

    def take_sums(which, many):
        others = slots.at[which, pl.ds(0, count - 1)]
        pltpu.make_async_copy(others, others, sum_recv.at[which % 2]).wait()
        total = jnp.broadcast_to(tree([slots[which, k] for k in range(count)]), (8, LANES))
        return [jnp.broadcast_to(total[:, k:k + 1], (8, LANES)) for k in range(many)]

    def basis(b, core, window, last=True):
        v1 = apply_b(b, core, window)
        v2 = apply_b(v1, core, window)
        return (b, v1, v2, apply_half(v2, core)) if last else (b, v1, v2)

    def spread(tile, like):
        wide_tile = jnp.concatenate([tile] * (like.shape[1] // LANES), axis=1)
        return jnp.concatenate([wide_tile] * (like.shape[0] // 8), axis=0)

    def mix(c, v):
        parts = [spread(a, x) * x for a, x in zip(c, v)]
        return (parts[0] + parts[1]) + parts[2]

    def pairs(x, y):
        return [dot(x[0], y[0]), dot(x[0], y[1]), dot(x[1], y[1]),
                dot(x[1], y[2]), dot(x[2], y[2]),
                2.0 * dot(x[2], x[3]) if x is y
                else fold(x[2] * y[3] + y[2] * x[3])]

    def own_small(v):
        return [x[:rows, :cols] for x in v]

    wait_halo(halo_recv.at[0], True)
    small_core = core_of("small")
    later = masked(field(0, "small"), "small")
    w = own_small(basis(value_rhs(later, 1, "small"), small_core, "small"))
    moments = pairs(w, w)
    pl.semaphore_wait(ready, nx - 1)
    send_sums(0, moments)
    wait_halo(halo_recv.at[1], False)
    core = core_of("tall")
    later = masked(field(0, "tall"), "tall")
    v = basis(value_rhs(later, 1, "tall"), core, "tall", last=False)
    vs = [shrink(x, MARGIN) for x in v]
    c = solve_small(take_sums(0, 6))

    first_small = mix(c, vs)
    w = own_small(basis(value_rhs(first_small, 0, "small"), small_core, "small"))
    send_sums(1, pairs(w, w))
    first = mix(c, v)
    v = basis(value_rhs(first, 0, "tall"), core, "tall", last=False)
    v = [x[low_mid:high_mid] for x in v]
    face = faces(first_small)
    density = masked(field(4, "mid"), "mid")
    mid_core = core_of("mid")
    c = solve_small(take_sums(1, 6))
    second = mix(c, v)

    a = basis(advance(density, faces(second), "mid"), mid_core, "mid", last=False)
    a = [shrink(x, 8) for x in a]
    last = apply_half(a[2], small_core)
    inner = own_small(a + [last])
    families = [
        own_small(basis(advance(a[i], face, "small"), small_core, "small")) for i in range(3)]
    moments = pairs(inner, inner)
    for i in range(3):
        for j in range(i, 3):
            moments += pairs(families[i], families[j])
    send_sums(2, moments)
    both_ref[0] = second[8:8 + rows, :cols]
    wait_halo(halo_send, None)
    others = slots.at[:, pl.ds(0, count - 1)]
    pltpu.make_async_copy(others, others, sum_send).wait()
    total = take_sums(2, len(moments))
    c = solve_small(total[:6])
    picks = [(i, j) for i in range(3) for j in range(i, 3)]
    weights = [c[i] * c[j] * (1.0 if i == j else 2.0) for i, j in picks]
    nu = [
        tree([weight * total[6 + 6 * at + k] for at, weight in enumerate(weights)])
        for k in range(6)
    ]
    e = solve_small(nu)
    result = mix(e, [mix(c, [families[i][k] for i in range(3)]) for k in range(3)])
    both_ref[1] = result


def solution(mesh):
    nx, ny = mesh.shape["gx"], mesh.shape["gy"]

    def shards(terminal, initial_density, density_guess, diagonal):
        rows, cols = terminal.shape
        tall = rows + 2 * MARGIN
        hbm = pl.BlockSpec(memory_space=pl.ANY)
        vmem = pl.BlockSpec(memory_space=pltpu.VMEM)
        shape = jax.ShapeDtypeStruct((rows, cols), jnp.float32)
        both = pl.pallas_call(
            functools.partial(kernel, nx, ny),
            out_shape=jax.ShapeDtypeStruct((2, rows, cols), jnp.float32),
            in_specs=[hbm] * 4,
            out_specs=vmem,
            scratch_shapes=[
                pltpu.VMEM((5, tall, cols), jnp.float32),
                pltpu.VMEM((5, tall, LANES), jnp.float32),
                pltpu.VMEM((5, tall, LANES), jnp.float32),
                pltpu.VMEM((3, 1, LANES), jnp.float32),
                pltpu.VMEM((3, nx * ny, 1, LANES), jnp.float32),
                pltpu.VMEM((5 * 4 * (rows // 8 + 2) * (cols // LANES + 2), 8, LANES), jnp.float32),
                pltpu.SemaphoreType.DMA,
                pltpu.SemaphoreType.DMA((2,)),
                pltpu.SemaphoreType.DMA,
                pltpu.SemaphoreType.DMA,
                pltpu.SemaphoreType.DMA((2,)),
                pltpu.SemaphoreType.REGULAR,
                pltpu.VMEM((tall, cols + LANES), jnp.float32),
                pltpu.VMEM((rows + 16, cols + LANES), jnp.float32),
                pltpu.VMEM((rows + 8, cols + LANES), jnp.float32),
            ],
            compiler_params=pltpu.CompilerParams(collective_id=0, has_side_effects=True, vmem_limit_bytes=4 * 1024 * 1024),
        )(*[pltpu.with_memory_space_constraint(x, pltpu.HBM) for x in (terminal, initial_density, density_guess, diagonal)])
        return both[0], both[1]

    placed = (P("gx", "gy"), P("gx", "gy"), P(None, "gx", "gy"), P("gx", "gy"))
    return jax.shard_map(
        shards,
        mesh=mesh,
        in_specs=placed,
        out_specs=(P("gx", "gy"), P("gx", "gy")),
        check_vma=False,
    )
```

```python
import functools

import jax
import jax.numpy as jnp
from jax import lax
from jax.experimental import pallas as pl
from jax.experimental.pallas import tpu as pltpu
from jax.sharding import PartitionSpec as P

MESH = pl.DeviceIdType.MESH

LEVELS = 2
MARGIN = 16
LANES = 128

inv_step = 0.5
coupling = 0.5

SCALE = 0.25
SHIFT = 5.5

DIRECTIONS = [(r, c) for r in (-1, 1) for c in (-1, 1)] + [(-1, 0), (1, 0), (0, -1), (0, 1)]
TINY = 2e-7


def solve_small(nu):
    g00 = nu[1] / SCALE + SHIFT * nu[0]
    g01 = nu[2] / SCALE + SHIFT * nu[1]
    g02 = nu[3] / SCALE + SHIFT * nu[2]
    g12 = nu[4] / SCALE + SHIFT * nu[3]
    g22 = nu[5] / SCALE + SHIFT * nu[4]
    g11 = g02
    inv0 = 1.0 / g00
    l10 = g01 * inv0
    l20 = g02 * inv0
    d1 = g11 - l10 * g01
    ok1 = d1 > TINY * g11
    inv1 = jnp.where(ok1, 1.0 / jnp.where(ok1, d1, 1.0), 0.0)
    t = g12 - l20 * g01
    l21 = t * inv1
    d2 = g22 - l20 * g02 - l21 * t
    ok2 = ok1 & (d2 > TINY * g22)
    inv2 = jnp.where(ok2, 1.0 / jnp.where(ok2, d2, 1.0), 0.0)
    y1 = nu[1] - l10 * nu[0]
    y2 = nu[2] - l20 * nu[0] - l21 * y1
    c2 = y2 * inv2
    c1 = y1 * inv1 - l21 * c2
    c0 = nu[0] * inv0 - l10 * c1 - l20 * c2
    return c0, c1, c2


def kernel(nx, ny, term_ref, dens_ref, guess_ref, diag_ref, both_ref,
           main, left, right, rim, edge, edge_left, edge_right, sent, slots, sizes, halo_send, halo_recv, own_sem, sum_send, sum_recv,
           ready, scaled_tall, scaled_mid, scaled_small):
    rows, cols = term_ref.shape
    gx = lax.axis_index("gx")
    gy = lax.axis_index("gy")
    count = nx * ny
    me = gx * ny + gy

    def inside(dr, dc):
        ok = None
        for here_at, step, size in ((gx, dr, nx), (gy, dc, ny)):
            if step == 1:
                test = here_at < size - 1
            elif step == -1:
                test = here_at > 0
            else:
                continue
            ok = test if ok is None else ok & test
        return ok

    def across(k):
        return (lax.rem(gx + k, nx), gy)

    def along(k):
        return (gx, lax.rem(gy + k, ny))

    barrier = pltpu.get_barrier_semaphore()
    greeted = nx + ny - 2
    for dr, dc in DIRECTIONS:
        if dr != 0 and dc != 0:
            there = inside(dr, dc)
            greeted = greeted + jnp.where(there, 1, 0)

            @pl.when(there)
            def _():
                pl.semaphore_signal(
                    barrier, inc=1, device_id=(gx + dr, gy + dc), device_id_type=MESH)

    for k in range(1, nx):
        pl.semaphore_signal(barrier, inc=1, device_id=across(k), device_id_type=MESH)
    for k in range(1, ny):
        pl.semaphore_signal(barrier, inc=1, device_id=along(k), device_id_type=MESH)

    here = pl.ds(MARGIN, rows)
    own = [
        pltpu.make_async_copy(source, main.at[at, here], own_sem)
        for at, source in enumerate(
            (term_ref, diag_ref, guess_ref.at[1], guess_ref.at[0], dens_ref))
    ]
    for copy in own:
        copy.start()
    wide = cols + LANES
    half = LANES // 2
    tall = rows + 2 * MARGIN
    low_mid, high_mid = MARGIN - 8, MARGIN + rows + 8

    def mask_of(size, cyclic, margin):
        row = lax.broadcasted_iota(jnp.int32, (size, wide), 0)
        col = lax.broadcasted_iota(jnp.int32, (size, wide), 1)
        col_low = jnp.where(gy < ny - 1, cols + half, cols)
        col_high = jnp.where(gy > 0, cols + half, wide)
        ok = (col < col_low) | (col >= col_high)
        if cyclic:
            row_low = jnp.where(gx < nx - 1, rows + 4, rows)
            row_high = jnp.where(gx > 0, rows + 4, size)
            return ok & ((row < row_low) | (row >= row_high))
        row_low = jnp.where(gx > 0, 0, margin)
        row_high = jnp.where(gx < nx - 1, size, margin + rows)
        return ok & (row >= row_low) & (row < row_high)

    scaled = {"tall": scaled_tall, "mid": scaled_mid, "small": scaled_small}
    scaled_tall[...] = jnp.where(mask_of(tall, False, MARGIN), SCALE, 0.0)
    scaled_mid[...] = jnp.where(mask_of(rows + 16, False, 8), SCALE, 0.0)
    scaled_small[...] = jnp.where(mask_of(rows + 8, True, 4), SCALE, 0.0)

    pltpu.make_async_copy(main.at[:, here], main.at[:, here], own_sem).wait()
    for part in range(2):
        for a in range(3):
            rim[part, 0, a] = main[a, MARGIN + 4 * part:MARGIN + 4 * part + 4]
            rim[part, 1, a] = main[a, MARGIN + rows - 4 * part - 4:MARGIN + rows - 4 * part]
    pl.semaphore_wait(barrier, greeted)

    def pieces(dr):
        if dr == 0:
            return [(0, 3, 0, rows), (3, 2, 0, rows)]
        return [(0, 3, 0, 4), (0, 3, 4, 4), (0, 4, 8, 8), (3, 2, 0, 8)]

    def halo(d, piece):
        dr, dc = DIRECTIONS[d]
        first, many, out, size = pieces(dr)[piece]
        if dr == 0:
            src_rows, dst_rows = here, here
        elif dr == 1:
            src_rows = pl.ds(MARGIN + rows - out - size, size)
            dst_rows = pl.ds(MARGIN - out - size, size)
        else:
            src_rows = pl.ds(MARGIN + out, size)
            dst_rows = pl.ds(MARGIN + rows + out, size)
        if dc == 0:
            src_cols, buf, rim_buf = pl.ds(0, cols), main, edge
        elif dc == 1:
            src_cols, buf, rim_buf = pl.ds(cols - LANES, LANES), left, edge_left
        else:
            src_cols, buf, rim_buf = pl.ds(0, LANES), right, edge_right
        src, dst = main.at[pl.ds(first, many), src_rows, src_cols], buf.at[pl.ds(first, many), dst_rows, :]
        if size == 4:
            src = rim.at[out // 4, 1 if dr == 1 else 0, :, :, src_cols]
            dst = rim_buf.at[out // 4, 1 if dr == 1 else 0]
        return pltpu.make_async_remote_copy(
            src_ref=src, dst_ref=dst,
            send_sem=halo_send, recv_sem=halo_recv.at[0 if piece == 0 else 1],
            device_id=(gx + dr, gy + dc), device_id_type=MESH)

    def start_halo(near):
        for d, (dr, dc) in enumerate(DIRECTIONS):
            @pl.when(inside(dr, dc))
            def _():
                for piece in [0] if near else range(1, len(pieces(dr))):
                    halo(d, piece).start()

    def tiles(ends, sides, near):
        total = 0
        for dr, dc in ((1, 0), (0, 1), (1, 1)):
            times = (ends if dr else 1) * (sides if dc else 1)
            for at, (_, many, _, size) in enumerate(pieces(dr)):
                if near is None or (at == 0) == near:
                    total += times * many * (size // 4) * (1 if dc else cols // LANES)
        return total

    def beside_count(here_at, size):
        return jnp.where(here_at > 0, 1, 0) + jnp.where(here_at < size - 1, 1, 0)

    def wait_halo(sem, near):
        for ends in range(min(1, nx - 1), min(2, nx - 1) + 1):
            for sides in range(min(1, ny - 1), min(2, ny - 1) + 1):
                many = tiles(ends, sides, near)
                if many == 0:
                    continue

                @pl.when((beside_count(gx, nx) == ends) & (beside_count(gy, ny) == sides))
                def _():
                    span = sizes.at[pl.ds(0, many)]
                    pltpu.make_async_copy(span, span, sem).wait()

    start_halo(True)
    for k in range(1, nx):
        pl.semaphore_signal(ready, inc=1, device_id=across(k), device_id_type=MESH)
    start_halo(False)

    def shrink(x, start):
        sub = lax.broadcasted_iota(jnp.int32, (8, x.shape[1]), 0)
        ends = jnp.where(sub < 4, x[start + rows:start + rows + 8], x[start - 8:start])
        return jnp.concatenate([x[start:start + rows], ends], axis=0)

    def joined(x, from_right, from_left):
        lane = lax.broadcasted_iota(jnp.int32, from_right.shape, 1)
        return jnp.concatenate([x, jnp.where(lane < half, from_right, from_left)], axis=1)

    def strip(a, begin, end):
        return joined(main[a, begin:end], right[a, begin:end], left[a, begin:end])

    def rims(a, one, other):
        return joined(*(
            jnp.concatenate([buf[part, side, a] for part, side in (one, other)], axis=0)
            for buf in (edge, edge_right, edge_left)))

    def field(a, window):
        if a > 2:
            if window == "tall":
                return strip(a, 0, tall)
            x = strip(a, low_mid, high_mid)
            return x if window == "mid" else shrink(x, 8)
        own_rows = strip(a, MARGIN, MARGIN + rows)
        if window == "small":
            return jnp.concatenate([own_rows, rims(a, (0, 0), (0, 1))], axis=0)
        above, below = rims(a, (1, 1), (0, 1)), rims(a, (0, 0), (1, 0))
        x = [above, own_rows, below]
        if window == "tall":
            x = [strip(a, 0, low_mid)] + x + [strip(a, high_mid, tall)]
        return jnp.concatenate(x, axis=0)

    def up(x):
        return pltpu.roll(x, 1, 0)

    def down(x):
        return pltpu.roll(x, x.shape[0] - 1, 0)

    def before(x):
        return pltpu.roll(x, 1, 1)

    def after(x):
        return pltpu.roll(x, x.shape[1] - 1, 1)

    def masked(x, window):
        return jnp.where(scaled[window][...] > 0.0, x, 0.0)

    def core_of(window):
        return masked(SCALE * (field(1, window) + (inv_step + 4.0 - SHIFT)), window)

    def apply_b(v, core, window):
        beside = (up(v) + down(v)) + (before(v) + after(v))
        return core * v - scaled[window][...] * beside

    def apply_half(v, core):
        return (0.5 * core) * v - SCALE * (down(v) + after(v))

    def hamiltonian(u):
        dx = u - up(u)
        dy = u - before(u)
        px, qx = jnp.maximum(dx, 0.0), jnp.minimum(dx, 0.0)
        py, qy = jnp.maximum(dy, 0.0), jnp.minimum(dy, 0.0)
        return (px * px + down(qx * qx)) + (py * py + after(qy * qy))

    def faces(u):
        sx = u - down(u)
        sy = u - after(u)
        return jnp.maximum(sx, 0.0), jnp.minimum(sx, 0.0), jnp.maximum(sy, 0.0), jnp.minimum(sy, 0.0)

    def advance(m, face, window):
        px, qx, py, qy = face
        fx = px * m + qx * down(m)
        fy = py * m + qy * after(m)
        net = (fx - up(fx)) + (fy - before(fy))
        return scaled[window][...] * ((inv_step / SCALE) * m - (1.0 / SCALE) * net)

    def value_rhs(later, level, window):
        guess = masked(coupling * field(2 if level == 1 else 3, window), window)
        own_part = (inv_step / SCALE) * later - (0.5 / SCALE) * hamiltonian(later)
        return scaled[window][...] * own_part + guess

    def tree(parts):
        while len(parts) > 1:
            odd = parts[len(parts) // 2 * 2:]
            parts = [parts[i] + parts[i + 1] for i in range(0, len(parts) - 1, 2)] + odd
        return parts[0]

    def fold(p):
        return tree([p[i:i + 8, j:j + LANES] for i in range(0, rows, 8) for j in range(0, cols, LANES)])

    def dot(x, y):
        return fold(x * y)

    sub8 = lax.broadcasted_iota(jnp.int32, (8, LANES), 0)
    lane8 = lax.broadcasted_iota(jnp.int32, (8, LANES), 1)

    def pack(tiles):
        spread = None
        for first in range(0, len(tiles), 8):
            group = tiles[first:first + 8]
            group = group + [jnp.zeros((8, LANES), jnp.float32)] * (8 - len(group))
            for step in (4, 2, 1):
                keep = lax.rem(sub8, 2 * step) < step
                group = [
                    jnp.where(keep, a + pltpu.roll(a, 8 - step, 0), b + pltpu.roll(b, step, 0))
                    for a, b in zip(group[:step], group[step:])
                ]
            sums = jnp.sum(group[0], axis=1, keepdims=True)
            part = jnp.where(lane8 == sub8 + first, sums, 0.0)
            spread = part if spread is None else spread + part
        return jnp.sum(spread, axis=0, keepdims=True)

    def send_sums(which, values):
        packed = pack(values)
        sent[which] = packed
        slots[which, me] = packed

        def send(px, py):
            pltpu.make_async_remote_copy(
                src_ref=sent.at[which], dst_ref=slots.at[which, me],
                send_sem=sum_send, recv_sem=sum_recv.at[which % 2],
                device_id=(px, py), device_id_type=MESH).start()

        def line(k, carry):
            px = lax.rem(gx + k, nx)
            for j in range(ny):
                send(px, jnp.where(2 * gy < ny, ny - 1 - j, j))
            return carry

        lax.fori_loop(1, nx, line, 0)
        for k in range(1, ny):
            send(gx, lax.rem(gy + k, ny))

    def take_sums(which, many):
        others = slots.at[which, pl.ds(0, count - 1)]
        pltpu.make_async_copy(others, others, sum_recv.at[which % 2]).wait()
        total = jnp.broadcast_to(tree([slots[which, k] for k in range(count)]), (8, LANES))
        return [jnp.broadcast_to(total[:, k:k + 1], (8, LANES)) for k in range(many)]

    def basis(b, core, window, last=True):
        v1 = apply_b(b, core, window)
        v2 = apply_b(v1, core, window)
        return (b, v1, v2, apply_half(v2, core)) if last else (b, v1, v2)

    def spread(tile, like):
        wide_tile = jnp.concatenate([tile] * (like.shape[1] // LANES), axis=1)
        return jnp.concatenate([wide_tile] * (like.shape[0] // 8), axis=0)

    def mix(c, v):
        parts = [spread(a, x) * x for a, x in zip(c, v)]
        return (parts[0] + parts[1]) + parts[2]

    def pairs(x, y):
        return [dot(x[0], y[0]), dot(x[0], y[1]), dot(x[1], y[1]),
                dot(x[1], y[2]), dot(x[2], y[2]),
                2.0 * dot(x[2], x[3]) if x is y
                else fold(x[2] * y[3] + y[2] * x[3])]

    def own_small(v):
        return [x[:rows, :cols] for x in v]

    wait_halo(halo_recv.at[0], True)
    small_core = core_of("small")
    later = masked(field(0, "small"), "small")
    w = own_small(basis(value_rhs(later, 1, "small"), small_core, "small"))
    moments = pairs(w, w)
    pl.semaphore_wait(ready, nx - 1)
    send_sums(0, moments)
    wait_halo(halo_recv.at[1], False)
    core = core_of("tall")
    later = masked(field(0, "tall"), "tall")
    v = basis(value_rhs(later, 1, "tall"), core, "tall", last=False)
    vs = [shrink(x, MARGIN) for x in v]
    c = solve_small(take_sums(0, 6))

    first_small = mix(c, vs)
    w = own_small(basis(value_rhs(first_small, 0, "small"), small_core, "small"))
    send_sums(1, pairs(w, w))
    first = mix(c, v)
    v = basis(value_rhs(first, 0, "tall"), core, "tall", last=False)
    v = [x[low_mid:high_mid] for x in v]
    face = faces(first_small)
    density = masked(field(4, "mid"), "mid")
    mid_core = core_of("mid")
    c = solve_small(take_sums(1, 6))
    second = mix(c, v)

    a = basis(advance(density, faces(second), "mid"), mid_core, "mid", last=False)
    a = [shrink(x, 8) for x in a]
    last = apply_half(a[2], small_core)
    inner = own_small(a + [last])
    families = [
        own_small(basis(advance(a[i], face, "small"), small_core, "small")) for i in range(3)]
    moments = pairs(inner, inner)
    for i in range(3):
        for j in range(i, 3):
            moments += pairs(families[i], families[j])
    send_sums(2, moments)
    both_ref[0] = second[8:8 + rows, :cols]
    wait_halo(halo_send, None)
    others = slots.at[:, pl.ds(0, count - 1)]
    pltpu.make_async_copy(others, others, sum_send).wait()
    total = take_sums(2, len(moments))
    c = solve_small(total[:6])
    picks = [(i, j) for i in range(3) for j in range(i, 3)]
    weights = [c[i] * c[j] * (1.0 if i == j else 2.0) for i, j in picks]
    nu = [
        tree([weight * total[6 + 6 * at + k] for at, weight in enumerate(weights)])
        for k in range(6)
    ]
    e = solve_small(nu)
    result = mix(e, [mix(c, [families[i][k] for i in range(3)]) for k in range(3)])
    both_ref[1] = result


def solution(mesh):
    nx, ny = mesh.shape["gx"], mesh.shape["gy"]

    def shards(terminal, initial_density, density_guess, diagonal):
        rows, cols = terminal.shape
        tall = rows + 2 * MARGIN
        hbm = pl.BlockSpec(memory_space=pl.ANY)
        vmem = pl.BlockSpec(memory_space=pltpu.VMEM)
        shape = jax.ShapeDtypeStruct((rows, cols), jnp.float32)
        both = pl.pallas_call(
            functools.partial(kernel, nx, ny),
            out_shape=jax.ShapeDtypeStruct((2, rows, cols), jnp.float32),
            in_specs=[hbm] * 4,
            out_specs=vmem,
            scratch_shapes=[
                pltpu.VMEM((5, tall, cols), jnp.float32),
                pltpu.VMEM((5, tall, LANES), jnp.float32),
                pltpu.VMEM((5, tall, LANES), jnp.float32),
                pltpu.VMEM((2, 2, 3, 4, cols), jnp.float32),
                pltpu.VMEM((2, 2, 3, 4, cols), jnp.float32),
                pltpu.VMEM((2, 2, 3, 4, LANES), jnp.float32),
                pltpu.VMEM((2, 2, 3, 4, LANES), jnp.float32),
                pltpu.VMEM((3, 1, LANES), jnp.float32),
                pltpu.VMEM((3, nx * ny, 1, LANES), jnp.float32),
                pltpu.VMEM((10 * 4 * (rows // 8 + 2) * (cols // LANES + 2), 4, LANES), jnp.float32),
                pltpu.SemaphoreType.DMA,
                pltpu.SemaphoreType.DMA((2,)),
                pltpu.SemaphoreType.DMA,
                pltpu.SemaphoreType.DMA,
                pltpu.SemaphoreType.DMA((2,)),
                pltpu.SemaphoreType.REGULAR,
                pltpu.VMEM((tall, cols + LANES), jnp.float32),
                pltpu.VMEM((rows + 16, cols + LANES), jnp.float32),
                pltpu.VMEM((rows + 8, cols + LANES), jnp.float32),
            ],
            compiler_params=pltpu.CompilerParams(collective_id=0, has_side_effects=True, vmem_limit_bytes=4 * 1024 * 1024),
        )(*[pltpu.with_memory_space_constraint(x, pltpu.HBM) for x in (terminal, initial_density, density_guess, diagonal)])
        return both[0], both[1]

    placed = (P("gx", "gy"), P("gx", "gy"), P(None, "gx", "gy"), P("gx", "gy"))
    return jax.shard_map(
        shards,
        mesh=mesh,
        in_specs=placed,
        out_specs=(P("gx", "gy"), P("gx", "gy")),
        check_vma=False,
    )
```

```python
import functools

import jax
import jax.numpy as jnp
from jax import lax
from jax.experimental import pallas as pl
from jax.experimental.pallas import tpu as pltpu
from jax.sharding import PartitionSpec as P

MESH = pl.DeviceIdType.MESH

LEVELS = 2
MARGIN = 16
LANES = 128

inv_step = 0.5
coupling = 0.5

SCALE = 0.25
SHIFT = 5.5

DIRECTIONS = [(r, c) for r in (-1, 1) for c in (-1, 1)] + [(-1, 0), (1, 0), (0, -1), (0, 1)]
TINY = 2e-7


def solve_small(nu):
    g00 = nu[1] / SCALE + SHIFT * nu[0]
    g01 = nu[2] / SCALE + SHIFT * nu[1]
    g02 = nu[3] / SCALE + SHIFT * nu[2]
    g12 = nu[4] / SCALE + SHIFT * nu[3]
    g22 = nu[5] / SCALE + SHIFT * nu[4]
    g11 = g02
    inv0 = 1.0 / g00
    l10 = g01 * inv0
    l20 = g02 * inv0
    d1 = g11 - l10 * g01
    ok1 = d1 > TINY * g11
    inv1 = jnp.where(ok1, 1.0 / jnp.where(ok1, d1, 1.0), 0.0)
    t = g12 - l20 * g01
    l21 = t * inv1
    d2 = g22 - l20 * g02 - l21 * t
    ok2 = ok1 & (d2 > TINY * g22)
    inv2 = jnp.where(ok2, 1.0 / jnp.where(ok2, d2, 1.0), 0.0)
    y1 = nu[1] - l10 * nu[0]
    y2 = nu[2] - l20 * nu[0] - l21 * y1
    c2 = y2 * inv2
    c1 = y1 * inv1 - l21 * c2
    c0 = nu[0] * inv0 - l10 * c1 - l20 * c2
    return c0, c1, c2


def kernel(nx, ny, term_ref, dens_ref, guess_ref, diag_ref, both_ref,
           main, left, right, rim, edge, edge_left, edge_right, sent, slots, sizes, halo_send, halo_recv, own_sem, sum_send, sum_recv,
           ready, scaled_tall, scaled_mid, scaled_small):
    rows, cols = term_ref.shape
    gx = lax.axis_index("gx")
    gy = lax.axis_index("gy")
    count = nx * ny
    me = gx * ny + gy

    def inside(dr, dc):
        ok = None
        for here_at, step, size in ((gx, dr, nx), (gy, dc, ny)):
            if step == 1:
                test = here_at < size - 1
            elif step == -1:
                test = here_at > 0
            else:
                continue
            ok = test if ok is None else ok & test
        return ok

    def across(k):
        return (lax.rem(gx + k, nx), gy)

    def along(k):
        return (gx, lax.rem(gy + k, ny))

    barrier = pltpu.get_barrier_semaphore()
    greeted = nx + ny - 2
    for dr, dc in DIRECTIONS:
        if dr != 0 and dc != 0:
            there = inside(dr, dc)
            greeted = greeted + jnp.where(there, 1, 0)

            @pl.when(there)
            def _():
                pl.semaphore_signal(
                    barrier, inc=1, device_id=(gx + dr, gy + dc), device_id_type=MESH)

    for k in range(1, nx):
        pl.semaphore_signal(barrier, inc=1, device_id=across(k), device_id_type=MESH)
    for k in range(1, ny):
        pl.semaphore_signal(barrier, inc=1, device_id=along(k), device_id_type=MESH)

    here = pl.ds(MARGIN, rows)
    own = [
        pltpu.make_async_copy(source, main.at[at, here], own_sem)
        for at, source in enumerate(
            (term_ref, diag_ref, guess_ref.at[1], guess_ref.at[0], dens_ref))
    ]
    for copy in own:
        copy.start()
    wide = cols + LANES
    half = LANES // 2
    tall = rows + 2 * MARGIN
    low_mid, high_mid = MARGIN - 8, MARGIN + rows + 8

    def mask_of(size, cyclic, margin):
        row = lax.broadcasted_iota(jnp.int32, (size, wide), 0)
        col = lax.broadcasted_iota(jnp.int32, (size, wide), 1)
        col_low = jnp.where(gy < ny - 1, cols + half, cols)
        col_high = jnp.where(gy > 0, cols + half, wide)
        ok = (col < col_low) | (col >= col_high)
        if cyclic:
            row_low = jnp.where(gx < nx - 1, rows + 4, rows)
            row_high = jnp.where(gx > 0, rows + 4, size)
            return ok & ((row < row_low) | (row >= row_high))
        row_low = jnp.where(gx > 0, 0, margin)
        row_high = jnp.where(gx < nx - 1, size, margin + rows)
        return ok & (row >= row_low) & (row < row_high)

    scaled = {"tall": scaled_tall, "mid": scaled_mid, "small": scaled_small}
    scaled_tall[...] = jnp.where(mask_of(tall, False, MARGIN), SCALE, 0.0)
    scaled_mid[...] = jnp.where(mask_of(rows + 16, False, 8), SCALE, 0.0)
    scaled_small[...] = jnp.where(mask_of(rows + 8, True, 4), SCALE, 0.0)

    pltpu.make_async_copy(main.at[:, here], main.at[:, here], own_sem).wait()
    for part in range(3):
        for a in range(3):
            rim[part, 0, a] = main[a, MARGIN + 4 * part:MARGIN + 4 * part + 4]
            rim[part, 1, a] = main[a, MARGIN + rows - 4 * part - 4:MARGIN + rows - 4 * part]
    pl.semaphore_wait(barrier, greeted)

    def pieces(dr, stage):
        if dr == 0:
            return [[(0, 3, 0, rows)], [], [(3, 2, 0, rows)]][stage]
        return [
            [(0, 3, 0, 4)],
            [(0, 3, 4, 4), (1, 2, 8, 4), (0, 1, 8, 8)],
            [(3, 2, 0, 8), (3, 1, 8, 8)],
        ][stage]

    def halo(d, stage, piece):
        dr, dc = DIRECTIONS[d]
        first, many, out, size = piece
        if dr == 0:
            src_rows, dst_rows = here, here
        elif dr == 1:
            src_rows = pl.ds(MARGIN + rows - out - size, size)
            dst_rows = pl.ds(MARGIN - out - size, size)
        else:
            src_rows = pl.ds(MARGIN + out, size)
            dst_rows = pl.ds(MARGIN + rows + out, size)
        if dc == 0:
            src_cols, buf, rim_buf = pl.ds(0, cols), main, edge
        elif dc == 1:
            src_cols, buf, rim_buf = pl.ds(cols - LANES, LANES), left, edge_left
        else:
            src_cols, buf, rim_buf = pl.ds(0, LANES), right, edge_right
        src = main.at[pl.ds(first, many), src_rows, src_cols]
        dst = buf.at[pl.ds(first, many), dst_rows, :]
        if size == 4:
            side = 1 if dr == 1 else 0
            src = rim.at[out // 4, side, pl.ds(first, many), :, src_cols]
            dst = rim_buf.at[out // 4, side, pl.ds(first, many)]
        return pltpu.make_async_remote_copy(
            src_ref=src, dst_ref=dst,
            send_sem=halo_send, recv_sem=halo_recv.at[stage],
            device_id=(gx + dr, gy + dc), device_id_type=MESH)

    def start_halo(stage):
        for d, (dr, dc) in enumerate(DIRECTIONS):
            if pieces(dr, stage):
                @pl.when(inside(dr, dc))
                def _():
                    for piece in pieces(dr, stage):
                        halo(d, stage, piece).start()

    def tiles(ends, sides, stages):
        total = 0
        for dr, dc in ((1, 0), (0, 1), (1, 1)):
            times = (ends if dr else 1) * (sides if dc else 1)
            for stage in stages:
                for _, many, _, size in pieces(dr, stage):
                    total += times * many * (size // 4) * (1 if dc else cols // LANES)
        return total

    def beside_count(here_at, size):
        return jnp.where(here_at > 0, 1, 0) + jnp.where(here_at < size - 1, 1, 0)

    def wait_halo(sem, *stages):
        for ends in range(min(1, nx - 1), min(2, nx - 1) + 1):
            for sides in range(min(1, ny - 1), min(2, ny - 1) + 1):
                many = tiles(ends, sides, stages)
                if many == 0:
                    continue

                @pl.when((beside_count(gx, nx) == ends) & (beside_count(gy, ny) == sides))
                def _():
                    span = sizes.at[pl.ds(0, many)]
                    pltpu.make_async_copy(span, span, sem).wait()

    start_halo(0)
    for k in range(1, nx):
        pl.semaphore_signal(ready, inc=1, device_id=across(k), device_id_type=MESH)
    start_halo(1)
    start_halo(2)

    def shrink(x, start):
        sub = lax.broadcasted_iota(jnp.int32, (8, x.shape[1]), 0)
        ends = jnp.where(sub < 4, x[start + rows:start + rows + 8], x[start - 8:start])
        return jnp.concatenate([x[start:start + rows], ends], axis=0)

    def joined(x, from_right, from_left):
        lane = lax.broadcasted_iota(jnp.int32, from_right.shape, 1)
        return jnp.concatenate([x, jnp.where(lane < half, from_right, from_left)], axis=1)

    def strip(a, begin, end):
        return joined(main[a, begin:end], right[a, begin:end], left[a, begin:end])

    def rims(a, one, other):
        return joined(*(
            jnp.concatenate([buf[part, side, a] for part, side in (one, other)], axis=0)
            for buf in (edge, edge_right, edge_left)))

    def field(a, window):
        if a > 2:
            if window == "tall":
                return strip(a, 0, tall)
            x = strip(a, low_mid, high_mid)
            return x if window == "mid" else shrink(x, 8)
        own_rows = strip(a, MARGIN, MARGIN + rows)
        if window == "small":
            return jnp.concatenate([own_rows, rims(a, (0, 0), (0, 1))], axis=0)
        above, below = rims(a, (1, 1), (0, 1)), rims(a, (0, 0), (1, 0))
        x = [above, own_rows, below]
        if window == "tall" and a == 0:
            x = [strip(a, 0, low_mid)] + x + [strip(a, high_mid, tall)]
        elif window == "tall":
            x = [rims(a, (2, 1), (2, 1))] + x + [rims(a, (2, 0), (2, 0))]
        return jnp.concatenate(x, axis=0)

    def up(x):
        return pltpu.roll(x, 1, 0)

    def down(x):
        return pltpu.roll(x, x.shape[0] - 1, 0)

    def before(x):
        return pltpu.roll(x, 1, 1)

    def after(x):
        return pltpu.roll(x, x.shape[1] - 1, 1)

    def masked(x, window):
        return jnp.where(scaled[window][...] > 0.0, x, 0.0)

    def core_of(window):
        return masked(SCALE * (field(1, window) + (inv_step + 4.0 - SHIFT)), window)

    def apply_b(v, core, window):
        beside = (up(v) + down(v)) + (before(v) + after(v))
        return core * v - scaled[window][...] * beside

    def apply_half(v, core):
        return (0.5 * core) * v - SCALE * (down(v) + after(v))

    def slopes(u):
        back_x, back_y = u - up(u), u - before(u)
        return back_x, down(back_x), back_y, after(back_y)

    def hamiltonian(slope):
        back_x, ahead_x, back_y, ahead_y = slope
        px, qx = jnp.maximum(back_x, 0.0), jnp.minimum(ahead_x, 0.0)
        py, qy = jnp.maximum(back_y, 0.0), jnp.minimum(ahead_y, 0.0)
        return (px * px + qx * qx) + (py * py + qy * qy)

    def falls(u):
        return u - down(u), u - after(u)

    def faces(fall):
        sx, sy = fall
        return jnp.maximum(sx, 0.0), jnp.minimum(sx, 0.0), jnp.maximum(sy, 0.0), jnp.minimum(sy, 0.0)

    def ahead(m):
        return m, down(m), after(m)

    def unit(window):
        return (1.0 / SCALE) * scaled[window][...]

    def advance(m_ahead, face, ones):
        m, below, beyond = m_ahead
        px, qx, py, qy = face
        fx = px * m + qx * below
        fy = py * m + qy * beyond
        net = (fx - up(fx)) + (fy - before(fy))
        return inv_step * m - ones * net

    def own_guess(level, window):
        return masked(coupling * field(2 if level == 1 else 3, window), window)

    def value_rhs(later, slope, guess, ones):
        return (inv_step * later + guess) - (0.5 * ones) * hamiltonian(slope)

    def tree(parts):
        while len(parts) > 1:
            odd = parts[len(parts) // 2 * 2:]
            parts = [parts[i] + parts[i + 1] for i in range(0, len(parts) - 1, 2)] + odd
        return parts[0]

    def fold(p):
        return tree([p[i:i + 8, j:j + LANES] for i in range(0, rows, 8) for j in range(0, cols, LANES)])

    def dot(x, y):
        return fold(x * y)

    sub8 = lax.broadcasted_iota(jnp.int32, (8, LANES), 0)
    lane8 = lax.broadcasted_iota(jnp.int32, (8, LANES), 1)

    def pack(tiles):
        spread = None
        for first in range(0, len(tiles), 8):
            group = tiles[first:first + 8]
            group = group + [jnp.zeros((8, LANES), jnp.float32)] * (8 - len(group))
            for step in (4, 2, 1):
                keep = lax.rem(sub8, 2 * step) < step
                group = [
                    jnp.where(keep, a + pltpu.roll(a, 8 - step, 0), b + pltpu.roll(b, step, 0))
                    for a, b in zip(group[:step], group[step:])
                ]
            sums = jnp.sum(group[0], axis=1, keepdims=True)
            part = jnp.where(lane8 == sub8 + first, sums, 0.0)
            spread = part if spread is None else spread + part
        return jnp.sum(spread, axis=0, keepdims=True)

    def send_sums(which, values):
        packed = pack(values)
        sent[which] = packed
        slots[which, me] = packed

        def send(px, py):
            pltpu.make_async_remote_copy(
                src_ref=sent.at[which], dst_ref=slots.at[which, me],
                send_sem=sum_send, recv_sem=sum_recv.at[which % 2],
                device_id=(px, py), device_id_type=MESH).start()

        def line(k, carry):
            px = lax.rem(gx + k, nx)
            for j in range(ny):
                send(px, jnp.where(2 * gy < ny, ny - 1 - j, j))
            return carry

        lax.fori_loop(1, nx, line, 0)
        for k in range(1, ny):
            send(gx, lax.rem(gy + k, ny))

    def take_sums(which, many):
        others = slots.at[which, pl.ds(0, count - 1)]
        pltpu.make_async_copy(others, others, sum_recv.at[which % 2]).wait()
        total = jnp.broadcast_to(tree([slots[which, k] for k in range(count)]), (8, LANES))
        return [jnp.broadcast_to(total[:, k:k + 1], (8, LANES)) for k in range(many)]

    def basis(b, core, window, last=True):
        v1 = apply_b(b, core, window)
        v2 = apply_b(v1, core, window)
        return (b, v1, v2, apply_half(v2, core)) if last else (b, v1, v2)

    def spread(tile, like):
        wide_tile = jnp.concatenate([tile] * (like.shape[1] // LANES), axis=1)
        return jnp.concatenate([wide_tile] * (like.shape[0] // 8), axis=0)

    def mix(c, v):
        parts = [spread(a, x) * x for a, x in zip(c, v)]
        return (parts[0] + parts[1]) + parts[2]

    def pairs(x, y):
        return [dot(x[0], y[0]), dot(x[0], y[1]), dot(x[1], y[1]),
                dot(x[1], y[2]), dot(x[2], y[2]),
                2.0 * dot(x[2], x[3]) if x is y
                else fold(x[2] * y[3] + y[2] * x[3])]

    def own_small(v):
        return [x[:rows, :cols] for x in v]

    wait_halo(halo_recv.at[0], 0)
    small_core = core_of("small")
    small_ones = unit("small")
    later = masked(field(0, "small"), "small")
    w = own_small(basis(
        value_rhs(later, slopes(later), own_guess(1, "small"), small_ones), small_core, "small"))
    moments = pairs(w, w)
    pl.semaphore_wait(ready, nx - 1)
    send_sums(0, moments)
    wait_halo(halo_recv.at[1], 1)
    core, ones = core_of("tall"), unit("tall")
    later = masked(field(0, "tall"), "tall")
    v = basis(
        value_rhs(later, slopes(later), own_guess(1, "tall"), ones), core, "tall", last=False)
    vs = [shrink(x, MARGIN) for x in v]
    steep = list(zip(*[slopes(x) for x in vs]))
    wait_halo(halo_recv.at[2], 2)
    guess = own_guess(0, "small")
    c = solve_small(take_sums(0, 6))

    first_small = mix(c, vs)
    w = own_small(basis(
        value_rhs(first_small, [mix(c, x) for x in steep], guess, small_ones), small_core, "small"))
    send_sums(1, pairs(w, w))
    first = mix(c, v)
    v = basis(value_rhs(first, slopes(first), own_guess(0, "tall"), ones), core, "tall", last=False)
    v = [x[low_mid:high_mid] for x in v]
    steep = list(zip(*[falls(x) for x in v]))
    face = faces(falls(first_small))
    density = ahead(masked(field(4, "mid"), "mid"))
    mid_core, mid_ones = core_of("mid"), unit("mid")
    c = solve_small(take_sums(1, 6))

    rhs = advance(density, faces([mix(c, x) for x in steep]), mid_ones)
    a = basis(rhs, mid_core, "mid", last=False)
    a = [shrink(x, 8) for x in a]
    last = apply_half(a[2], small_core)
    inner = own_small(a + [last])
    families = [
        own_small(basis(advance(ahead(x), face, small_ones), small_core, "small")) for x in a]
    moments = pairs(inner, inner)
    for i in range(3):
        for j in range(i, 3):
            moments += pairs(families[i], families[j])
    send_sums(2, moments)
    both_ref[0] = mix(c, [x[8:8 + rows, :cols] for x in v])
    wait_halo(halo_send, 0, 1, 2)
    others = slots.at[:, pl.ds(0, count - 1)]
    pltpu.make_async_copy(others, others, sum_send).wait()
    total = take_sums(2, len(moments))
    c = solve_small(total[:6])
    picks = [(i, j) for i in range(3) for j in range(i, 3)]
    weights = [c[i] * c[j] * (1.0 if i == j else 2.0) for i, j in picks]
    nu = [
        tree([weight * total[6 + 6 * at + k] for at, weight in enumerate(weights)])
        for k in range(6)
    ]
    e = solve_small(nu)
    result = mix(e, [mix(c, [families[i][k] for i in range(3)]) for k in range(3)])
    both_ref[1] = result


def solution(mesh):
    nx, ny = mesh.shape["gx"], mesh.shape["gy"]

    def shards(terminal, initial_density, density_guess, diagonal):
        rows, cols = terminal.shape
        tall = rows + 2 * MARGIN
        hbm = pl.BlockSpec(memory_space=pl.ANY)
        vmem = pl.BlockSpec(memory_space=pltpu.VMEM)
        shape = jax.ShapeDtypeStruct((rows, cols), jnp.float32)
        both = pl.pallas_call(
            functools.partial(kernel, nx, ny),
            out_shape=jax.ShapeDtypeStruct((2, rows, cols), jnp.float32),
            in_specs=[hbm] * 4,
            out_specs=vmem,
            scratch_shapes=[
                pltpu.VMEM((5, tall, cols), jnp.float32),
                pltpu.VMEM((5, tall, LANES), jnp.float32),
                pltpu.VMEM((5, tall, LANES), jnp.float32),
                pltpu.VMEM((3, 2, 3, 4, cols), jnp.float32),
                pltpu.VMEM((3, 2, 3, 4, cols), jnp.float32),
                pltpu.VMEM((3, 2, 3, 4, LANES), jnp.float32),
                pltpu.VMEM((3, 2, 3, 4, LANES), jnp.float32),
                pltpu.VMEM((3, 1, LANES), jnp.float32),
                pltpu.VMEM((3, nx * ny, 1, LANES), jnp.float32),
                pltpu.VMEM((10 * 4 * (rows // 8 + 2) * (cols // LANES + 2), 4, LANES), jnp.float32),
                pltpu.SemaphoreType.DMA,
                pltpu.SemaphoreType.DMA((3,)),
                pltpu.SemaphoreType.DMA,
                pltpu.SemaphoreType.DMA,
                pltpu.SemaphoreType.DMA((2,)),
                pltpu.SemaphoreType.REGULAR,
                pltpu.VMEM((tall, cols + LANES), jnp.float32),
                pltpu.VMEM((rows + 16, cols + LANES), jnp.float32),
                pltpu.VMEM((rows + 8, cols + LANES), jnp.float32),
            ],
            compiler_params=pltpu.CompilerParams(collective_id=0, has_side_effects=True, vmem_limit_bytes=4 * 1024 * 1024),
        )(*[pltpu.with_memory_space_constraint(x, pltpu.HBM) for x in (terminal, initial_density, density_guess, diagonal)])
        return both[0], both[1]

    placed = (P("gx", "gy"), P("gx", "gy"), P(None, "gx", "gy"), P("gx", "gy"))
    return jax.shard_map(
        shards,
        mesh=mesh,
        in_specs=placed,
        out_specs=(P("gx", "gy"), P("gx", "gy")),
        check_vma=False,
    )
```

```python
import functools

import jax
import jax.numpy as jnp
from jax import lax
from jax.experimental import pallas as pl
from jax.experimental.pallas import tpu as pltpu
from jax.sharding import PartitionSpec as P

MESH = pl.DeviceIdType.MESH

LEVELS = 2
MARGIN = 16
LANES = 128

inv_step = 0.5
coupling = 0.5

SCALE = 0.25
SHIFT = 5.5

DIRECTIONS = [(r, c) for r in (-1, 1) for c in (-1, 1)] + [(-1, 0), (1, 0), (0, -1), (0, 1)]
TINY = 2e-7


def solve_small(nu):
    g00 = nu[1] / SCALE + SHIFT * nu[0]
    g01 = nu[2] / SCALE + SHIFT * nu[1]
    g02 = nu[3] / SCALE + SHIFT * nu[2]
    g12 = nu[4] / SCALE + SHIFT * nu[3]
    g22 = nu[5] / SCALE + SHIFT * nu[4]
    g11 = g02
    inv0 = 1.0 / g00
    l10 = g01 * inv0
    l20 = g02 * inv0
    d1 = g11 - l10 * g01
    ok1 = d1 > TINY * g11
    inv1 = jnp.where(ok1, 1.0 / jnp.where(ok1, d1, 1.0), 0.0)
    t = g12 - l20 * g01
    l21 = t * inv1
    d2 = g22 - l20 * g02 - l21 * t
    ok2 = ok1 & (d2 > TINY * g22)
    inv2 = jnp.where(ok2, 1.0 / jnp.where(ok2, d2, 1.0), 0.0)
    y1 = nu[1] - l10 * nu[0]
    y2 = nu[2] - l20 * nu[0] - l21 * y1
    c2 = y2 * inv2
    c1 = y1 * inv1 - l21 * c2
    c0 = nu[0] * inv0 - l10 * c1 - l20 * c2
    return c0, c1, c2


def kernel(nx, ny, term_ref, dens_ref, guess_ref, diag_ref, both_ref,
           main, left, right, rim, edge, edge_left, edge_right, sent, slots, sizes, halo_send, halo_recv, own_sem, sum_send, sum_recv,
           ready, scaled_tall, scaled_mid, scaled_small):
    rows, cols = term_ref.shape
    gx = lax.axis_index("gx")
    gy = lax.axis_index("gy")
    count = nx * ny
    me = gx * ny + gy

    def inside(dr, dc):
        ok = None
        for here_at, step, size in ((gx, dr, nx), (gy, dc, ny)):
            if step == 1:
                test = here_at < size - 1
            elif step == -1:
                test = here_at > 0
            else:
                continue
            ok = test if ok is None else ok & test
        return ok

    def across(k):
        return (lax.rem(gx + k, nx), gy)

    def along(k):
        return (gx, lax.rem(gy + k, ny))

    barrier = pltpu.get_barrier_semaphore()
    greeted = nx + ny - 2
    for dr, dc in DIRECTIONS:
        if dr != 0 and dc != 0:
            there = inside(dr, dc)
            greeted = greeted + jnp.where(there, 1, 0)

            @pl.when(there)
            def _():
                pl.semaphore_signal(
                    barrier, inc=1, device_id=(gx + dr, gy + dc), device_id_type=MESH)

    for k in range(1, nx):
        pl.semaphore_signal(barrier, inc=1, device_id=across(k), device_id_type=MESH)
    for k in range(1, ny):
        pl.semaphore_signal(barrier, inc=1, device_id=along(k), device_id_type=MESH)

    here = pl.ds(MARGIN, rows)
    own = [
        pltpu.make_async_copy(source, main.at[at, here], own_sem)
        for at, source in enumerate(
            (term_ref, diag_ref, guess_ref.at[1], guess_ref.at[0], dens_ref))
    ]
    for copy in own:
        copy.start()
    wide = cols + LANES
    half = LANES // 2
    tall = rows + 2 * MARGIN
    low_mid, high_mid = MARGIN - 8, MARGIN + rows + 8

    def mask_of(size, cyclic, margin):
        row = lax.broadcasted_iota(jnp.int32, (size, wide), 0)
        col = lax.broadcasted_iota(jnp.int32, (size, wide), 1)
        col_low = jnp.where(gy < ny - 1, cols + half, cols)
        col_high = jnp.where(gy > 0, cols + half, wide)
        ok = (col < col_low) | (col >= col_high)
        if cyclic:
            row_low = jnp.where(gx < nx - 1, rows + 4, rows)
            row_high = jnp.where(gx > 0, rows + 4, size)
            return ok & ((row < row_low) | (row >= row_high))
        row_low = jnp.where(gx > 0, 0, margin)
        row_high = jnp.where(gx < nx - 1, size, margin + rows)
        return ok & (row >= row_low) & (row < row_high)

    scaled = {"tall": scaled_tall, "mid": scaled_mid, "small": scaled_small}
    scaled_tall[...] = jnp.where(mask_of(tall, False, MARGIN), SCALE, 0.0)
    scaled_mid[...] = jnp.where(mask_of(rows + 16, False, 8), SCALE, 0.0)
    scaled_small[...] = jnp.where(mask_of(rows + 8, True, 4), SCALE, 0.0)

    pltpu.make_async_copy(main.at[:, here], main.at[:, here], own_sem).wait()
    for part in range(3):
        for a in range(3):
            rim[part, 0, a] = main[a, MARGIN + 4 * part:MARGIN + 4 * part + 4]
            rim[part, 1, a] = main[a, MARGIN + rows - 4 * part - 4:MARGIN + rows - 4 * part]
    pl.semaphore_wait(barrier, greeted)

    def pieces(dr, stage):
        if dr == 0:
            return [[(0, 3, 0, rows)], [], [(3, 2, 0, rows)]][stage]
        return [
            [(0, 3, 0, 4)],
            [(0, 3, 4, 4), (1, 2, 8, 4), (0, 1, 8, 8)],
            [(3, 2, 0, 8), (3, 1, 8, 8)],
        ][stage]

    def halo(d, stage, piece):
        dr, dc = DIRECTIONS[d]
        first, many, out, size = piece
        if dr == 0:
            src_rows, dst_rows = here, here
        elif dr == 1:
            src_rows = pl.ds(MARGIN + rows - out - size, size)
            dst_rows = pl.ds(MARGIN - out - size, size)
        else:
            src_rows = pl.ds(MARGIN + out, size)
            dst_rows = pl.ds(MARGIN + rows + out, size)
        if dc == 0:
            src_cols, buf, rim_buf = pl.ds(0, cols), main, edge
        elif dc == 1:
            src_cols, buf, rim_buf = pl.ds(cols - LANES, LANES), left, edge_left
        else:
            src_cols, buf, rim_buf = pl.ds(0, LANES), right, edge_right
        src = main.at[pl.ds(first, many), src_rows, src_cols]
        dst = buf.at[pl.ds(first, many), dst_rows, :]
        if size == 4:
            side = 1 if dr == 1 else 0
            src = rim.at[out // 4, side, pl.ds(first, many), :, src_cols]
            dst = rim_buf.at[out // 4, side, pl.ds(first, many)]
        return pltpu.make_async_remote_copy(
            src_ref=src, dst_ref=dst,
            send_sem=halo_send, recv_sem=halo_recv.at[stage],
            device_id=(gx + dr, gy + dc), device_id_type=MESH)

    def start_halo(stage):
        for d, (dr, dc) in enumerate(DIRECTIONS):
            if pieces(dr, stage):
                @pl.when(inside(dr, dc))
                def _():
                    for piece in pieces(dr, stage):
                        halo(d, stage, piece).start()

    def tiles(ends, sides, stages):
        total = 0
        for dr, dc in ((1, 0), (0, 1), (1, 1)):
            times = (ends if dr else 1) * (sides if dc else 1)
            for stage in stages:
                for _, many, _, size in pieces(dr, stage):
                    total += times * many * (size // 4) * (1 if dc else cols // LANES)
        return total

    def beside_count(here_at, size):
        return jnp.where(here_at > 0, 1, 0) + jnp.where(here_at < size - 1, 1, 0)

    def wait_halo(sem, *stages):
        for ends in range(min(1, nx - 1), min(2, nx - 1) + 1):
            for sides in range(min(1, ny - 1), min(2, ny - 1) + 1):
                many = tiles(ends, sides, stages)
                if many == 0:
                    continue

                @pl.when((beside_count(gx, nx) == ends) & (beside_count(gy, ny) == sides))
                def _():
                    span = sizes.at[pl.ds(0, many)]
                    pltpu.make_async_copy(span, span, sem).wait()

    start_halo(0)
    for k in range(1, nx):
        pl.semaphore_signal(ready, inc=1, device_id=across(k), device_id_type=MESH)
    start_halo(1)
    start_halo(2)

    def shrink(x, start):
        sub = lax.broadcasted_iota(jnp.int32, (8, x.shape[1]), 0)
        ends = jnp.where(sub < 4, x[start + rows:start + rows + 8], x[start - 8:start])
        return jnp.concatenate([x[start:start + rows], ends], axis=0)

    def joined(x, from_right, from_left):
        lane = lax.broadcasted_iota(jnp.int32, from_right.shape, 1)
        return jnp.concatenate([x, jnp.where(lane < half, from_right, from_left)], axis=1)

    def strip(a, begin, end):
        return joined(main[a, begin:end], right[a, begin:end], left[a, begin:end])

    def rims(a, one, other):
        return joined(*(
            jnp.concatenate([buf[part, side, a] for part, side in (one, other)], axis=0)
            for buf in (edge, edge_right, edge_left)))

    def field(a, window):
        if a > 2:
            if window == "tall":
                return strip(a, 0, tall)
            x = strip(a, low_mid, high_mid)
            return x if window == "mid" else shrink(x, 8)
        own_rows = strip(a, MARGIN, MARGIN + rows)
        if window == "small":
            return jnp.concatenate([own_rows, rims(a, (0, 0), (0, 1))], axis=0)
        above, below = rims(a, (1, 1), (0, 1)), rims(a, (0, 0), (1, 0))
        x = [above, own_rows, below]
        if window == "tall" and a == 0:
            x = [strip(a, 0, low_mid)] + x + [strip(a, high_mid, tall)]
        elif window == "tall":
            x = [rims(a, (2, 1), (2, 1))] + x + [rims(a, (2, 0), (2, 0))]
        return jnp.concatenate(x, axis=0)

    def up(x):
        return pltpu.roll(x, 1, 0)

    def down(x):
        return pltpu.roll(x, x.shape[0] - 1, 0)

    def before(x):
        return pltpu.roll(x, 1, 1)

    def after(x):
        return pltpu.roll(x, x.shape[1] - 1, 1)

    def masked(x, window):
        return jnp.where(scaled[window][...] > 0.0, x, 0.0)

    def core_of(window):
        return masked(SCALE * (field(1, window) + (inv_step + 4.0 - SHIFT)), window)

    def apply_b(v, core, window):
        beside = (up(v) + down(v)) + (before(v) + after(v))
        return core * v - scaled[window][...] * beside

    def apply_half(v, core):
        return (0.5 * core) * v - SCALE * (down(v) + after(v))

    def slopes(u):
        back_x, back_y = u - up(u), u - before(u)
        return back_x, down(back_x), back_y, after(back_y)

    def hamiltonian(slope):
        back_x, ahead_x, back_y, ahead_y = slope
        px, qx = jnp.maximum(back_x, 0.0), jnp.minimum(ahead_x, 0.0)
        py, qy = jnp.maximum(back_y, 0.0), jnp.minimum(ahead_y, 0.0)
        return (px * px + qx * qx) + (py * py + qy * qy)

    def falls(u):
        return u - down(u), u - after(u)

    def faces(fall):
        sx, sy = fall
        return jnp.maximum(sx, 0.0), jnp.minimum(sx, 0.0), jnp.maximum(sy, 0.0), jnp.minimum(sy, 0.0)

    def ahead(m):
        return m, down(m), after(m)

    def unit(window):
        return (1.0 / SCALE) * scaled[window][...]

    def advance(m_ahead, face, ones):
        m, below, beyond = m_ahead
        px, qx, py, qy = face
        fx = px * m + qx * below
        fy = py * m + qy * beyond
        net = (fx - up(fx)) + (fy - before(fy))
        return inv_step * m - ones * net

    def own_guess(level, window):
        return masked(coupling * field(2 if level == 1 else 3, window), window)

    def value_rhs(later, slope, guess, ones):
        return (inv_step * later + guess) - (0.5 * ones) * hamiltonian(slope)

    def tree(parts):
        while len(parts) > 1:
            odd = parts[len(parts) // 2 * 2:]
            parts = [parts[i] + parts[i + 1] for i in range(0, len(parts) - 1, 2)] + odd
        return parts[0]

    def fold(p):
        return tree([p[i:i + 8, j:j + LANES] for i in range(0, rows, 8) for j in range(0, cols, LANES)])

    def dot(x, y):
        return fold(x * y)

    sub8 = lax.broadcasted_iota(jnp.int32, (8, LANES), 0)
    lane8 = lax.broadcasted_iota(jnp.int32, (8, LANES), 1)

    def pack(tiles):
        spread = None
        for first in range(0, len(tiles), 8):
            group = tiles[first:first + 8]
            group = group + [jnp.zeros((8, LANES), jnp.float32)] * (8 - len(group))
            for step in (4, 2, 1):
                keep = lax.rem(sub8, 2 * step) < step
                group = [
                    jnp.where(keep, a + pltpu.roll(a, 8 - step, 0), b + pltpu.roll(b, step, 0))
                    for a, b in zip(group[:step], group[step:])
                ]
            sums = jnp.sum(group[0], axis=1, keepdims=True)
            part = jnp.where(lane8 == sub8 + first, sums, 0.0)
            spread = part if spread is None else spread + part
        return jnp.sum(spread, axis=0, keepdims=True)

    def send_sums(which, values):
        packed = pack(values)
        sent[which] = packed
        slots[which, me] = packed

        def send(px, py):
            pltpu.make_async_remote_copy(
                src_ref=sent.at[which], dst_ref=slots.at[which, me],
                send_sem=sum_send, recv_sem=sum_recv.at[which % 2],
                device_id=(px, py), device_id_type=MESH).start()

        for begin in (2, 1):
            def column(j, carry):
                for k in range(begin, nx, 2):
                    send(lax.rem(gx + k, nx), jnp.where(2 * gy < ny, ny - 1 - j, j))
                return carry

            lax.fori_loop(0, ny, column, 0)
        for k in range(1, ny):
            send(gx, lax.rem(gy + k, ny))

    def take_sums(which, many):
        others = slots.at[which, pl.ds(0, count - 1)]
        pltpu.make_async_copy(others, others, sum_recv.at[which % 2]).wait()
        total = jnp.broadcast_to(tree([slots[which, k] for k in range(count)]), (8, LANES))
        return [jnp.broadcast_to(total[:, k:k + 1], (8, LANES)) for k in range(many)]

    def basis(b, core, window, last=True):
        v1 = apply_b(b, core, window)
        v2 = apply_b(v1, core, window)
        return (b, v1, v2, apply_half(v2, core)) if last else (b, v1, v2)

    def spread(tile, like):
        wide_tile = jnp.concatenate([tile] * (like.shape[1] // LANES), axis=1)
        return jnp.concatenate([wide_tile] * (like.shape[0] // 8), axis=0)

    def mix(c, v):
        parts = [spread(a, x) * x for a, x in zip(c, v)]
        return (parts[0] + parts[1]) + parts[2]

    def pairs(x, y):
        return [dot(x[0], y[0]), dot(x[0], y[1]), dot(x[1], y[1]),
                dot(x[1], y[2]), dot(x[2], y[2]),
                2.0 * dot(x[2], x[3]) if x is y
                else fold(x[2] * y[3] + y[2] * x[3])]

    def own_small(v):
        return [x[:rows, :cols] for x in v]

    wait_halo(halo_recv.at[0], 0)
    small_core = core_of("small")
    small_ones = unit("small")
    later = masked(field(0, "small"), "small")
    w = own_small(basis(
        value_rhs(later, slopes(later), own_guess(1, "small"), small_ones), small_core, "small"))
    moments = pairs(w, w)
    pl.semaphore_wait(ready, nx - 1)
    send_sums(0, moments)
    wait_halo(halo_recv.at[1], 1)
    core, ones = core_of("tall"), unit("tall")
    later = masked(field(0, "tall"), "tall")
    v = basis(
        value_rhs(later, slopes(later), own_guess(1, "tall"), ones), core, "tall", last=False)
    vs = [shrink(x, MARGIN) for x in v]
    steep = list(zip(*[slopes(x) for x in vs]))
    wait_halo(halo_recv.at[2], 2)
    guess = own_guess(0, "small")
    c = solve_small(take_sums(0, 6))

    first_small = mix(c, vs)
    w = own_small(basis(
        value_rhs(first_small, [mix(c, x) for x in steep], guess, small_ones), small_core, "small"))
    send_sums(1, pairs(w, w))
    first = mix(c, v)
    v = basis(value_rhs(first, slopes(first), own_guess(0, "tall"), ones), core, "tall", last=False)
    v = [x[low_mid:high_mid] for x in v]
    steep = list(zip(*[falls(x) for x in v]))
    face = faces(falls(first_small))
    density = ahead(masked(field(4, "mid"), "mid"))
    mid_core, mid_ones = core_of("mid"), unit("mid")
    c = solve_small(take_sums(1, 6))

    rhs = advance(density, faces([mix(c, x) for x in steep]), mid_ones)
    a = basis(rhs, mid_core, "mid", last=False)
    a = [shrink(x, 8) for x in a]
    last = apply_half(a[2], small_core)
    inner = own_small(a + [last])
    families = [
        own_small(basis(advance(ahead(x), face, small_ones), small_core, "small")) for x in a]
    moments = pairs(inner, inner)
    for i in range(3):
        for j in range(i, 3):
            moments += pairs(families[i], families[j])
    send_sums(2, moments)
    both_ref[0] = mix(c, [x[8:8 + rows, :cols] for x in v])
    wait_halo(halo_send, 0, 1, 2)
    others = slots.at[:, pl.ds(0, count - 1)]
    pltpu.make_async_copy(others, others, sum_send).wait()
    total = take_sums(2, len(moments))
    c = solve_small(total[:6])
    picks = [(i, j) for i in range(3) for j in range(i, 3)]
    weights = [c[i] * c[j] * (1.0 if i == j else 2.0) for i, j in picks]
    nu = [
        tree([weight * total[6 + 6 * at + k] for at, weight in enumerate(weights)])
        for k in range(6)
    ]
    e = solve_small(nu)
    result = mix(e, [mix(c, [families[i][k] for i in range(3)]) for k in range(3)])
    both_ref[1] = result


def solution(mesh):
    nx, ny = mesh.shape["gx"], mesh.shape["gy"]

    def shards(terminal, initial_density, density_guess, diagonal):
        rows, cols = terminal.shape
        tall = rows + 2 * MARGIN
        hbm = pl.BlockSpec(memory_space=pl.ANY)
        vmem = pl.BlockSpec(memory_space=pltpu.VMEM)
        shape = jax.ShapeDtypeStruct((rows, cols), jnp.float32)
        both = pl.pallas_call(
            functools.partial(kernel, nx, ny),
            out_shape=jax.ShapeDtypeStruct((2, rows, cols), jnp.float32),
            in_specs=[hbm] * 4,
            out_specs=vmem,
            scratch_shapes=[
                pltpu.VMEM((5, tall, cols), jnp.float32),
                pltpu.VMEM((5, tall, LANES), jnp.float32),
                pltpu.VMEM((5, tall, LANES), jnp.float32),
                pltpu.VMEM((3, 2, 3, 4, cols), jnp.float32),
                pltpu.VMEM((3, 2, 3, 4, cols), jnp.float32),
                pltpu.VMEM((3, 2, 3, 4, LANES), jnp.float32),
                pltpu.VMEM((3, 2, 3, 4, LANES), jnp.float32),
                pltpu.VMEM((3, 1, LANES), jnp.float32),
                pltpu.VMEM((3, nx * ny, 1, LANES), jnp.float32),
                pltpu.VMEM((10 * 4 * (rows // 8 + 2) * (cols // LANES + 2), 4, LANES), jnp.float32),
                pltpu.SemaphoreType.DMA,
                pltpu.SemaphoreType.DMA((3,)),
                pltpu.SemaphoreType.DMA,
                pltpu.SemaphoreType.DMA,
                pltpu.SemaphoreType.DMA((2,)),
                pltpu.SemaphoreType.REGULAR,
                pltpu.VMEM((tall, cols + LANES), jnp.float32),
                pltpu.VMEM((rows + 16, cols + LANES), jnp.float32),
                pltpu.VMEM((rows + 8, cols + LANES), jnp.float32),
            ],
            compiler_params=pltpu.CompilerParams(collective_id=0, has_side_effects=True, vmem_limit_bytes=4 * 1024 * 1024),
        )(*[pltpu.with_memory_space_constraint(x, pltpu.HBM) for x in (terminal, initial_density, density_guess, diagonal)])
        return both[0], both[1]

    placed = (P("gx", "gy"), P("gx", "gy"), P(None, "gx", "gy"), P("gx", "gy"))
    return jax.shard_map(
        shards,
        mesh=mesh,
        in_specs=placed,
        out_specs=(P("gx", "gy"), P("gx", "gy")),
        check_vma=False,
    )
```

```python
import functools

import jax
import jax.numpy as jnp
from jax import lax
from jax.experimental import pallas as pl
from jax.experimental.pallas import tpu as pltpu
from jax.sharding import PartitionSpec as P

MESH = pl.DeviceIdType.MESH

LEVELS = 2
MARGIN = 16
LANES = 128

inv_step = 0.5
coupling = 0.5

SCALE = 0.25
SHIFT = 5.5

DIRECTIONS = [(r, c) for r in (-1, 1) for c in (-1, 1)] + [(-1, 0), (1, 0), (0, -1), (0, 1)]
TINY = 2e-7


def solve_small(nu):
    g00 = nu[1] / SCALE + SHIFT * nu[0]
    g01 = nu[2] / SCALE + SHIFT * nu[1]
    g02 = nu[3] / SCALE + SHIFT * nu[2]
    g12 = nu[4] / SCALE + SHIFT * nu[3]
    g22 = nu[5] / SCALE + SHIFT * nu[4]
    g11 = g02
    inv0 = 1.0 / g00
    l10 = g01 * inv0
    l20 = g02 * inv0
    d1 = g11 - l10 * g01
    ok1 = d1 > TINY * g11
    inv1 = jnp.where(ok1, 1.0 / jnp.where(ok1, d1, 1.0), 0.0)
    t = g12 - l20 * g01
    l21 = t * inv1
    d2 = g22 - l20 * g02 - l21 * t
    ok2 = ok1 & (d2 > TINY * g22)
    inv2 = jnp.where(ok2, 1.0 / jnp.where(ok2, d2, 1.0), 0.0)
    y1 = nu[1] - l10 * nu[0]
    y2 = nu[2] - l20 * nu[0] - l21 * y1
    c2 = y2 * inv2
    c1 = y1 * inv1 - l21 * c2
    c0 = nu[0] * inv0 - l10 * c1 - l20 * c2
    return c0, c1, c2


def kernel(nx, ny, term_ref, dens_ref, guess_ref, diag_ref, both_ref,
           main, left, right, rim, edge, edge_left, edge_right, sent, slots, sizes, halo_send, halo_recv, own_sem, sum_send, sum_recv,
           ready, scaled_tall, scaled_mid, scaled_small):
    rows, cols = term_ref.shape
    gx = lax.axis_index("gx")
    gy = lax.axis_index("gy")
    count = nx * ny
    me = gx * ny + gy

    def inside(dr, dc):
        ok = None
        for here_at, step, size in ((gx, dr, nx), (gy, dc, ny)):
            if step == 1:
                test = here_at < size - 1
            elif step == -1:
                test = here_at > 0
            else:
                continue
            ok = test if ok is None else ok & test
        return ok

    def across(k):
        return (lax.rem(gx + k, nx), gy)

    def along(k):
        return (gx, lax.rem(gy + k, ny))

    barrier = pltpu.get_barrier_semaphore()
    greeted = nx + ny - 2
    for dr, dc in DIRECTIONS:
        if dr != 0 and dc != 0:
            there = inside(dr, dc)
            greeted = greeted + jnp.where(there, 1, 0)

            @pl.when(there)
            def _():
                pl.semaphore_signal(
                    barrier, inc=1, device_id=(gx + dr, gy + dc), device_id_type=MESH)

    for k in range(1, nx):
        pl.semaphore_signal(barrier, inc=1, device_id=across(k), device_id_type=MESH)
    for k in range(1, ny):
        pl.semaphore_signal(barrier, inc=1, device_id=along(k), device_id_type=MESH)

    here = pl.ds(MARGIN, rows)
    own = [
        pltpu.make_async_copy(source, main.at[at, here], own_sem)
        for at, source in enumerate(
            (term_ref, diag_ref, guess_ref.at[1], guess_ref.at[0], dens_ref))
    ]
    for copy in own:
        copy.start()
    wide = cols + LANES
    half = LANES // 2
    tall = rows + 2 * MARGIN
    low_mid, high_mid = MARGIN - 8, MARGIN + rows + 8

    def mask_of(size, cyclic, margin):
        row = lax.broadcasted_iota(jnp.int32, (size, wide), 0)
        col = lax.broadcasted_iota(jnp.int32, (size, wide), 1)
        col_low = jnp.where(gy < ny - 1, cols + half, cols)
        col_high = jnp.where(gy > 0, cols + half, wide)
        ok = (col < col_low) | (col >= col_high)
        if cyclic:
            row_low = jnp.where(gx < nx - 1, rows + 4, rows)
            row_high = jnp.where(gx > 0, rows + 4, size)
            return ok & ((row < row_low) | (row >= row_high))
        row_low = jnp.where(gx > 0, 0, margin)
        row_high = jnp.where(gx < nx - 1, size, margin + rows)
        return ok & (row >= row_low) & (row < row_high)

    scaled = {"tall": scaled_tall, "mid": scaled_mid, "small": scaled_small}
    scaled_tall[...] = jnp.where(mask_of(tall, False, MARGIN), SCALE, 0.0)
    scaled_mid[...] = jnp.where(mask_of(rows + 16, False, 8), SCALE, 0.0)
    scaled_small[...] = jnp.where(mask_of(rows + 8, True, 4), SCALE, 0.0)

    pltpu.make_async_copy(main.at[:, here], main.at[:, here], own_sem).wait()
    for part in range(3):
        for a in range(3):
            rim[part, 0, a] = main[a, MARGIN + 4 * part:MARGIN + 4 * part + 4]
            rim[part, 1, a] = main[a, MARGIN + rows - 4 * part - 4:MARGIN + rows - 4 * part]
    pl.semaphore_wait(barrier, greeted)

    def pieces(dr, stage):
        if dr == 0:
            return [[(0, 3, 0, rows)], [], [(3, 2, 0, rows)]][stage]
        return [
            [(0, 3, 0, 4)],
            [(0, 3, 4, 4), (1, 2, 8, 4), (0, 1, 8, 8)],
            [(3, 2, 0, 8), (3, 1, 8, 8)],
        ][stage]

    def halo(d, stage, piece):
        dr, dc = DIRECTIONS[d]
        first, many, out, size = piece
        if dr == 0:
            src_rows, dst_rows = here, here
        elif dr == 1:
            src_rows = pl.ds(MARGIN + rows - out - size, size)
            dst_rows = pl.ds(MARGIN - out - size, size)
        else:
            src_rows = pl.ds(MARGIN + out, size)
            dst_rows = pl.ds(MARGIN + rows + out, size)
        if dc == 0:
            src_cols, buf, rim_buf = pl.ds(0, cols), main, edge
        elif dc == 1:
            src_cols, buf, rim_buf = pl.ds(cols - LANES, LANES), left, edge_left
        else:
            src_cols, buf, rim_buf = pl.ds(0, LANES), right, edge_right
        src = main.at[pl.ds(first, many), src_rows, src_cols]
        dst = buf.at[pl.ds(first, many), dst_rows, :]
        if size == 4:
            side = 1 if dr == 1 else 0
            src = rim.at[out // 4, side, pl.ds(first, many), :, src_cols]
            dst = rim_buf.at[out // 4, side, pl.ds(first, many)]
        return pltpu.make_async_remote_copy(
            src_ref=src, dst_ref=dst,
            send_sem=halo_send, recv_sem=halo_recv.at[stage],
            device_id=(gx + dr, gy + dc), device_id_type=MESH)

    def start_halo(stage):
        for d, (dr, dc) in enumerate(DIRECTIONS):
            if pieces(dr, stage):
                @pl.when(inside(dr, dc))
                def _():
                    for piece in pieces(dr, stage):
                        halo(d, stage, piece).start()

    def tiles(ends, sides, stages):
        total = 0
        for dr, dc in ((1, 0), (0, 1), (1, 1)):
            times = (ends if dr else 1) * (sides if dc else 1)
            for stage in stages:
                for _, many, _, size in pieces(dr, stage):
                    total += times * many * (size // 4) * (1 if dc else cols // LANES)
        return total

    def beside_count(here_at, size):
        return jnp.where(here_at > 0, 1, 0) + jnp.where(here_at < size - 1, 1, 0)

    def wait_halo(sem, *stages):
        for ends in range(min(1, nx - 1), min(2, nx - 1) + 1):
            for sides in range(min(1, ny - 1), min(2, ny - 1) + 1):
                many = tiles(ends, sides, stages)
                if many == 0:
                    continue

                @pl.when((beside_count(gx, nx) == ends) & (beside_count(gy, ny) == sides))
                def _():
                    span = sizes.at[pl.ds(0, many)]
                    pltpu.make_async_copy(span, span, sem).wait()

    start_halo(0)
    for k in range(1, nx):
        pl.semaphore_signal(ready, inc=1, device_id=across(k), device_id_type=MESH)
    start_halo(1)
    start_halo(2)

    def shrink(x, start):
        sub = lax.broadcasted_iota(jnp.int32, (8, x.shape[1]), 0)
        ends = jnp.where(sub < 4, x[start + rows:start + rows + 8], x[start - 8:start])
        return jnp.concatenate([x[start:start + rows], ends], axis=0)

    def joined(x, from_right, from_left):
        lane = lax.broadcasted_iota(jnp.int32, from_right.shape, 1)
        return jnp.concatenate([x, jnp.where(lane < half, from_right, from_left)], axis=1)

    def strip(a, begin, end):
        return joined(main[a, begin:end], right[a, begin:end], left[a, begin:end])

    def rims(a, one, other):
        return joined(*(
            jnp.concatenate([buf[part, side, a] for part, side in (one, other)], axis=0)
            for buf in (edge, edge_right, edge_left)))

    def field(a, window):
        if a > 2:
            if window == "tall":
                return strip(a, 0, tall)
            x = strip(a, low_mid, high_mid)
            return x if window == "mid" else shrink(x, 8)
        own_rows = strip(a, MARGIN, MARGIN + rows)
        if window == "small":
            return jnp.concatenate([own_rows, rims(a, (0, 0), (0, 1))], axis=0)
        above, below = rims(a, (1, 1), (0, 1)), rims(a, (0, 0), (1, 0))
        x = [above, own_rows, below]
        if window == "tall" and a == 0:
            x = [strip(a, 0, low_mid)] + x + [strip(a, high_mid, tall)]
        elif window == "tall":
            x = [rims(a, (2, 1), (2, 1))] + x + [rims(a, (2, 0), (2, 0))]
        return jnp.concatenate(x, axis=0)

    def up(x):
        return pltpu.roll(x, 1, 0)

    def down(x):
        return pltpu.roll(x, x.shape[0] - 1, 0)

    def before(x):
        return pltpu.roll(x, 1, 1)

    def after(x):
        return pltpu.roll(x, x.shape[1] - 1, 1)

    def masked(x, window):
        return jnp.where(scaled[window][...] > 0.0, x, 0.0)

    def core_of(window):
        return masked(SCALE * (field(1, window) + (inv_step + 4.0 - SHIFT)), window)

    def apply_b(v, core, window):
        beside = (up(v) + down(v)) + (before(v) + after(v))
        return core * v - scaled[window][...] * beside

    def apply_half(v, core):
        return (0.5 * core) * v - SCALE * (down(v) + after(v))

    def slopes(u):
        return u - up(u), down(u) - u, u - before(u), after(u) - u

    def hamiltonian(slope):
        back_x, ahead_x, back_y, ahead_y = slope
        px, qx = jnp.maximum(back_x, 0.0), jnp.minimum(ahead_x, 0.0)
        py, qy = jnp.maximum(back_y, 0.0), jnp.minimum(ahead_y, 0.0)
        return (px * px + qx * qx) + (py * py + qy * qy)

    def falls(u):
        return u - down(u), u - after(u)

    def faces(fall):
        sx, sy = fall
        return jnp.maximum(sx, 0.0), jnp.minimum(sx, 0.0), jnp.maximum(sy, 0.0), jnp.minimum(sy, 0.0)

    def ahead(m):
        return m, down(m), after(m)

    def unit(window):
        return (1.0 / SCALE) * scaled[window][...]

    def advance(m_ahead, face, ones, face_behind=None):
        m, below, beyond = m_ahead
        px, qx, py, qy = face
        fx = px * m + qx * below
        fy = py * m + qy * beyond
        if face_behind is None:
            fy_behind = before(fy)
        else:
            fy_behind = face_behind[0] * before(m) + face_behind[1] * m
        net = (fx - up(fx)) + (fy - fy_behind)
        return inv_step * m - ones * net

    def own_guess(level, window):
        return masked(coupling * field(2 if level == 1 else 3, window), window)

    def value_rhs(later, slope, guess, ones):
        return (inv_step * later + guess) - (0.5 * ones) * hamiltonian(slope)

    def tree(parts):
        while len(parts) > 1:
            odd = parts[len(parts) // 2 * 2:]
            parts = [parts[i] + parts[i + 1] for i in range(0, len(parts) - 1, 2)] + odd
        return parts[0]

    def fold(p):
        return tree([p[i:i + 8, j:j + LANES] for i in range(0, rows, 8) for j in range(0, cols, LANES)])

    def dot(x, y):
        return fold(x * y)

    sub8 = lax.broadcasted_iota(jnp.int32, (8, LANES), 0)
    lane8 = lax.broadcasted_iota(jnp.int32, (8, LANES), 1)

    def pack(tiles):
        spread = None
        for first in range(0, len(tiles), 8):
            group = tiles[first:first + 8]
            group = group + [jnp.zeros((8, LANES), jnp.float32)] * (8 - len(group))
            for step in (4, 2, 1):
                keep = lax.rem(sub8, 2 * step) < step
                group = [
                    jnp.where(keep, a + pltpu.roll(a, 8 - step, 0), b + pltpu.roll(b, step, 0))
                    for a, b in zip(group[:step], group[step:])
                ]
            sums = jnp.sum(group[0], axis=1, keepdims=True)
            part = jnp.where(lane8 == sub8 + first, sums, 0.0)
            spread = part if spread is None else spread + part
        return jnp.sum(spread, axis=0, keepdims=True)

    def send_sums(which, values):
        packed = pack(values)
        sent[which] = packed
        slots[which, me] = packed

        def send(px, py):
            pltpu.make_async_remote_copy(
                src_ref=sent.at[which], dst_ref=slots.at[which, me],
                send_sem=sum_send, recv_sem=sum_recv.at[which % 2],
                device_id=(px, py), device_id_type=MESH).start()

        for begin in (2, 1):
            def column(j, carry):
                for k in sorted(range(begin, nx, 2), key=lambda k: min(k, nx - k)):
                    send(lax.rem(gx + k, nx), jnp.where(2 * gy < ny, ny - 1 - j, j))
                return carry

            lax.fori_loop(0, ny, column, 0)
        for k in range(1, ny):
            send(gx, lax.rem(gy + k, ny))

    def take_sums(which, many):
        others = slots.at[which, pl.ds(0, count - 1)]
        pltpu.make_async_copy(others, others, sum_recv.at[which % 2]).wait()
        total = jnp.broadcast_to(tree([slots[which, k] for k in range(count)]), (8, LANES))
        return [jnp.broadcast_to(total[:, k:k + 1], (8, LANES)) for k in range(many)]

    def basis(b, core, window, last=True):
        v1 = apply_b(b, core, window)
        v2 = apply_b(v1, core, window)
        return (b, v1, v2, apply_half(v2, core)) if last else (b, v1, v2)

    def spread(tile, like):
        wide_tile = jnp.concatenate([tile] * (like.shape[1] // LANES), axis=1)
        return jnp.concatenate([wide_tile] * (like.shape[0] // 8), axis=0)

    def mix(c, v):
        parts = [spread(a, x) * x for a, x in zip(c, v)]
        return (parts[0] + parts[1]) + parts[2]

    def pairs(x, y):
        return [dot(x[0], y[0]), dot(x[0], y[1]), dot(x[1], y[1]),
                dot(x[1], y[2]), dot(x[2], y[2]),
                2.0 * dot(x[2], x[3]) if x is y
                else fold(x[2] * y[3] + y[2] * x[3])]

    def own_small(v):
        return [x[:rows, :cols] for x in v]

    wait_halo(halo_recv.at[0], 0)
    small_core = core_of("small")
    small_ones = unit("small")
    later = masked(field(0, "small"), "small")
    w = own_small(basis(
        value_rhs(later, slopes(later), own_guess(1, "small"), small_ones), small_core, "small"))
    moments = pairs(w, w)
    pl.semaphore_wait(ready, nx - 1)
    send_sums(0, moments)
    wait_halo(halo_recv.at[1], 1)
    core, ones = core_of("tall"), unit("tall")
    later = masked(field(0, "tall"), "tall")
    v = basis(
        value_rhs(later, slopes(later), own_guess(1, "tall"), ones), core, "tall", last=False)
    vs = [shrink(x, MARGIN) for x in v]
    steep = list(zip(*[slopes(x) for x in vs]))
    wait_halo(halo_recv.at[2], 2)
    guess = own_guess(0, "small")
    c = solve_small(take_sums(0, 6))

    first_small = mix(c, vs)
    w = own_small(basis(
        value_rhs(first_small, [mix(c, x) for x in steep], guess, small_ones), small_core, "small"))
    send_sums(1, pairs(w, w))
    first = mix(c, v)
    v = basis(value_rhs(first, slopes(first), own_guess(0, "tall"), ones), core, "tall", last=False)
    v = [x[low_mid:high_mid] for x in v]
    steep = list(zip(*[falls(x) for x in v]))
    face = faces(falls(first_small))
    behind = before(face[2]), before(face[3])
    density = ahead(masked(field(4, "mid"), "mid"))
    mid_core, mid_ones = core_of("mid"), unit("mid")
    c = solve_small(take_sums(1, 6))

    rhs = advance(density, faces([mix(c, x) for x in steep]), mid_ones)
    a = basis(rhs, mid_core, "mid", last=False)
    a = [shrink(x, 8) for x in a]
    last = apply_half(a[2], small_core)
    inner = own_small(a + [last])
    families = [
        own_small(basis(
            advance(ahead(x), face, small_ones, behind if x is a[2] else None), small_core, "small"))
        for x in a]
    moments = pairs(inner, inner)
    for i in range(3):
        for j in range(i, 3):
            moments += pairs(families[i], families[j])
    send_sums(2, moments)
    both_ref[0] = mix(c, [x[8:8 + rows, :cols] for x in v])
    wait_halo(halo_send, 0, 1, 2)
    others = slots.at[:, pl.ds(0, count - 1)]
    pltpu.make_async_copy(others, others, sum_send).wait()
    total = take_sums(2, len(moments))
    c = solve_small(total[:6])
    picks = [(i, j) for i in range(3) for j in range(i, 3)]
    weights = [c[i] * c[j] * (1.0 if i == j else 2.0) for i, j in picks]
    nu = [
        tree([weight * total[6 + 6 * at + k] for at, weight in enumerate(weights)])
        for k in range(6)
    ]
    e = solve_small(nu)
    result = mix(e, [mix(c, [families[i][k] for i in range(3)]) for k in range(3)])
    both_ref[1] = result


def solution(mesh):
    nx, ny = mesh.shape["gx"], mesh.shape["gy"]

    def shards(terminal, initial_density, density_guess, diagonal):
        rows, cols = terminal.shape
        tall = rows + 2 * MARGIN
        hbm = pl.BlockSpec(memory_space=pl.ANY)
        vmem = pl.BlockSpec(memory_space=pltpu.VMEM)
        shape = jax.ShapeDtypeStruct((rows, cols), jnp.float32)
        both = pl.pallas_call(
            functools.partial(kernel, nx, ny),
            out_shape=jax.ShapeDtypeStruct((2, rows, cols), jnp.float32),
            in_specs=[hbm] * 4,
            out_specs=vmem,
            scratch_shapes=[
                pltpu.VMEM((5, tall, cols), jnp.float32),
                pltpu.VMEM((5, tall, LANES), jnp.float32),
                pltpu.VMEM((5, tall, LANES), jnp.float32),
                pltpu.VMEM((3, 2, 3, 4, cols), jnp.float32),
                pltpu.VMEM((3, 2, 3, 4, cols), jnp.float32),
                pltpu.VMEM((3, 2, 3, 4, LANES), jnp.float32),
                pltpu.VMEM((3, 2, 3, 4, LANES), jnp.float32),
                pltpu.VMEM((3, 1, LANES), jnp.float32),
                pltpu.VMEM((3, nx * ny, 1, LANES), jnp.float32),
                pltpu.VMEM((10 * 4 * (rows // 8 + 2) * (cols // LANES + 2), 4, LANES), jnp.float32),
                pltpu.SemaphoreType.DMA,
                pltpu.SemaphoreType.DMA((3,)),
                pltpu.SemaphoreType.DMA,
                pltpu.SemaphoreType.DMA,
                pltpu.SemaphoreType.DMA((2,)),
                pltpu.SemaphoreType.REGULAR,
                pltpu.VMEM((tall, cols + LANES), jnp.float32),
                pltpu.VMEM((rows + 16, cols + LANES), jnp.float32),
                pltpu.VMEM((rows + 8, cols + LANES), jnp.float32),
            ],
            compiler_params=pltpu.CompilerParams(collective_id=0, has_side_effects=True, vmem_limit_bytes=4 * 1024 * 1024),
        )(*[pltpu.with_memory_space_constraint(x, pltpu.HBM) for x in (terminal, initial_density, density_guess, diagonal)])
        return both[0], both[1]

    placed = (P("gx", "gy"), P("gx", "gy"), P(None, "gx", "gy"), P("gx", "gy"))
    return jax.shard_map(
        shards,
        mesh=mesh,
        in_specs=placed,
        out_specs=(P("gx", "gy"), P("gx", "gy")),
        check_vma=False,
    )
```

```python
import functools

import jax
import jax.numpy as jnp
from jax import lax
from jax.experimental import pallas as pl
from jax.experimental.pallas import tpu as pltpu
from jax.sharding import PartitionSpec as P

MESH = pl.DeviceIdType.MESH

LEVELS = 2
MARGIN = 16
LANES = 128

inv_step = 0.5
coupling = 0.5

SCALE = 0.25
SHIFT = 5.5

CORNERS = [(r, c) for r in (-1, 1) for c in (-1, 1)]
DIRECTIONS = [(-1, 0), (1, 0)] + CORNERS + [(0, -1), (0, 1)]
TINY = 2e-7


def solve_small(nu):
    g00 = nu[1] / SCALE + SHIFT * nu[0]
    g01 = nu[2] / SCALE + SHIFT * nu[1]
    g02 = nu[3] / SCALE + SHIFT * nu[2]
    g12 = nu[4] / SCALE + SHIFT * nu[3]
    g22 = nu[5] / SCALE + SHIFT * nu[4]
    g11 = g02
    inv0 = 1.0 / g00
    l10 = g01 * inv0
    l20 = g02 * inv0
    d1 = g11 - l10 * g01
    ok1 = d1 > TINY * g11
    inv1 = jnp.where(ok1, 1.0 / jnp.where(ok1, d1, 1.0), 0.0)
    t = g12 - l20 * g01
    l21 = t * inv1
    d2 = g22 - l20 * g02 - l21 * t
    ok2 = ok1 & (d2 > TINY * g22)
    inv2 = jnp.where(ok2, 1.0 / jnp.where(ok2, d2, 1.0), 0.0)
    y1 = nu[1] - l10 * nu[0]
    y2 = nu[2] - l20 * nu[0] - l21 * y1
    c2 = y2 * inv2
    c1 = y1 * inv1 - l21 * c2
    c0 = nu[0] * inv0 - l10 * c1 - l20 * c2
    return c0, c1, c2


def kernel(nx, ny, term_ref, dens_ref, guess_ref, diag_ref, both_ref,
           main, left, right, rim, edge, edge_left, edge_right, sent, slots, sizes, halo_send, halo_recv, own_sem, sum_send, sum_recv,
           ready, scaled_tall, scaled_mid, scaled_small):
    rows, cols = term_ref.shape
    gx = lax.axis_index("gx")
    gy = lax.axis_index("gy")
    count = nx * ny
    me = gx * ny + gy

    def inside(dr, dc):
        ok = None
        for here_at, step, size in ((gx, dr, nx), (gy, dc, ny)):
            if step == 1:
                test = here_at < size - 1
            elif step == -1:
                test = here_at > 0
            else:
                continue
            ok = test if ok is None else ok & test
        return ok

    def across(k):
        return (lax.rem(gx + k, nx), gy)

    def along(k):
        return (gx, lax.rem(gy + k, ny))

    barrier = pltpu.get_barrier_semaphore()
    greeted = nx + ny - 2
    for dr, dc in DIRECTIONS:
        if dr != 0 and dc != 0:
            there = inside(dr, dc)
            greeted = greeted + jnp.where(there, 1, 0)

            @pl.when(there)
            def _():
                pl.semaphore_signal(
                    barrier, inc=1, device_id=(gx + dr, gy + dc), device_id_type=MESH)

    for k in range(1, ny):
        pl.semaphore_signal(barrier, inc=1, device_id=along(k), device_id_type=MESH)
    for k in range(1, nx):
        pl.semaphore_signal(barrier, inc=1, device_id=across(k), device_id_type=MESH)

    here = pl.ds(MARGIN, rows)
    own = [
        pltpu.make_async_copy(source, main.at[at, here], own_sem)
        for at, source in enumerate(
            (term_ref, diag_ref, guess_ref.at[1], guess_ref.at[0], dens_ref))
    ]
    for copy in own:
        copy.start()
    wide = cols + LANES
    half = LANES // 2
    tall = rows + 2 * MARGIN
    low_mid, high_mid = MARGIN - 8, MARGIN + rows + 8

    def mask_of(size, cyclic, margin):
        row = lax.broadcasted_iota(jnp.int32, (size, wide), 0)
        col = lax.broadcasted_iota(jnp.int32, (size, wide), 1)
        col_low = jnp.where(gy < ny - 1, cols + half, cols)
        col_high = jnp.where(gy > 0, cols + half, wide)
        ok = (col < col_low) | (col >= col_high)
        if cyclic:
            row_low = jnp.where(gx < nx - 1, rows + 4, rows)
            row_high = jnp.where(gx > 0, rows + 4, size)
            return ok & ((row < row_low) | (row >= row_high))
        row_low = jnp.where(gx > 0, 0, margin)
        row_high = jnp.where(gx < nx - 1, size, margin + rows)
        return ok & (row >= row_low) & (row < row_high)

    scaled = {"tall": scaled_tall, "mid": scaled_mid, "small": scaled_small}
    scaled_tall[...] = jnp.where(mask_of(tall, False, MARGIN), SCALE, 0.0)
    scaled_mid[...] = jnp.where(mask_of(rows + 16, False, 8), SCALE, 0.0)
    scaled_small[...] = jnp.where(mask_of(rows + 8, True, 4), SCALE, 0.0)

    pltpu.make_async_copy(main.at[:, here], main.at[:, here], own_sem).wait()
    for part in range(3):
        for a in range(4 if part == 2 else 3):
            rim[part, 0, a] = main[a, MARGIN + 4 * part:MARGIN + 4 * part + 4]
            rim[part, 1, a] = main[a, MARGIN + rows - 4 * part - 4:MARGIN + rows - 4 * part]
    pl.semaphore_wait(barrier, greeted)

    def pieces(dr, stage):
        if dr == 0:
            return [[(0, 3, 0, rows)], [], [(3, 2, 0, rows)]][stage]
        return [
            [(0, 3, 0, 4)],
            [(0, 3, 4, 4), (1, 2, 8, 4), (0, 1, 8, 8)],
            [(3, 2, 0, 8), (3, 1, 8, 4)],
        ][stage]

    def halo(d, stage, piece):
        dr, dc = DIRECTIONS[d]
        first, many, out, size = piece
        if dr == 0:
            src_rows, dst_rows = here, here
        elif dr == 1:
            src_rows = pl.ds(MARGIN + rows - out - size, size)
            dst_rows = pl.ds(MARGIN - out - size, size)
        else:
            src_rows = pl.ds(MARGIN + out, size)
            dst_rows = pl.ds(MARGIN + rows + out, size)
        if dc == 0:
            src_cols, buf, rim_buf = pl.ds(0, cols), main, edge
        elif dc == 1:
            src_cols, buf, rim_buf = pl.ds(cols - LANES, LANES), left, edge_left
        else:
            src_cols, buf, rim_buf = pl.ds(0, LANES), right, edge_right
        src = main.at[pl.ds(first, many), src_rows, src_cols]
        dst = buf.at[pl.ds(first, many), dst_rows, :]
        if size == 4:
            side = 1 if dr == 1 else 0
            src = rim.at[out // 4, side, pl.ds(first, many), :, src_cols]
            dst = rim_buf.at[out // 4, side, pl.ds(first, many)]
        return pltpu.make_async_remote_copy(
            src_ref=src, dst_ref=dst,
            send_sem=halo_send, recv_sem=halo_recv.at[stage],
            device_id=(gx + dr, gy + dc), device_id_type=MESH)

    def start_halo(stage):
        for d, (dr, dc) in enumerate(DIRECTIONS):
            if pieces(dr, stage):
                @pl.when(inside(dr, dc))
                def _():
                    for piece in pieces(dr, stage):
                        halo(d, stage, piece).start()

    def tiles(ends, sides, stages):
        total = 0
        for dr, dc in ((1, 0), (0, 1), (1, 1)):
            times = (ends if dr else 1) * (sides if dc else 1)
            for stage in stages:
                for _, many, _, size in pieces(dr, stage):
                    total += times * many * (size // 4) * (1 if dc else cols // LANES)
        return total

    def beside_count(here_at, size):
        return jnp.where(here_at > 0, 1, 0) + jnp.where(here_at < size - 1, 1, 0)

    def wait_halo(sem, *stages):
        for ends in range(min(1, nx - 1), min(2, nx - 1) + 1):
            for sides in range(min(1, ny - 1), min(2, ny - 1) + 1):
                many = tiles(ends, sides, stages)
                if many == 0:
                    continue

                @pl.when((beside_count(gx, nx) == ends) & (beside_count(gy, ny) == sides))
                def _():
                    span = sizes.at[pl.ds(0, many)]
                    pltpu.make_async_copy(span, span, sem).wait()

    start_halo(0)
    for k in range(1, nx):
        pl.semaphore_signal(ready, inc=1, device_id=across(k), device_id_type=MESH)
    start_halo(1)
    start_halo(2)

    def shrink(x, start):
        sub = lax.broadcasted_iota(jnp.int32, (8, x.shape[1]), 0)
        ends = jnp.where(sub < 4, x[start + rows:start + rows + 8], x[start - 8:start])
        return jnp.concatenate([x[start:start + rows], ends], axis=0)

    def joined(x, from_right, from_left):
        lane = lax.broadcasted_iota(jnp.int32, from_right.shape, 1)
        return jnp.concatenate([x, jnp.where(lane < half, from_right, from_left)], axis=1)

    def strip(a, begin, end):
        return joined(main[a, begin:end], right[a, begin:end], left[a, begin:end])

    def rims(a, one, other):
        return joined(*(
            jnp.concatenate([buf[part, side, a] for part, side in (one, other)], axis=0)
            for buf in (edge, edge_right, edge_left)))

    def field(a, window):
        if a > 2:
            x = strip(a, low_mid, high_mid)
            if window == "tall":
                return jnp.concatenate(
                    [rims(a, (2, 1), (2, 1)), x, rims(a, (2, 0), (2, 0))], axis=0)
            return x if window == "mid" else shrink(x, 8)
        own_rows = strip(a, MARGIN, MARGIN + rows)
        if window == "small":
            return jnp.concatenate([own_rows, rims(a, (0, 0), (0, 1))], axis=0)
        above, below = rims(a, (1, 1), (0, 1)), rims(a, (0, 0), (1, 0))
        x = [above, own_rows, below]
        if window == "tall" and a == 0:
            x = [strip(a, 0, low_mid)] + x + [strip(a, high_mid, tall)]
        elif window == "tall":
            x = [rims(a, (2, 1), (2, 1))] + x + [rims(a, (2, 0), (2, 0))]
        return jnp.concatenate(x, axis=0)

    def up(x):
        return pltpu.roll(x, 1, 0)

    def down(x):
        return pltpu.roll(x, x.shape[0] - 1, 0)

    def before(x):
        return pltpu.roll(x, 1, 1)

    def after(x):
        return pltpu.roll(x, x.shape[1] - 1, 1)

    def masked(x, window):
        return jnp.where(scaled[window][...] > 0.0, x, 0.0)

    def core_of(window):
        return masked(SCALE * (field(1, window) + (inv_step + 4.0 - SHIFT)), window)

    def apply_b(v, core, window):
        beside = (up(v) + down(v)) + (before(v) + after(v))
        return core * v - scaled[window][...] * beside

    def apply_half(v, core):
        return (0.5 * core) * v - SCALE * (down(v) + after(v))

    def slopes(u):
        return u - up(u), down(u) - u, u - before(u), after(u) - u

    def hamiltonian(slope):
        back_x, ahead_x, back_y, ahead_y = slope
        px, qx = jnp.maximum(back_x, 0.0), jnp.minimum(ahead_x, 0.0)
        py, qy = jnp.maximum(back_y, 0.0), jnp.minimum(ahead_y, 0.0)
        return (px * px + qx * qx) + (py * py + qy * qy)

    def falls(u):
        return u - down(u), u - after(u)

    def faces(fall):
        sx, sy = fall
        return jnp.maximum(sx, 0.0), jnp.minimum(sx, 0.0), jnp.maximum(sy, 0.0), jnp.minimum(sy, 0.0)

    def ahead(m):
        return m, down(m), after(m)

    def unit(window):
        return (1.0 / SCALE) * scaled[window][...]

    def advance(m_ahead, face, ones, face_behind=None):
        m, below, beyond = m_ahead
        px, qx, py, qy = face
        fx = px * m + qx * below
        fy = py * m + qy * beyond
        if face_behind is None:
            fy_behind = before(fy)
        else:
            fy_behind = face_behind[0] * before(m) + face_behind[1] * m
        net = (fx - up(fx)) + (fy - fy_behind)
        return inv_step * m - ones * net

    def own_guess(level, window):
        return masked(coupling * field(2 if level == 1 else 3, window), window)

    def value_rhs(later, slope, guess, ones):
        return (inv_step * later + guess) - (0.5 * ones) * hamiltonian(slope)

    def tree(parts):
        while len(parts) > 1:
            odd = parts[len(parts) // 2 * 2:]
            parts = [parts[i] + parts[i + 1] for i in range(0, len(parts) - 1, 2)] + odd
        return parts[0]

    def fold(p):
        return tree([p[i:i + 8, j:j + LANES] for i in range(0, rows, 8) for j in range(0, cols, LANES)])

    def dot(x, y):
        return fold(x * y)

    sub8 = lax.broadcasted_iota(jnp.int32, (8, LANES), 0)
    lane8 = lax.broadcasted_iota(jnp.int32, (8, LANES), 1)

    def pack(tiles):
        spread = None
        for first in range(0, len(tiles), 8):
            group = tiles[first:first + 8]
            group = group + [jnp.zeros((8, LANES), jnp.float32)] * (8 - len(group))
            for step in (4, 2, 1):
                keep = lax.rem(sub8, 2 * step) < step
                group = [
                    jnp.where(keep, a + pltpu.roll(a, 8 - step, 0), b + pltpu.roll(b, step, 0))
                    for a, b in zip(group[:step], group[step:])
                ]
            sums = jnp.sum(group[0], axis=1, keepdims=True)
            part = jnp.where(lane8 == sub8 + first, sums, 0.0)
            spread = part if spread is None else spread + part
        return jnp.sum(spread, axis=0, keepdims=True)

    def send_sums(which, values):
        packed = pack(values)
        sent[which] = packed
        slots[which, me] = packed

        def send(px, py):
            pltpu.make_async_remote_copy(
                src_ref=sent.at[which], dst_ref=slots.at[which, me],
                send_sem=sum_send, recv_sem=sum_recv.at[which % 2],
                device_id=(px, py), device_id_type=MESH).start()

        for begin in (2, 1):
            def column(j, carry):
                for k in sorted(range(begin, nx, 2), key=lambda k: min(k, nx - k)):
                    send(lax.rem(gx + k, nx), jnp.where(2 * gy < ny, ny - 1 - j, j))
                return carry

            lax.fori_loop(0, ny, column, 0)
        for k in range(1, ny):
            send(gx, lax.rem(gy + k, ny))

    def take_sums(which, many):
        others = slots.at[which, pl.ds(0, count - 1)]
        pltpu.make_async_copy(others, others, sum_recv.at[which % 2]).wait()
        total = jnp.broadcast_to(tree([slots[which, k] for k in range(count)]), (8, LANES))
        return [jnp.broadcast_to(total[:, k:k + 1], (8, LANES)) for k in range(many)]

    def basis(b, core, window, last=True):
        v1 = apply_b(b, core, window)
        v2 = apply_b(v1, core, window)
        return (b, v1, v2, apply_half(v2, core)) if last else (b, v1, v2)

    def spread(tile, like):
        wide_tile = jnp.concatenate([tile] * (like.shape[1] // LANES), axis=1)
        return jnp.concatenate([wide_tile] * (like.shape[0] // 8), axis=0)

    def mix(c, v):
        parts = [spread(a, x) * x for a, x in zip(c, v)]
        return (parts[0] + parts[1]) + parts[2]

    def pairs(x, y):
        return [dot(x[0], y[0]), dot(x[0], y[1]), dot(x[1], y[1]),
                dot(x[1], y[2]), dot(x[2], y[2]),
                2.0 * dot(x[2], x[3]) if x is y
                else fold(x[2] * y[3] + y[2] * x[3])]

    def own_small(v):
        return [x[:rows, :cols] for x in v]

    wait_halo(halo_recv.at[0], 0)
    small_core = core_of("small")
    small_ones = unit("small")
    later = masked(field(0, "small"), "small")
    w = own_small(basis(
        value_rhs(later, slopes(later), own_guess(1, "small"), small_ones), small_core, "small"))
    moments = pairs(w, w)
    pl.semaphore_wait(ready, nx - 1)
    send_sums(0, moments)
    wait_halo(halo_recv.at[1], 1)
    core, ones = core_of("tall"), unit("tall")
    later = masked(field(0, "tall"), "tall")
    v = basis(
        value_rhs(later, slopes(later), own_guess(1, "tall"), ones), core, "tall", last=False)
    vs = [shrink(x, MARGIN) for x in v]
    steep = list(zip(*[slopes(x) for x in vs]))
    wait_halo(halo_recv.at[2], 2)
    guess = own_guess(0, "small")
    c = solve_small(take_sums(0, 6))

    first_small = mix(c, vs)
    w = own_small(basis(
        value_rhs(first_small, [mix(c, x) for x in steep], guess, small_ones), small_core, "small"))
    send_sums(1, pairs(w, w))
    first = mix(c, v)
    v = basis(value_rhs(first, slopes(first), own_guess(0, "tall"), ones), core, "tall", last=False)
    v = [x[low_mid:high_mid] for x in v]
    steep = list(zip(*[falls(x) for x in v]))
    face = faces(falls(first_small))
    behind = before(face[2]), before(face[3])
    density = ahead(masked(field(4, "mid"), "mid"))
    mid_core, mid_ones = core_of("mid"), unit("mid")
    c = solve_small(take_sums(1, 6))

    rhs = advance(density, faces([mix(c, x) for x in steep]), mid_ones)
    a = basis(rhs, mid_core, "mid", last=False)
    a = [shrink(x, 8) for x in a]
    last = apply_half(a[2], small_core)
    inner = own_small(a + [last])
    families = [
        own_small(basis(
            advance(ahead(x), face, small_ones, behind if x is a[2] else None), small_core, "small"))
        for x in a]
    moments = pairs(inner, inner)
    for i in range(3):
        for j in range(i, 3):
            moments += pairs(families[i], families[j])
    send_sums(2, moments)
    both_ref[0] = mix(c, [x[8:8 + rows, :cols] for x in v])
    wait_halo(halo_send, 0, 1, 2)
    others = slots.at[:, pl.ds(0, count - 1)]
    pltpu.make_async_copy(others, others, sum_send).wait()
    total = take_sums(2, len(moments))
    c = solve_small(total[:6])
    picks = [(i, j) for i in range(3) for j in range(i, 3)]
    weights = [c[i] * c[j] * (1.0 if i == j else 2.0) for i, j in picks]
    nu = [
        tree([weight * total[6 + 6 * at + k] for at, weight in enumerate(weights)])
        for k in range(6)
    ]
    e = solve_small(nu)
    result = mix(e, [mix(c, [families[i][k] for i in range(3)]) for k in range(3)])
    both_ref[1] = result


def solution(mesh):
    nx, ny = mesh.shape["gx"], mesh.shape["gy"]

    def shards(terminal, initial_density, density_guess, diagonal):
        rows, cols = terminal.shape
        tall = rows + 2 * MARGIN
        hbm = pl.BlockSpec(memory_space=pl.ANY)
        vmem = pl.BlockSpec(memory_space=pltpu.VMEM)
        shape = jax.ShapeDtypeStruct((rows, cols), jnp.float32)
        both = pl.pallas_call(
            functools.partial(kernel, nx, ny),
            out_shape=jax.ShapeDtypeStruct((2, rows, cols), jnp.float32),
            in_specs=[hbm] * 4,
            out_specs=vmem,
            scratch_shapes=[
                pltpu.VMEM((5, tall, cols), jnp.float32),
                pltpu.VMEM((5, tall, LANES), jnp.float32),
                pltpu.VMEM((5, tall, LANES), jnp.float32),
                pltpu.VMEM((3, 2, 4, 4, cols), jnp.float32),
                pltpu.VMEM((3, 2, 4, 4, cols), jnp.float32),
                pltpu.VMEM((3, 2, 4, 4, LANES), jnp.float32),
                pltpu.VMEM((3, 2, 4, 4, LANES), jnp.float32),
                pltpu.VMEM((3, 1, LANES), jnp.float32),
                pltpu.VMEM((3, nx * ny, 1, LANES), jnp.float32),
                pltpu.VMEM((10 * 4 * (rows // 8 + 2) * (cols // LANES + 2), 4, LANES), jnp.float32),
                pltpu.SemaphoreType.DMA,
                pltpu.SemaphoreType.DMA((3,)),
                pltpu.SemaphoreType.DMA,
                pltpu.SemaphoreType.DMA,
                pltpu.SemaphoreType.DMA((2,)),
                pltpu.SemaphoreType.REGULAR,
                pltpu.VMEM((tall, cols + LANES), jnp.float32),
                pltpu.VMEM((rows + 16, cols + LANES), jnp.float32),
                pltpu.VMEM((rows + 8, cols + LANES), jnp.float32),
            ],
            compiler_params=pltpu.CompilerParams(collective_id=0, has_side_effects=True, vmem_limit_bytes=8 * 1024 * 1024),
        )(*[pltpu.with_memory_space_constraint(x, pltpu.HBM) for x in (terminal, initial_density, density_guess, diagonal)])
        return both[0], both[1]

    placed = (P("gx", "gy"), P("gx", "gy"), P(None, "gx", "gy"), P("gx", "gy"))
    return jax.shard_map(
        shards,
        mesh=mesh,
        in_specs=placed,
        out_specs=(P("gx", "gy"), P("gx", "gy")),
        check_vma=False,
    )
```

```python
import functools

import jax
import jax.numpy as jnp
from jax import lax
from jax.experimental import pallas as pl
from jax.experimental.pallas import tpu as pltpu
from jax.sharding import PartitionSpec as P

MESH = pl.DeviceIdType.MESH

LEVELS = 2
MARGIN = 16
LANES = 128

inv_step = 0.5
coupling = 0.5

SCALE = 0.25
SHIFT = 5.5

CORNERS = [(r, c) for r in (-1, 1) for c in (-1, 1)]
DIRECTIONS = [(-1, 0), (1, 0)] + CORNERS + [(0, -1), (0, 1)]
TINY = 2e-7


def solve_small(nu):
    g00 = nu[1] / SCALE + SHIFT * nu[0]
    g01 = nu[2] / SCALE + SHIFT * nu[1]
    g02 = nu[3] / SCALE + SHIFT * nu[2]
    g12 = nu[4] / SCALE + SHIFT * nu[3]
    g22 = nu[5] / SCALE + SHIFT * nu[4]
    g11 = g02
    inv0 = 1.0 / g00
    l10 = g01 * inv0
    l20 = g02 * inv0
    d1 = g11 - l10 * g01
    ok1 = d1 > TINY * g11
    inv1 = jnp.where(ok1, 1.0 / jnp.where(ok1, d1, 1.0), 0.0)
    t = g12 - l20 * g01
    l21 = t * inv1
    d2 = g22 - l20 * g02 - l21 * t
    ok2 = ok1 & (d2 > TINY * g22)
    inv2 = jnp.where(ok2, 1.0 / jnp.where(ok2, d2, 1.0), 0.0)
    y1 = nu[1] - l10 * nu[0]
    y2 = nu[2] - l20 * nu[0] - l21 * y1
    c2 = y2 * inv2
    c1 = y1 * inv1 - l21 * c2
    c0 = nu[0] * inv0 - l10 * c1 - l20 * c2
    return c0, c1, c2


def kernel(nx, ny, term_ref, dens_ref, guess_ref, diag_ref, both_ref,
           main, left, right, rim, edge, edge_left, edge_right, sent, slots, sizes, halo_send, halo_recv, own_sem, sum_send, sum_recv,
           ready, scaled_tall, scaled_mid, scaled_small):
    rows, cols = term_ref.shape
    gx = lax.axis_index("gx")
    gy = lax.axis_index("gy")
    count = nx * ny
    me = gx * ny + gy

    def inside(dr, dc):
        ok = None
        for here_at, step, size in ((gx, dr, nx), (gy, dc, ny)):
            if step == 1:
                test = here_at < size - 1
            elif step == -1:
                test = here_at > 0
            else:
                continue
            ok = test if ok is None else ok & test
        return ok

    def across(k):
        return (lax.rem(gx + k, nx), gy)

    def along(k):
        return (gx, lax.rem(gy + k, ny))

    barrier = pltpu.get_barrier_semaphore()
    greeted = nx + ny - 2
    for dr, dc in DIRECTIONS:
        if dr != 0 and dc != 0:
            there = inside(dr, dc)
            greeted = greeted + jnp.where(there, 1, 0)

            @pl.when(there)
            def _():
                pl.semaphore_signal(
                    barrier, inc=1, device_id=(gx + dr, gy + dc), device_id_type=MESH)

    for k in range(1, ny):
        pl.semaphore_signal(barrier, inc=1, device_id=along(k), device_id_type=MESH)
    for k in range(1, nx):
        pl.semaphore_signal(barrier, inc=1, device_id=across(k), device_id_type=MESH)

    here = pl.ds(MARGIN, rows)
    own = [
        pltpu.make_async_copy(source, main.at[at, here], own_sem)
        for at, source in enumerate(
            (term_ref, diag_ref, guess_ref.at[1], guess_ref.at[0], dens_ref))
    ]
    for copy in own:
        copy.start()
    wide = cols + LANES
    half = LANES // 2
    tall = rows + 2 * MARGIN
    low_mid, high_mid = MARGIN - 8, MARGIN + rows + 8

    def mask_of(size, cyclic, margin):
        row = lax.broadcasted_iota(jnp.int32, (size, wide), 0)
        col = lax.broadcasted_iota(jnp.int32, (size, wide), 1)
        col_low = jnp.where(gy < ny - 1, cols + half, cols)
        col_high = jnp.where(gy > 0, cols + half, wide)
        ok = (col < col_low) | (col >= col_high)
        if cyclic:
            row_low = jnp.where(gx < nx - 1, rows + 4, rows)
            row_high = jnp.where(gx > 0, rows + 4, size)
            return ok & ((row < row_low) | (row >= row_high))
        row_low = jnp.where(gx > 0, 0, margin)
        row_high = jnp.where(gx < nx - 1, size, margin + rows)
        return ok & (row >= row_low) & (row < row_high)

    scaled = {"tall": scaled_tall, "mid": scaled_mid, "small": scaled_small}
    scaled_tall[...] = jnp.where(mask_of(tall, False, MARGIN), SCALE, 0.0)
    scaled_mid[...] = jnp.where(mask_of(rows + 16, False, 8), SCALE, 0.0)
    scaled_small[...] = jnp.where(mask_of(rows + 8, True, 4), SCALE, 0.0)

    pltpu.make_async_copy(main.at[:, here], main.at[:, here], own_sem).wait()
    for part in range(3):
        for a in range(4 if part == 2 else 3):
            rim[part, 0, a] = main[a, MARGIN + 4 * part:MARGIN + 4 * part + 4]
            rim[part, 1, a] = main[a, MARGIN + rows - 4 * part - 4:MARGIN + rows - 4 * part]
    pl.semaphore_wait(barrier, greeted)

    def pieces(dr, stage):
        if dr == 0:
            return [[(0, 3, 0, rows)], [], [(3, 2, 0, rows)]][stage]
        return [
            [(0, 3, 0, 4)],
            [(0, 3, 4, 4), (1, 2, 8, 4), (0, 1, 8, 8)],
            [(3, 2, 0, 8), (3, 1, 8, 4)],
        ][stage]

    def halo(d, stage, piece):
        dr, dc = DIRECTIONS[d]
        first, many, out, size = piece
        if dr == 0:
            src_rows, dst_rows = here, here
        elif dr == 1:
            src_rows = pl.ds(MARGIN + rows - out - size, size)
            dst_rows = pl.ds(MARGIN - out - size, size)
        else:
            src_rows = pl.ds(MARGIN + out, size)
            dst_rows = pl.ds(MARGIN + rows + out, size)
        if dc == 0:
            src_cols, buf, rim_buf = pl.ds(0, cols), main, edge
        elif dc == 1:
            src_cols, buf, rim_buf = pl.ds(cols - LANES, LANES), left, edge_left
        else:
            src_cols, buf, rim_buf = pl.ds(0, LANES), right, edge_right
        src = main.at[pl.ds(first, many), src_rows, src_cols]
        dst = buf.at[pl.ds(first, many), dst_rows, :]
        if size == 4:
            side = 1 if dr == 1 else 0
            src = rim.at[out // 4, side, pl.ds(first, many), :, src_cols]
            dst = rim_buf.at[out // 4, side, pl.ds(first, many)]
        return pltpu.make_async_remote_copy(
            src_ref=src, dst_ref=dst,
            send_sem=halo_send, recv_sem=halo_recv.at[stage],
            device_id=(gx + dr, gy + dc), device_id_type=MESH)

    def start_halo(stage):
        for d, (dr, dc) in enumerate(DIRECTIONS):
            if pieces(dr, stage):
                @pl.when(inside(dr, dc))
                def _():
                    for piece in pieces(dr, stage):
                        halo(d, stage, piece).start()

    def tiles(ends, sides, stages):
        total = 0
        for dr, dc in ((1, 0), (0, 1), (1, 1)):
            times = (ends if dr else 1) * (sides if dc else 1)
            for stage in stages:
                for _, many, _, size in pieces(dr, stage):
                    total += times * many * (size // 4) * (1 if dc else cols // LANES)
        return total

    def beside_count(here_at, size):
        return jnp.where(here_at > 0, 1, 0) + jnp.where(here_at < size - 1, 1, 0)

    def wait_halo(sem, *stages):
        for ends in range(min(1, nx - 1), min(2, nx - 1) + 1):
            for sides in range(min(1, ny - 1), min(2, ny - 1) + 1):
                many = tiles(ends, sides, stages)
                if many == 0:
                    continue

                @pl.when((beside_count(gx, nx) == ends) & (beside_count(gy, ny) == sides))
                def _():
                    span = sizes.at[pl.ds(0, many)]
                    pltpu.make_async_copy(span, span, sem).wait()

    start_halo(0)
    for k in range(1, nx):
        pl.semaphore_signal(ready, inc=1, device_id=across(k), device_id_type=MESH)
    start_halo(1)
    start_halo(2)

    def shrink(x, start):
        sub = lax.broadcasted_iota(jnp.int32, (8, x.shape[1]), 0)
        ends = jnp.where(sub < 4, x[start + rows:start + rows + 8], x[start - 8:start])
        return jnp.concatenate([x[start:start + rows], ends], axis=0)

    def joined(x, from_right, from_left):
        lane = lax.broadcasted_iota(jnp.int32, from_right.shape, 1)
        return jnp.concatenate([x, jnp.where(lane < half, from_right, from_left)], axis=1)

    def strip(a, begin, end):
        return joined(main[a, begin:end], right[a, begin:end], left[a, begin:end])

    def rims(a, one, other):
        return joined(*(
            jnp.concatenate([buf[part, side, a] for part, side in (one, other)], axis=0)
            for buf in (edge, edge_right, edge_left)))

    def field(a, window):
        if a > 2:
            x = strip(a, low_mid, high_mid)
            if window == "tall":
                return jnp.concatenate(
                    [rims(a, (2, 1), (2, 1)), x, rims(a, (2, 0), (2, 0))], axis=0)
            return x if window == "mid" else shrink(x, 8)
        own_rows = strip(a, MARGIN, MARGIN + rows)
        if window == "small":
            return jnp.concatenate([own_rows, rims(a, (0, 0), (0, 1))], axis=0)
        above, below = rims(a, (1, 1), (0, 1)), rims(a, (0, 0), (1, 0))
        x = [above, own_rows, below]
        if window == "tall" and a == 0:
            x = [strip(a, 0, low_mid)] + x + [strip(a, high_mid, tall)]
        elif window == "tall":
            x = [rims(a, (2, 1), (2, 1))] + x + [rims(a, (2, 0), (2, 0))]
        return jnp.concatenate(x, axis=0)

    def up(x):
        return pltpu.roll(x, 1, 0)

    def down(x):
        return pltpu.roll(x, x.shape[0] - 1, 0)

    def before(x):
        return pltpu.roll(x, 1, 1)

    def after(x):
        return pltpu.roll(x, x.shape[1] - 1, 1)

    def masked(x, window):
        return jnp.where(scaled[window][...] > 0.0, x, 0.0)

    def core_of(window):
        return masked(SCALE * (field(1, window) + (inv_step + 4.0 - SHIFT)), window)

    def apply_b(v, core, window):
        beside = (up(v) + down(v)) + (before(v) + after(v))
        return core * v - scaled[window][...] * beside

    def apply_half(v, core):
        return (0.5 * core) * v - SCALE * (down(v) + after(v))

    def slopes(u):
        return u - up(u), down(u) - u, u - before(u), after(u) - u

    def hamiltonian(slope):
        back_x, ahead_x, back_y, ahead_y = slope
        px, qx = jnp.maximum(back_x, 0.0), jnp.minimum(ahead_x, 0.0)
        py, qy = jnp.maximum(back_y, 0.0), jnp.minimum(ahead_y, 0.0)
        return (px * px + qx * qx) + (py * py + qy * qy)

    def falls(u):
        return u - down(u), u - after(u)

    def faces(fall):
        sx, sy = fall
        return jnp.maximum(sx, 0.0), jnp.minimum(sx, 0.0), jnp.maximum(sy, 0.0), jnp.minimum(sy, 0.0)

    def ahead(m):
        return m, down(m), after(m)

    def unit(window):
        return (1.0 / SCALE) * scaled[window][...]

    def advance(m_ahead, face, ones, face_behind=None):
        m, below, beyond = m_ahead
        px, qx, py, qy = face
        fx = px * m + qx * below
        fy = py * m + qy * beyond
        if face_behind is None:
            fy_behind = before(fy)
        else:
            fy_behind = face_behind[0] * before(m) + face_behind[1] * m
        net = (fx - up(fx)) + (fy - fy_behind)
        return inv_step * m - ones * net

    def own_guess(level, window):
        return masked(coupling * field(2 if level == 1 else 3, window), window)

    def value_rhs(later, slope, guess, ones):
        return (inv_step * later + guess) - (0.5 * ones) * hamiltonian(slope)

    def tree(parts):
        while len(parts) > 1:
            odd = parts[len(parts) // 2 * 2:]
            parts = [parts[i] + parts[i + 1] for i in range(0, len(parts) - 1, 2)] + odd
        return parts[0]

    def fold(p):
        return tree([p[i:i + 8, j:j + LANES] for i in range(0, rows, 8) for j in range(0, cols, LANES)])

    def dot(x, y):
        return fold(x * y)

    sub8 = lax.broadcasted_iota(jnp.int32, (8, LANES), 0)
    lane8 = lax.broadcasted_iota(jnp.int32, (8, LANES), 1)

    def pack(tiles):
        spread = None
        for first in range(0, len(tiles), 8):
            group = tiles[first:first + 8]
            group = group + [jnp.zeros((8, LANES), jnp.float32)] * (8 - len(group))
            for step in (4, 2, 1):
                keep = lax.rem(sub8, 2 * step) < step
                group = [
                    jnp.where(keep, a + pltpu.roll(a, 8 - step, 0), b + pltpu.roll(b, step, 0))
                    for a, b in zip(group[:step], group[step:])
                ]
            sums = jnp.sum(group[0], axis=1, keepdims=True)
            part = jnp.where(lane8 == sub8 + first, sums, 0.0)
            spread = part if spread is None else spread + part
        return jnp.sum(spread, axis=0, keepdims=True)

    def send_sums(which, values):
        packed = pack(values)
        sent[which] = packed
        slots[which, me] = packed

        def send(px, py):
            pltpu.make_async_remote_copy(
                src_ref=sent.at[which], dst_ref=slots.at[which, me],
                send_sem=sum_send, recv_sem=sum_recv.at[which % 2],
                device_id=(px, py), device_id_type=MESH).start()

        for begin in (2, 1):
            def column(j, carry):
                for k in sorted(range(begin, nx, 2), key=lambda k: min(k, nx - k)):
                    send(lax.rem(gx + k, nx), jnp.where(2 * gy < ny, ny - 1 - j, j))
                return carry

            lax.fori_loop(0, ny, column, 0, unroll=count <= 64)
        for k in range(1, ny):
            send(gx, lax.rem(gy + k, ny))

    def take_sums(which, many):
        others = slots.at[which, pl.ds(0, count - 1)]
        pltpu.make_async_copy(others, others, sum_recv.at[which % 2]).wait()
        total = jnp.broadcast_to(tree([slots[which, k] for k in range(count)]), (8, LANES))
        return [jnp.broadcast_to(total[:, k:k + 1], (8, LANES)) for k in range(many)]

    def basis(b, core, window, last=True):
        v1 = apply_b(b, core, window)
        v2 = apply_b(v1, core, window)
        return (b, v1, v2, apply_half(v2, core)) if last else (b, v1, v2)

    def spread(tile, like):
        wide_tile = jnp.concatenate([tile] * (like.shape[1] // LANES), axis=1)
        return jnp.concatenate([wide_tile] * (like.shape[0] // 8), axis=0)

    def mix(c, v):
        parts = [spread(a, x) * x for a, x in zip(c, v)]
        return (parts[0] + parts[1]) + parts[2]

    def pairs(x, y):
        return [dot(x[0], y[0]), dot(x[0], y[1]), dot(x[1], y[1]),
                dot(x[1], y[2]), dot(x[2], y[2]),
                2.0 * dot(x[2], x[3]) if x is y
                else fold(x[2] * y[3] + y[2] * x[3])]

    def own_small(v):
        return [x[:rows, :cols] for x in v]

    wait_halo(halo_recv.at[0], 0)
    small_core = core_of("small")
    small_ones = unit("small")
    later = masked(field(0, "small"), "small")
    w = own_small(basis(
        value_rhs(later, slopes(later), own_guess(1, "small"), small_ones), small_core, "small"))
    moments = pairs(w, w)
    pl.semaphore_wait(ready, nx - 1)
    send_sums(0, moments)
    wait_halo(halo_recv.at[1], 1)
    core, ones = core_of("tall"), unit("tall")
    later = masked(field(0, "tall"), "tall")
    v = basis(
        value_rhs(later, slopes(later), own_guess(1, "tall"), ones), core, "tall", last=False)
    vs = [shrink(x, MARGIN) for x in v]
    steep = list(zip(*[slopes(x) for x in vs]))
    wait_halo(halo_recv.at[2], 2)
    guess = own_guess(0, "small")
    c = solve_small(take_sums(0, 6))

    first_small = mix(c, vs)
    w = own_small(basis(
        value_rhs(first_small, [mix(c, x) for x in steep], guess, small_ones), small_core, "small"))
    send_sums(1, pairs(w, w))
    first = mix(c, v)
    v = basis(value_rhs(first, slopes(first), own_guess(0, "tall"), ones), core, "tall", last=False)
    v = [x[low_mid:high_mid] for x in v]
    steep = list(zip(*[falls(x) for x in v]))
    face = faces(falls(first_small))
    behind = before(face[2]), before(face[3])
    density = ahead(masked(field(4, "mid"), "mid"))
    mid_core, mid_ones = core_of("mid"), unit("mid")
    c = solve_small(take_sums(1, 6))

    rhs = advance(density, faces([mix(c, x) for x in steep]), mid_ones)
    a = basis(rhs, mid_core, "mid", last=False)
    a = [shrink(x, 8) for x in a]
    last = apply_half(a[2], small_core)
    inner = own_small(a + [last])
    families = [
        own_small(basis(
            advance(ahead(x), face, small_ones, behind if x is a[2] else None), small_core, "small"))
        for x in a]
    moments = pairs(inner, inner)
    for i in range(3):
        for j in range(i, 3):
            moments += pairs(families[i], families[j])
    send_sums(2, moments)
    both_ref[0] = mix(c, [x[8:8 + rows, :cols] for x in v])
    wait_halo(halo_send, 0, 1, 2)
    others = slots.at[:, pl.ds(0, count - 1)]
    pltpu.make_async_copy(others, others, sum_send).wait()
    total = take_sums(2, len(moments))
    c = solve_small(total[:6])
    picks = [(i, j) for i in range(3) for j in range(i, 3)]
    weights = [c[i] * c[j] * (1.0 if i == j else 2.0) for i, j in picks]
    nu = [
        tree([weight * total[6 + 6 * at + k] for at, weight in enumerate(weights)])
        for k in range(6)
    ]
    e = solve_small(nu)
    result = mix(e, [mix(c, [families[i][k] for i in range(3)]) for k in range(3)])
    both_ref[1] = result


def solution(mesh):
    nx, ny = mesh.shape["gx"], mesh.shape["gy"]

    def shards(terminal, initial_density, density_guess, diagonal):
        rows, cols = terminal.shape
        tall = rows + 2 * MARGIN
        hbm = pl.BlockSpec(memory_space=pl.ANY)
        vmem = pl.BlockSpec(memory_space=pltpu.VMEM)
        shape = jax.ShapeDtypeStruct((rows, cols), jnp.float32)
        both = pl.pallas_call(
            functools.partial(kernel, nx, ny),
            out_shape=jax.ShapeDtypeStruct((2, rows, cols), jnp.float32),
            in_specs=[hbm] * 4,
            out_specs=vmem,
            scratch_shapes=[
                pltpu.VMEM((5, tall, cols), jnp.float32),
                pltpu.VMEM((5, tall, LANES), jnp.float32),
                pltpu.VMEM((5, tall, LANES), jnp.float32),
                pltpu.VMEM((3, 2, 4, 4, cols), jnp.float32),
                pltpu.VMEM((3, 2, 4, 4, cols), jnp.float32),
                pltpu.VMEM((3, 2, 4, 4, LANES), jnp.float32),
                pltpu.VMEM((3, 2, 4, 4, LANES), jnp.float32),
                pltpu.VMEM((3, 1, LANES), jnp.float32),
                pltpu.VMEM((3, nx * ny, 1, LANES), jnp.float32),
                pltpu.VMEM((10 * 4 * (rows // 8 + 2) * (cols // LANES + 2), 4, LANES), jnp.float32),
                pltpu.SemaphoreType.DMA,
                pltpu.SemaphoreType.DMA((3,)),
                pltpu.SemaphoreType.DMA,
                pltpu.SemaphoreType.DMA,
                pltpu.SemaphoreType.DMA((2,)),
                pltpu.SemaphoreType.REGULAR,
                pltpu.VMEM((tall, cols + LANES), jnp.float32),
                pltpu.VMEM((rows + 16, cols + LANES), jnp.float32),
                pltpu.VMEM((rows + 8, cols + LANES), jnp.float32),
            ],
            compiler_params=pltpu.CompilerParams(collective_id=0, has_side_effects=True, vmem_limit_bytes=8 * 1024 * 1024),
        )(*[pltpu.with_memory_space_constraint(x, pltpu.HBM) for x in (terminal, initial_density, density_guess, diagonal)])
        return both[0], both[1]

    placed = (P("gx", "gy"), P("gx", "gy"), P(None, "gx", "gy"), P("gx", "gy"))
    return jax.shard_map(
        shards,
        mesh=mesh,
        in_specs=placed,
        out_specs=(P("gx", "gy"), P("gx", "gy")),
        check_vma=False,
    )
```

```python
import functools

import jax
import jax.numpy as jnp
from jax import lax
from jax.experimental import pallas as pl
from jax.experimental.pallas import tpu as pltpu
from jax.sharding import PartitionSpec as P

MESH = pl.DeviceIdType.MESH

LEVELS = 2
MARGIN = 16
LANES = 128

inv_step = 0.5
coupling = 0.5

SCALE = 0.25
SHIFT = 5.5

CORNERS = [(r, c) for r in (-1, 1) for c in (-1, 1)]
DIRECTIONS = [(-1, 0), (1, 0)] + CORNERS + [(0, -1), (0, 1)]
TINY = 2e-7


def solve_small(nu):
    g00 = nu[1] / SCALE + SHIFT * nu[0]
    g01 = nu[2] / SCALE + SHIFT * nu[1]
    g02 = nu[3] / SCALE + SHIFT * nu[2]
    g12 = nu[4] / SCALE + SHIFT * nu[3]
    g22 = nu[5] / SCALE + SHIFT * nu[4]
    g11 = g02
    inv0 = 1.0 / g00
    l10 = g01 * inv0
    l20 = g02 * inv0
    d1 = g11 - l10 * g01
    ok1 = d1 > TINY * g11
    inv1 = jnp.where(ok1, 1.0 / jnp.where(ok1, d1, 1.0), 0.0)
    t = g12 - l20 * g01
    l21 = t * inv1
    d2 = g22 - l20 * g02 - l21 * t
    ok2 = ok1 & (d2 > TINY * g22)
    inv2 = jnp.where(ok2, 1.0 / jnp.where(ok2, d2, 1.0), 0.0)
    y1 = nu[1] - l10 * nu[0]
    y2 = nu[2] - l20 * nu[0] - l21 * y1
    c2 = y2 * inv2
    c1 = y1 * inv1 - l21 * c2
    c0 = nu[0] * inv0 - l10 * c1 - l20 * c2
    return c0, c1, c2


def kernel(nx, ny, term_ref, dens_ref, guess_ref, diag_ref, both_ref,
           main, left, right, rim, edge, edge_left, edge_right, sent, slots, sizes, halo_send, halo_recv, own_sem, sum_send, sum_recv,
           ready, scaled_tall, scaled_mid, scaled_small):
    rows, cols = term_ref.shape
    gx = lax.axis_index("gx")
    gy = lax.axis_index("gy")
    count = nx * ny
    me = gx * ny + gy

    def inside(dr, dc):
        ok = None
        for here_at, step, size in ((gx, dr, nx), (gy, dc, ny)):
            if step == 1:
                test = here_at < size - 1
            elif step == -1:
                test = here_at > 0
            else:
                continue
            ok = test if ok is None else ok & test
        return ok

    def across(k):
        return (lax.rem(gx + k, nx), gy)

    def along(k):
        return (gx, lax.rem(gy + k, ny))

    barrier = pltpu.get_barrier_semaphore()
    greeted = nx + ny - 2
    for dr, dc in DIRECTIONS:
        if dr != 0 and dc != 0:
            there = inside(dr, dc)
            greeted = greeted + jnp.where(there, 1, 0)

            @pl.when(there)
            def _():
                pl.semaphore_signal(
                    barrier, inc=1, device_id=(gx + dr, gy + dc), device_id_type=MESH)

    for k in range(1, ny):
        pl.semaphore_signal(barrier, inc=1, device_id=along(k), device_id_type=MESH)
    for k in range(1, nx):
        pl.semaphore_signal(barrier, inc=1, device_id=across(k), device_id_type=MESH)

    here = pl.ds(MARGIN, rows)
    own = [
        pltpu.make_async_copy(source, main.at[at, here], own_sem)
        for at, source in enumerate(
            (term_ref, diag_ref, guess_ref.at[1], guess_ref.at[0], dens_ref))
    ]
    for copy in own:
        copy.start()
    wide = cols + LANES
    half = LANES // 2
    tall = rows + 2 * MARGIN
    low_mid, high_mid = MARGIN - 8, MARGIN + rows + 8

    def mask_of(size, cyclic, margin):
        row = lax.broadcasted_iota(jnp.int32, (size, wide), 0)
        col = lax.broadcasted_iota(jnp.int32, (size, wide), 1)
        col_low = jnp.where(gy < ny - 1, cols + half, cols)
        col_high = jnp.where(gy > 0, cols + half, wide)
        ok = (col < col_low) | (col >= col_high)
        if cyclic:
            row_low = jnp.where(gx < nx - 1, rows + 4, rows)
            row_high = jnp.where(gx > 0, rows + 4, size)
            return ok & ((row < row_low) | (row >= row_high))
        row_low = jnp.where(gx > 0, 0, margin)
        row_high = jnp.where(gx < nx - 1, size, margin + rows)
        return ok & (row >= row_low) & (row < row_high)

    scaled = {"tall": scaled_tall, "mid": scaled_mid, "small": scaled_small}
    scaled_tall[...] = jnp.where(mask_of(tall, False, MARGIN), SCALE, 0.0)
    scaled_mid[...] = jnp.where(mask_of(rows + 16, False, 8), SCALE, 0.0)
    scaled_small[...] = jnp.where(mask_of(rows + 8, True, 4), SCALE, 0.0)

    pltpu.make_async_copy(main.at[:, here], main.at[:, here], own_sem).wait()
    for part in range(3):
        for a in range(4 if part == 2 else 3):
            rim[part, 0, a] = main[a, MARGIN + 4 * part:MARGIN + 4 * part + 4]
            rim[part, 1, a] = main[a, MARGIN + rows - 4 * part - 4:MARGIN + rows - 4 * part]
    pl.semaphore_wait(barrier, greeted)

    def pieces(dr, stage):
        if dr == 0:
            return [[(0, 3, 0, rows)], [], [(3, 2, 0, rows)]][stage]
        return [
            [(0, 3, 0, 4)],
            [(0, 3, 4, 4), (1, 2, 8, 4), (0, 1, 8, 8)],
            [(3, 2, 0, 8), (3, 1, 8, 4)],
        ][stage]

    def halo(d, stage, piece):
        dr, dc = DIRECTIONS[d]
        first, many, out, size = piece
        if dr == 0:
            src_rows, dst_rows = here, here
        elif dr == 1:
            src_rows = pl.ds(MARGIN + rows - out - size, size)
            dst_rows = pl.ds(MARGIN - out - size, size)
        else:
            src_rows = pl.ds(MARGIN + out, size)
            dst_rows = pl.ds(MARGIN + rows + out, size)
        if dc == 0:
            src_cols, buf, rim_buf = pl.ds(0, cols), main, edge
        elif dc == 1:
            src_cols, buf, rim_buf = pl.ds(cols - LANES, LANES), left, edge_left
        else:
            src_cols, buf, rim_buf = pl.ds(0, LANES), right, edge_right
        src = main.at[pl.ds(first, many), src_rows, src_cols]
        dst = buf.at[pl.ds(first, many), dst_rows, :]
        if size == 4:
            side = 1 if dr == 1 else 0
            src = rim.at[out // 4, side, pl.ds(first, many), :, src_cols]
            dst = rim_buf.at[out // 4, side, pl.ds(first, many)]
        return pltpu.make_async_remote_copy(
            src_ref=src, dst_ref=dst,
            send_sem=halo_send, recv_sem=halo_recv.at[stage],
            device_id=(gx + dr, gy + dc), device_id_type=MESH)

    def start_halo(stage):
        for d, (dr, dc) in enumerate(DIRECTIONS):
            if pieces(dr, stage):
                @pl.when(inside(dr, dc))
                def _():
                    for piece in pieces(dr, stage):
                        halo(d, stage, piece).start()

    def tiles(ends, sides, stages):
        total = 0
        for dr, dc in ((1, 0), (0, 1), (1, 1)):
            times = (ends if dr else 1) * (sides if dc else 1)
            for stage in stages:
                for _, many, _, size in pieces(dr, stage):
                    total += times * many * (size // 4) * (1 if dc else cols // LANES)
        return total

    def beside_count(here_at, size):
        return jnp.where(here_at > 0, 1, 0) + jnp.where(here_at < size - 1, 1, 0)

    def wait_halo(sem, *stages):
        for ends in range(min(1, nx - 1), min(2, nx - 1) + 1):
            for sides in range(min(1, ny - 1), min(2, ny - 1) + 1):
                many = tiles(ends, sides, stages)
                if many == 0:
                    continue

                @pl.when((beside_count(gx, nx) == ends) & (beside_count(gy, ny) == sides))
                def _():
                    span = sizes.at[pl.ds(0, many)]
                    pltpu.make_async_copy(span, span, sem).wait()

    start_halo(0)
    for k in range(1, nx):
        pl.semaphore_signal(ready, inc=1, device_id=across(k), device_id_type=MESH)
    start_halo(1)
    start_halo(2)

    def shrink(x, start):
        sub = lax.broadcasted_iota(jnp.int32, (8, x.shape[1]), 0)
        ends = jnp.where(sub < 4, x[start + rows:start + rows + 8], x[start - 8:start])
        return jnp.concatenate([x[start:start + rows], ends], axis=0)

    def joined(x, from_right, from_left):
        lane = lax.broadcasted_iota(jnp.int32, from_right.shape, 1)
        return jnp.concatenate([x, jnp.where(lane < half, from_right, from_left)], axis=1)

    def strip(a, begin, end):
        return joined(main[a, begin:end], right[a, begin:end], left[a, begin:end])

    def rims(a, one, other):
        return joined(*(
            jnp.concatenate([buf[part, side, a] for part, side in (one, other)], axis=0)
            for buf in (edge, edge_right, edge_left)))

    def field(a, window):
        if a > 2:
            x = strip(a, low_mid, high_mid)
            if window == "tall":
                return jnp.concatenate(
                    [rims(a, (2, 1), (2, 1)), x, rims(a, (2, 0), (2, 0))], axis=0)
            return x if window == "mid" else shrink(x, 8)
        own_rows = strip(a, MARGIN, MARGIN + rows)
        if window == "small":
            return jnp.concatenate([own_rows, rims(a, (0, 0), (0, 1))], axis=0)
        above, below = rims(a, (1, 1), (0, 1)), rims(a, (0, 0), (1, 0))
        x = [above, own_rows, below]
        if window == "tall" and a == 0:
            x = [strip(a, 0, low_mid)] + x + [strip(a, high_mid, tall)]
        elif window == "tall":
            x = [rims(a, (2, 1), (2, 1))] + x + [rims(a, (2, 0), (2, 0))]
        return jnp.concatenate(x, axis=0)

    def up(x):
        return pltpu.roll(x, 1, 0)

    def down(x):
        return pltpu.roll(x, x.shape[0] - 1, 0)

    def before(x):
        return pltpu.roll(x, 1, 1)

    def after(x):
        return pltpu.roll(x, x.shape[1] - 1, 1)

    def masked(x, window):
        return jnp.where(scaled[window][...] > 0.0, x, 0.0)

    def core_of(window):
        return masked(SCALE * (field(1, window) + (inv_step + 4.0 - SHIFT)), window)

    def apply_b(v, core, window):
        beside = (up(v) + down(v)) + (before(v) + after(v))
        return core * v - scaled[window][...] * beside

    def apply_half(v, core):
        return (0.5 * core) * v - SCALE * (down(v) + after(v))

    def slopes(u):
        back = u - up(u)
        return back, down(back), u - before(u), after(u) - u

    def hamiltonian(slope):
        back_x, ahead_x, back_y, ahead_y = slope
        px, qx = jnp.maximum(back_x, 0.0), jnp.minimum(ahead_x, 0.0)
        py, qy = jnp.maximum(back_y, 0.0), jnp.minimum(ahead_y, 0.0)
        return (px * px + qx * qx) + (py * py + qy * qy)

    def falls(u):
        return u - down(u), u - after(u)

    def faces(fall):
        sx, sy = fall
        return jnp.maximum(sx, 0.0), jnp.minimum(sx, 0.0), jnp.maximum(sy, 0.0), jnp.minimum(sy, 0.0)

    def ahead(m):
        return m, down(m), after(m)

    def unit(window):
        return (1.0 / SCALE) * scaled[window][...]

    def advance(m_ahead, face, ones, face_behind=None):
        m, below, beyond = m_ahead
        px, qx, py, qy = face
        fx = px * m + qx * below
        fy = py * m + qy * beyond
        if face_behind is None:
            fy_behind = before(fy)
        else:
            fy_behind = face_behind[0] * before(m) + face_behind[1] * m
        net = (fx - up(fx)) + (fy - fy_behind)
        return inv_step * m - ones * net

    def own_guess(level, window):
        return masked(coupling * field(2 if level == 1 else 3, window), window)

    def value_rhs(later, slope, guess, ones):
        return (inv_step * later + guess) - (0.5 * ones) * hamiltonian(slope)

    def tree(parts):
        while len(parts) > 1:
            odd = parts[len(parts) // 2 * 2:]
            parts = [parts[i] + parts[i + 1] for i in range(0, len(parts) - 1, 2)] + odd
        return parts[0]

    def fold(p):
        return tree([p[i:i + 8, j:j + LANES] for i in range(0, rows, 8) for j in range(0, cols, LANES)])

    def dot(x, y):
        return fold(x * y)

    sub8 = lax.broadcasted_iota(jnp.int32, (8, LANES), 0)
    lane8 = lax.broadcasted_iota(jnp.int32, (8, LANES), 1)

    def pack(tiles):
        spread = None
        for first in range(0, len(tiles), 8):
            group = tiles[first:first + 8]
            group = group + [jnp.zeros((8, LANES), jnp.float32)] * (8 - len(group))
            for step in (4, 2, 1):
                keep = lax.rem(sub8, 2 * step) < step
                group = [
                    jnp.where(keep, a + pltpu.roll(a, 8 - step, 0), b + pltpu.roll(b, step, 0))
                    for a, b in zip(group[:step], group[step:])
                ]
            sums = jnp.sum(group[0], axis=1, keepdims=True)
            part = jnp.where(lane8 == sub8 + first, sums, 0.0)
            spread = part if spread is None else spread + part
        return jnp.sum(spread, axis=0, keepdims=True)

    def send_sums(which, values):
        packed = pack(values)
        sent[which] = packed
        slots[which, me] = packed

        def send(px, py):
            pltpu.make_async_remote_copy(
                src_ref=sent.at[which], dst_ref=slots.at[which, me],
                send_sem=sum_send, recv_sem=sum_recv.at[which % 2],
                device_id=(px, py), device_id_type=MESH).start()

        for begin in (2, 1):
            def column(j, carry):
                for k in sorted(range(begin, nx, 2), key=lambda k: min(k, nx - k)):
                    send(lax.rem(gx + k, nx), jnp.where(2 * gy < ny, ny - 1 - j, j))
                return carry

            lax.fori_loop(0, ny, column, 0, unroll=count <= 64)
        for k in range(1, ny):
            send(gx, lax.rem(gy + k, ny))

    def take_sums(which, many):
        others = slots.at[which, pl.ds(0, count - 1)]
        pltpu.make_async_copy(others, others, sum_recv.at[which % 2]).wait()
        total = jnp.broadcast_to(tree([slots[which, k] for k in range(count)]), (8, LANES))
        return [jnp.broadcast_to(total[:, k:k + 1], (8, LANES)) for k in range(many)]

    def basis(b, core, window, last=True):
        v1 = apply_b(b, core, window)
        v2 = apply_b(v1, core, window)
        return (b, v1, v2, apply_half(v2, core)) if last else (b, v1, v2)

    def spread(tile, like):
        wide_tile = jnp.concatenate([tile] * (like.shape[1] // LANES), axis=1)
        return jnp.concatenate([wide_tile] * (like.shape[0] // 8), axis=0)

    def mix(c, v):
        parts = [spread(a, x) * x for a, x in zip(c, v)]
        return (parts[0] + parts[1]) + parts[2]

    def pairs(x, y):
        return [dot(x[0], y[0]), dot(x[0], y[1]), dot(x[1], y[1]),
                dot(x[1], y[2]), dot(x[2], y[2]),
                2.0 * dot(x[2], x[3]) if x is y
                else fold(x[2] * y[3] + y[2] * x[3])]

    def own_small(v):
        return [x[:rows, :cols] for x in v]

    wait_halo(halo_recv.at[0], 0)
    small_core = core_of("small")
    small_ones = unit("small")
    later = masked(field(0, "small"), "small")
    w = own_small(basis(
        value_rhs(later, slopes(later), own_guess(1, "small"), small_ones), small_core, "small"))
    moments = pairs(w, w)
    pl.semaphore_wait(ready, nx - 1)
    send_sums(0, moments)
    wait_halo(halo_recv.at[1], 1)
    core, ones = core_of("tall"), unit("tall")
    later = masked(field(0, "tall"), "tall")
    v = basis(
        value_rhs(later, slopes(later), own_guess(1, "tall"), ones), core, "tall", last=False)
    vs = [shrink(x, MARGIN) for x in v]
    steep = list(zip(*[slopes(x) for x in vs]))
    wait_halo(halo_recv.at[2], 2)
    guess = own_guess(0, "small")
    c = solve_small(take_sums(0, 6))

    first_small = mix(c, vs)
    w = own_small(basis(
        value_rhs(first_small, [mix(c, x) for x in steep], guess, small_ones), small_core, "small"))
    send_sums(1, pairs(w, w))
    first = mix(c, v)
    v = basis(value_rhs(first, slopes(first), own_guess(0, "tall"), ones), core, "tall", last=False)
    v = [x[low_mid:high_mid] for x in v]
    steep = list(zip(*[falls(x) for x in v]))
    face = faces(falls(first_small))
    behind = before(face[2]), before(face[3])
    density = ahead(masked(field(4, "mid"), "mid"))
    mid_core, mid_ones = core_of("mid"), unit("mid")
    c = solve_small(take_sums(1, 6))

    rhs = advance(density, faces([mix(c, x) for x in steep]), mid_ones)
    a = basis(rhs, mid_core, "mid", last=False)
    a = [shrink(x, 8) for x in a]
    last = apply_half(a[2], small_core)
    inner = own_small(a + [last])
    families = [
        own_small(basis(
            advance(ahead(x), face, small_ones, behind if x is a[2] else None), small_core, "small"))
        for x in a]
    moments = pairs(inner, inner)
    for i in range(3):
        for j in range(i, 3):
            moments += pairs(families[i], families[j])
    send_sums(2, moments)
    both_ref[0] = mix(c, [x[8:8 + rows, :cols] for x in v])
    wait_halo(halo_send, 0, 1, 2)
    others = slots.at[:, pl.ds(0, count - 1)]
    pltpu.make_async_copy(others, others, sum_send).wait()
    total = take_sums(2, len(moments))
    c = solve_small(total[:6])
    picks = [(i, j) for i in range(3) for j in range(i, 3)]
    weights = [c[i] * c[j] * (1.0 if i == j else 2.0) for i, j in picks]
    nu = [
        tree([weight * total[6 + 6 * at + k] for at, weight in enumerate(weights)])
        for k in range(6)
    ]
    e = solve_small(nu)
    result = mix(e, [mix(c, [families[i][k] for i in range(3)]) for k in range(3)])
    both_ref[1] = result


def solution(mesh):
    nx, ny = mesh.shape["gx"], mesh.shape["gy"]

    def shards(terminal, initial_density, density_guess, diagonal):
        rows, cols = terminal.shape
        tall = rows + 2 * MARGIN
        hbm = pl.BlockSpec(memory_space=pl.ANY)
        vmem = pl.BlockSpec(memory_space=pltpu.VMEM)
        shape = jax.ShapeDtypeStruct((rows, cols), jnp.float32)
        both = pl.pallas_call(
            functools.partial(kernel, nx, ny),
            out_shape=jax.ShapeDtypeStruct((2, rows, cols), jnp.float32),
            in_specs=[hbm] * 4,
            out_specs=vmem,
            scratch_shapes=[
                pltpu.VMEM((5, tall, cols), jnp.float32),
                pltpu.VMEM((5, tall, LANES), jnp.float32),
                pltpu.VMEM((5, tall, LANES), jnp.float32),
                pltpu.VMEM((3, 2, 4, 4, cols), jnp.float32),
                pltpu.VMEM((3, 2, 4, 4, cols), jnp.float32),
                pltpu.VMEM((3, 2, 4, 4, LANES), jnp.float32),
                pltpu.VMEM((3, 2, 4, 4, LANES), jnp.float32),
                pltpu.VMEM((3, 1, LANES), jnp.float32),
                pltpu.VMEM((3, nx * ny, 1, LANES), jnp.float32),
                pltpu.VMEM((10 * 4 * (rows // 8 + 2) * (cols // LANES + 2), 4, LANES), jnp.float32),
                pltpu.SemaphoreType.DMA,
                pltpu.SemaphoreType.DMA((3,)),
                pltpu.SemaphoreType.DMA,
                pltpu.SemaphoreType.DMA,
                pltpu.SemaphoreType.DMA((2,)),
                pltpu.SemaphoreType.REGULAR,
                pltpu.VMEM((tall, cols + LANES), jnp.float32),
                pltpu.VMEM((rows + 16, cols + LANES), jnp.float32),
                pltpu.VMEM((rows + 8, cols + LANES), jnp.float32),
            ],
            compiler_params=pltpu.CompilerParams(collective_id=0, has_side_effects=True, vmem_limit_bytes=8 * 1024 * 1024),
        )(*[pltpu.with_memory_space_constraint(x, pltpu.HBM) for x in (terminal, initial_density, density_guess, diagonal)])
        return both[0], both[1]

    placed = (P("gx", "gy"), P("gx", "gy"), P(None, "gx", "gy"), P("gx", "gy"))
    return jax.shard_map(
        shards,
        mesh=mesh,
        in_specs=placed,
        out_specs=(P("gx", "gy"), P("gx", "gy")),
        check_vma=False,
    )
```
